128 devices in a mesh: pod: 1, data: 2 (over core), cp: 64 (over z, y, x).
Axes of the slice: x: 4, y: 4, z: 4, core: 2. Of those that a mesh axis runs over, the one named last changes fastest.
Arguments:
- c_latent: bfloat16 [2, 65536, 512], P(('pod', 'data'), 'cp')
- k_rope: bfloat16 [2, 65536, 64], P(('pod', 'data'), 'cp')
- queries: bfloat16 [2, 65536, 1, 192], P(('pod', 'data'), 'cp')
- w_uk: bfloat16 [512, 1, 128], replicated
- w_uv: bfloat16 [512, 1, 128], replicated
- d_out: bfloat16 [2, 65536, 1, 128], P(('pod', 'data'), 'cp')
Outputs:
- output 1: bfloat16 [2, 65536, 1, 128], P(('pod', 'data'), 'cp')
- output 2: float32 [2, 65536, 1, 192], P(('pod', 'data'), 'cp')
- output 3: float32 [2, 65536, 512], P(('pod', 'data'), 'cp')
- output 4: float32 [2, 65536, 64], P(('pod', 'data'), 'cp')
- output 5: float32 [512, 1, 128], P('pod')
- output 6: float32 [512, 1, 128], P('pod')
All inputs are finite; a program needn't handle non-finite values.
Results may differ from the reference program's by a relative error of at most 0.00698307.
Values are sent between devices in bfloat16 or wider.
A program may use at most 1 GiB of HBM per device.

```python
import functools
import jax
import jax.numpy as jnp
from jax import lax

NUM_SEQS = 2
RING_SIZE = 64
TOK_DEV = 1024
NUM_HEADS = 1
LATENT = 512
ROPE_DIM = 64
NOPE_DIM = 128
VALUE_DIM = 128

SEQ_LEN = RING_SIZE * TOK_DEV
HALF_LEN = TOK_DEV // 2
NUM_CHUNKS = 2 * RING_SIZE
QK_DIM = NOPE_DIM + ROPE_DIM


def setup_inputs(seed: int = 0, part: int = 0) -> dict:
    base_key = jax.random.key(seed)
    shared_key, data_key = jax.random.split(base_key)
    part_key = jax.random.fold_in(data_key, part)
    key_c, key_kpe, key_q, key_grad = jax.random.split(part_key, 4)
    key_uk, key_uv = jax.random.split(shared_key)
    latent = jax.random.normal(key_c, (NUM_SEQS, SEQ_LEN, LATENT), jnp.float32)
    rope_key = jax.random.normal(key_kpe, (NUM_SEQS, SEQ_LEN, ROPE_DIM), jnp.float32)
    queries = jax.random.normal(key_q, (NUM_SEQS, SEQ_LEN, NUM_HEADS, QK_DIM), jnp.float32)
    w_uk = jax.random.normal(key_uk, (LATENT, NUM_HEADS, NOPE_DIM), jnp.float32) * LATENT ** -0.5
    w_uv = jax.random.normal(key_uv, (LATENT, NUM_HEADS, VALUE_DIM), jnp.float32) * LATENT ** -0.5
    d_out = jax.random.normal(key_grad, (NUM_SEQS, SEQ_LEN, NUM_HEADS, VALUE_DIM), jnp.float32)
    return {'c_latent': latent.astype(jnp.bfloat16), 'k_rope': rope_key.astype(jnp.bfloat16), 'queries': queries.astype(jnp.bfloat16), 'w_uk': w_uk.astype(jnp.bfloat16), 'w_uv': w_uv.astype(jnp.bfloat16), 'd_out': d_out.astype(jnp.bfloat16)}


def token_positions():
    rows = jnp.arange(SEQ_LEN)
    dev_index = rows // TOK_DEV
    piece = jnp.where((rows // HALF_LEN) % 2 == 0, dev_index, NUM_CHUNKS - 1 - dev_index)
    return piece * HALF_LEN + rows % HALF_LEN


def piece_attention(q_piece, key_nope, key_rope, values, mask):
    q_nope = q_piece[..., :NOPE_DIM]
    q_rope = q_piece[..., NOPE_DIM:]
    scores = jnp.einsum('qhd,khd->hqk', q_nope, key_nope) + jnp.einsum('qhe,ke->hqk', q_rope, key_rope)
    scores = jnp.where(mask[None], scores * QK_DIM ** -0.5, -1.0e30)
    weights = jax.nn.softmax(scores, axis=-1)
    return jnp.einsum('hqk,khd->qhd', weights, values)


def reference(c_latent, k_rope, queries, w_uk, w_uv, d_out):
    positions = token_positions()
    piece_pos = positions.reshape(NUM_CHUNKS, HALF_LEN)
    uk_flat = w_uk.reshape(LATENT, NUM_HEADS * NOPE_DIM)
    uv_flat = w_uv.reshape(LATENT, NUM_HEADS * VALUE_DIM)

    def one_sequence(carry, seq_in):
        latent_seq, rope_seq, query_seq, grad_seq = seq_in
        key_nope = jnp.dot(latent_seq, uk_flat, preferred_element_type=jnp.float32).astype(jnp.bfloat16)
        values = jnp.dot(latent_seq, uv_flat, preferred_element_type=jnp.float32).astype(jnp.bfloat16)
        key_nope = key_nope.astype(jnp.float32).reshape(SEQ_LEN, NUM_HEADS, NOPE_DIM)
        values = values.astype(jnp.float32).reshape(SEQ_LEN, NUM_HEADS, VALUE_DIM)
        key_rope = rope_seq.astype(jnp.float32)
        q_pieces = query_seq.astype(jnp.float32).reshape(NUM_CHUNKS, HALF_LEN, NUM_HEADS, QK_DIM)
        g_pieces = grad_seq.astype(jnp.float32).reshape(NUM_CHUNKS, HALF_LEN, NUM_HEADS, VALUE_DIM)

        def piece_step(grad_sums, piece_in):
            q_piece, g_piece, pos_piece = piece_in
            mask = positions[None, :] <= pos_piece[:, None]
            attend = functools.partial(piece_attention, mask=mask)
            out_piece, pullback = jax.vjp(attend, q_piece, key_nope, key_rope, values)
            dq_piece, dk_nope, dk_rope, d_values = pullback(g_piece)
            grad_sums = (grad_sums[0] + dk_nope, grad_sums[1] + dk_rope, grad_sums[2] + d_values)
            return grad_sums, (out_piece.astype(jnp.bfloat16), dq_piece)

        start_sums = (jnp.zeros_like(key_nope), jnp.zeros_like(key_rope), jnp.zeros_like(values))
        grad_sums, piece_outs = lax.scan(piece_step, start_sums, (q_pieces, g_pieces, piece_pos))
        dk_nope, dk_rope, d_values = grad_sums
        dk_flat = dk_nope.reshape(SEQ_LEN, NUM_HEADS * NOPE_DIM)
        dv_flat = d_values.reshape(SEQ_LEN, NUM_HEADS * VALUE_DIM)
        grad_latent = jnp.dot(dk_flat, uk_flat.astype(jnp.float32).T, preferred_element_type=jnp.float32) + jnp.dot(dv_flat, uv_flat.astype(jnp.float32).T, preferred_element_type=jnp.float32)
        latent32 = latent_seq.astype(jnp.float32)
        carry = (carry[0] + jnp.dot(latent32.T, dk_flat, preferred_element_type=jnp.float32), carry[1] + jnp.dot(latent32.T, dv_flat, preferred_element_type=jnp.float32))
        results = (piece_outs[0].reshape(SEQ_LEN, NUM_HEADS, VALUE_DIM), piece_outs[1].reshape(SEQ_LEN, NUM_HEADS, QK_DIM), grad_latent, dk_rope)
        return carry, results

    start_carry = (jnp.zeros((LATENT, NUM_HEADS * NOPE_DIM), jnp.float32), jnp.zeros((LATENT, NUM_HEADS * VALUE_DIM), jnp.float32))
    weight_grads, results = lax.scan(one_sequence, start_carry, (c_latent, k_rope, queries, d_out))
    attn_out, grad_queries, grad_latent, grad_rope = results
    grad_w_uk = weight_grads[0].reshape(LATENT, NUM_HEADS, NOPE_DIM)
    grad_w_uv = weight_grads[1].reshape(LATENT, NUM_HEADS, VALUE_DIM)
    return (attn_out, grad_queries, grad_latent, grad_rope, grad_w_uk, grad_w_uv)
```

```python
import functools

import jax
import jax.numpy as jnp
from jax import lax
from jax.experimental import pallas as pl
from jax.experimental.pallas import tpu as pltpu
from jax.sharding import PartitionSpec as P

BF = jnp.bfloat16
F32 = jnp.float32
NEG_BIG = -1.0e30
HALF = 512
NOPE = 128
ROPE = 64
QK = NOPE + ROPE
VAL = 128
AUG = 16
SCALE = QK ** -0.5
EXP2_SCALE = SCALE * 1.4426950408889634


def mm(a, b):
    return jnp.dot(a, b, preferred_element_type=F32)


def gray(r):
    return r ^ (r >> 1)


def core_kernel(qn_in, qr_in, kn_in, kr_in, vt_in, do_in,
                o_recv, dq_recv, dk_recv, dv_recv,
                q_s, qr_s, k_s, kr_s, vt_s, do_s, qt_s, kt_s, dot_s,
                ot_s, m_s, l_s, dq_s, dqr_s, dk_s, dv_s, st_s, st_r,
                sc0, sc1, dp0, dp1, pr0, pr1, ds0, ds1,
                q_send, q_recv_sem, k_send, k_recv_sem, do_send, do_recv_sem,
                st_send, st_recv_sem, o_send, o_recv_sem, dq_send, dq_recv_sem, dk_send, dk_recv_sem, own_sem):
    me = lax.axis_index('cp')
    x = me % 4
    y0 = (me // 4) % 2
    y1 = (me // 8) % 2
    z = me // 16
    row = me // 8
    col = me % 8

    def row_slot(rank):
        return 4 * (y0 ^ (rank // 4)) + (x + gray(rank % 4)) % 4

    def col_slot(rank):
        return 2 * ((z + gray(rank % 4)) % 4) + (y1 ^ (rank // 4))

    def row_dev(rank):
        return {'cp': 8 * row + row_slot(rank)}

    def col_dev(rank):
        return {'cp': 8 * col_slot(rank) + col}

    barrier = pltpu.get_barrier_semaphore()
    for r in range(1, 8):
        pl.semaphore_signal(barrier, inc=1, device_id=row_dev(r))
        pl.semaphore_signal(barrier, inc=1, device_id=col_dev(r))
    pl.semaphore_wait(barrier, 14)

    def q_copies(n, src_n, src_r, slot, dev):
        return [
            pltpu.make_async_remote_copy(src_n, q_s.at[slot, :, :, pl.ds(0, NOPE)], q_send.at[0, n], q_recv_sem.at[0, slot], device_id=dev),
            pltpu.make_async_remote_copy(src_r, qr_s.at[slot], q_send.at[1, n], q_recv_sem.at[1, slot], device_id=dev),
        ]

    def k_copies(n, src_n, src_r, src_v, slot, dev):
        return [
            pltpu.make_async_remote_copy(src_n, k_s.at[slot, :, :, pl.ds(0, NOPE)], k_send.at[0, n], k_recv_sem.at[0, slot], device_id=dev),
            pltpu.make_async_remote_copy(src_r, kr_s.at[slot], k_send.at[1, n], k_recv_sem.at[1, slot], device_id=dev),
            pltpu.make_async_remote_copy(src_v, vt_s.at[slot, :, pl.ds(0, VAL)], k_send.at[2, n], k_recv_sem.at[2, slot], device_id=dev),
        ]

    def do_copies(n, src, slot, dev):
        return [pltpu.make_async_remote_copy(src, do_s.at[slot, :, :, pl.ds(0, VAL)], do_send.at[n], do_recv_sem.at[slot], device_id=dev)]

    def own_q(n):
        return q_copies(n, qn_in, qr_in, col, row_dev(n + 1))

    def own_k(n):
        return k_copies(n, kn_in, kr_in, vt_in, row, col_dev(n + 1))

    def own_do(n):
        return do_copies(n, do_in, col, row_dev(n + 1))

    def pair_q(n):
        s = row_slot(4)
        return q_copies(4 + n, q_s.at[s, :, :, pl.ds(0, NOPE)], qr_s.at[s], s, row_dev(n + 1))

    def pair_k(n):
        s = col_slot(4)
        return k_copies(4 + n, k_s.at[s, :, :, pl.ds(0, NOPE)], kr_s.at[s], vt_s.at[s, :, pl.ds(0, VAL)], s, col_dev(n + 1))

    def pair_do(n):
        s = row_slot(4)
        return do_copies(4 + n, do_s.at[s, :, :, pl.ds(0, VAL)], s, row_dev(n + 1))

    def start(copies):
        for c in copies:
            c.start()

    for n in (3, 0, 1, 2):
        start(own_q(n))
        start(own_k(n))
    for n in (3, 0, 1, 2):
        start(own_do(n))

    ones = jnp.where(lax.broadcasted_iota(jnp.int32, (AUG, HALF), 0) < 3, 1.0, 0.0).astype(BF)

    def clear(s, _):
        for h in range(2):
            ot_s[s, h] = jnp.zeros((VAL, HALF), F32)
            dq_s[s, h] = jnp.zeros((HALF, QK), F32)
            dk_s[s, h] = jnp.zeros((QK, HALF), F32)
            dv_s[s, h] = jnp.zeros((VAL, HALF), F32)
            m_s[s, h] = jnp.full((1, HALF), NEG_BIG, F32)
            l_s[s, h] = jnp.zeros((1, HALF), F32)
            kt_s[s, h, QK:QK + AUG] = ones
            vt_s[s, h, VAL:VAL + AUG] = ones
        return 0

    def place_q(s, h):
        q_s[s, h, :, NOPE:QK] = qr_s[s, :, h * ROPE:(h + 1) * ROPE]
        qt_s[s, h] = q_s[s, h, :, 0:QK].T

    def place_k(s, h):
        k_s[s, h, :, NOPE:QK] = kr_s[s, :, h * ROPE:(h + 1) * ROPE]
        kt_s[s, h, 0:QK] = k_s[s, h].T

    def place_do(s):
        for h in range(2):
            dot_s[s, h] = do_s[s, h, :, 0:VAL].T

    q_s[col, :, :, 0:NOPE] = qn_in[...]
    qr_s[col] = qr_in[...]
    k_s[row, :, :, 0:NOPE] = kn_in[...]
    kr_s[row] = kr_in[...]
    vt_s[row, :, 0:VAL] = vt_in[...]
    do_s[col, :, :, 0:VAL] = do_in[...]
    for h in range(2):
        place_q(col, h)
        place_k(row, h)
    place_do(col)
    lax.fori_loop(0, 8, clear, 0)

    def wait_q(rank):
        for c in q_copies(0, qn_in, qr_in, row_slot(rank), row_dev(1)):
            c.wait_recv()

    def wait_k(rank):
        for c in k_copies(0, kn_in, kr_in, vt_in, col_slot(rank), col_dev(1)):
            c.wait_recv()

    def wait_do(rank):
        for c in do_copies(0, do_in, row_slot(rank), row_dev(1)):
            c.wait_recv()

    def low_pair(ks, qs):
        return jnp.where((ks < row) | ((ks == row) & (col <= qs)), 0, 1)

    def f_rank(t):
        late = t >= 40
        u = jnp.where(late, t - 40, t)
        mid = t >= 20
        v = jnp.where(mid, t - 20, t)
        a = jnp.where(late, 5 + u // 8, v // 4)
        b = jnp.where(late, u % 8, jnp.where(mid, 4, 0) + v % 4)
        return a, b

    def f_block(t, second):
        a, b = f_rank(t)
        ks, qs = col_slot(a), row_slot(b)
        if not second:
            return ks, qs, 0, 1
        h = low_pair(ks, qs)
        return ks, qs, h, h

    def f_scores(sc, blk):
        ks, qs, kh, qh = blk
        sc[...] = mm(k_s[ks, kh], qt_s[qs, qh])

    def f_soft(s, qs, qh):
        m0 = m_s[qs, qh]
        m1 = jnp.maximum(m0, jnp.max(s, axis=0, keepdims=True))
        p = jnp.exp2((s - m1) * EXP2_SCALE)
        alpha = jnp.exp2((m0 - m1) * EXP2_SCALE)
        l_s[qs, qh] = l_s[qs, qh] * alpha + jnp.sum(p, axis=0, keepdims=True)
        m_s[qs, qh] = m1
        return p.astype(BF), alpha

    def f_use(sc, blk, mask=False):
        ks, qs, kh, qh = blk
        s = sc[...]
        if mask:
            keys = lax.broadcasted_iota(jnp.int32, (HALF, HALF), 0)
            rows = lax.broadcasted_iota(jnp.int32, (HALF, HALF), 1)
            s = jnp.where(keys <= rows, s, NEG_BIG)
        p, alpha = f_soft(s, qs, qh)
        ot_s[qs, qh] = ot_s[qs, qh] * alpha + mm(vt_s[ks, kh, 0:VAL], p)

    for kh, qh in ((0, 0), (0, 1), (1, 1)):
        blk = (row, col, kh, qh)
        f_scores(sc0, blk)
        f_use(sc0, blk, mask=kh == qh)

    def stats_copy(slot, n):
        return pltpu.make_async_remote_copy(st_s.at[slot], st_r.at[slot, col], st_send.at[slot, n - 1], st_recv_sem.at[slot], device_id=row_dev(n))

    def send_stats(qs):
        for h in range(2):
            d = jnp.sum(ot_s[qs, h] * dot_s[qs, h].astype(F32), axis=0, keepdims=True)
            for j in range(4):
                c = slice(128 * j, 128 * j + 128)
                r = 4 * h + j
                st_s[qs, r:r + 1] = m_s[qs, h, :, c]
                st_s[qs, 8 + r:9 + r] = l_s[qs, h, :, c]
                st_s[qs, 16 + r:17 + r] = d[:, c]

    def start_stats(qs):
        for n in range(1, 8):
            stats_copy(qs, n).start()
        st_r[qs, col] = st_s[qs]

    def f_arrive(t):
        a, b = f_rank(t)
        first_q = (t < 4) | ((t >= 20) & (t < 24))
        first_k = ((t < 20) & (t % 4 == 0)) | ((t >= 40) & (t % 8 == 0))

        @pl.when(first_q & (b > 0) & (b != 4))
        def _():
            wait_q(b)

        @pl.when(first_q & (b > 0))
        def _():
            s = row_slot(b)
            for h in range(2):
                place_q(s, h)

        @pl.when(first_k & (a > 0) & (a != 4))
        def _():
            wait_k(a)

        @pl.when(first_k & (a > 0))
        def _():
            s = col_slot(a)
            for h in range(2):
                place_k(s, h)

        @pl.when(t == T_RELAY_Q)
        def _():
            wait_q(4)
            for n in range(3):
                start(pair_q(n))

        @pl.when(t == T_RELAY_K)
        def _():
            wait_k(4)
            for n in range(3):
                start(pair_k(n))

        @pl.when(t == T_RELAY_DO)
        def _():
            wait_do(4)
            for n in range(3):
                start(pair_do(n))
            place_do(row_slot(4))

        @pl.when((t >= 48) & (t < 56) & (b > 0))
        def _():
            @pl.when(b != 4)
            def _():
                wait_do(b)
                place_do(row_slot(b))

    f_arrive(1)
    f_scores(sc0, f_block(1, False))

    def f_step(t, _):
        nxt = jnp.minimum(t + 1, 63)

        @pl.when(t < 63)
        def _():
            f_arrive(nxt)

        b1, b2 = f_block(t, False), f_block(t, True)
        f_scores(sc1, b2)
        f_use(sc0, b1)
        f_scores(sc0, f_block(nxt, False))
        f_use(sc1, b2)

        @pl.when(t >= 57)
        def _():
            start_stats(row_slot(t - 57))

        @pl.when(t >= 56)
        def _():
            send_stats(row_slot(t - 56))
        return 0

    lax.fori_loop(1, 64, f_step, 0)
    start_stats(row_slot(7))

    def columns(v):
        flat = jnp.concatenate([v[j:j + 1] for j in range(4)], axis=1)
        hi = flat.astype(BF).astype(F32)
        mid = (flat - hi).astype(BF).astype(F32)
        lo = flat - hi - mid
        return jnp.concatenate([hi, mid, lo, jnp.zeros((AUG - 3, HALF), F32)], axis=0).T.astype(BF)

    def prepare(qs):
        pltpu.make_async_copy(st_r.at[qs, pl.ds(0, 7)], st_r.at[qs, pl.ds(0, 7)], st_recv_sem.at[qs]).wait()
        m = st_r[qs, :, 0:8]
        m_all = jnp.max(m, axis=0)
        w = jnp.exp2((m - m_all[None]) * EXP2_SCALE)
        l_all = jnp.sum(w * st_r[qs, :, 8:16], axis=0)
        inv = 1.0 / l_all
        delta = jnp.sum(w * st_r[qs, :, 16:24], axis=0) * inv
        lse = m_all + jnp.log2(l_all) * (1.0 / EXP2_SCALE)
        mine = jnp.exp2((st_s[qs, 0:8] - m_all) * EXP2_SCALE) * inv
        for h in range(2):
            q_s[qs, h, :, QK:QK + AUG] = columns(-lse[4 * h:4 * h + 4])
            do_s[qs, h, :, VAL:VAL + AUG] = columns(-delta[4 * h:4 * h + 4])
            for j in range(4):
                r = 4 * h + j
                c = slice(128 * j, 128 * j + 128)
                ot_s[qs, h, :, c] = ot_s[qs, h, :, c] * mine[r:r + 1]

    def o_copy(rank):
        s = row_slot(rank)
        return pltpu.make_async_remote_copy(ot_s.at[s], o_recv.at[col], o_send.at[rank], o_recv_sem.at[col], device_id=row_dev(rank))

    def b_rank(t):
        own = t >= 56
        return jnp.where(own, 0, 1 + t // 8), jnp.where(own, t - 55, t % 8)

    def b_block(t, second):
        a, b = b_rank(t)
        ks, qs = col_slot(a), row_slot(b)
        if not second:
            return ks, qs, 0, 1
        h = low_pair(ks, qs)
        return ks, qs, h, h

    def b_scores(sc, dp, blk):
        ks, qs, kh, qh = blk
        sc[...] = mm(q_s[qs, qh], kt_s[ks, kh])
        dp[...] = mm(do_s[qs, qh], vt_s[ks, kh])

    def b_elem(sc, dp, pr, ds, blk, mask=False):
        ks, qs, kh, qh = blk
        p = jnp.exp2(sc[...] * EXP2_SCALE)
        if mask:
            rows = lax.broadcasted_iota(jnp.int32, (HALF, HALF), 0)
            keys = lax.broadcasted_iota(jnp.int32, (HALF, HALF), 1)
            p = jnp.where(keys <= rows, p, 0.0)
        pr[...] = p.astype(BF)
        ds[...] = (p * dp[...]).astype(BF)

    def b_grads(pr, ds, blk):
        ks, qs, kh, qh = blk
        p = pr[...]
        g = ds[...]
        dv_s[ks, kh] += mm(dot_s[qs, qh], p)
        dk_s[ks, kh] += mm(qt_s[qs, qh], g)
        dq_s[qs, qh] += mm(g, k_s[ks, kh])

    def dkv_copies(rank):
        s = col_slot(rank)
        dev = col_dev(rank)
        return [
            pltpu.make_async_remote_copy(dk_s.at[s], dk_recv.at[row], dk_send.at[0, rank], dk_recv_sem.at[0, row], device_id=dev),
            pltpu.make_async_remote_copy(dv_s.at[s], dv_recv.at[row], dk_send.at[1, rank], dk_recv_sem.at[1, row], device_id=dev),
        ]

    def dq_copies(rank):
        s = row_slot(rank)
        dev = row_dev(rank)
        return [
            pltpu.make_async_remote_copy(dq_s.at[s, :, :, pl.ds(0, NOPE)], dq_recv.at[col, pl.ds(0, 2)], dq_send.at[0, rank], dq_recv_sem.at[0, col], device_id=dev),
            pltpu.make_async_remote_copy(dqr_s.at[s], dq_recv.at[col, 2], dq_send.at[1, rank], dq_recv_sem.at[1, col], device_id=dev),
        ]

    def pack_dq(qs):
        dqr_s[qs, :, 0:ROPE] = dq_s[qs, 0, :, NOPE:QK]
        dqr_s[qs, :, ROPE:2 * ROPE] = dq_s[qs, 1, :, NOPE:QK]

    pr1[...] = jnp.zeros((HALF, HALF), BF)
    ds1[...] = jnp.zeros((HALF, HALF), BF)
    prepare(row_slot(0))
    b_scores(sc0, dp0, b_block(0, False))

    def b_step(t, _):
        @pl.when(t < 7)
        def _():
            prepare(row_slot(t + 1))

        b1, b2 = b_block(t, False), b_block(t, True)
        prev = b_block(jnp.maximum(t - 1, 0), True)
        nxt = b_block(jnp.minimum(t + 1, 62), False)
        b_scores(sc1, dp1, b2)
        b_elem(sc0, dp0, pr0, ds0, b1)
        b_grads(pr1, ds1, prev)
        b_scores(sc0, dp0, nxt)
        b_elem(sc1, dp1, pr1, ds1, b2)
        b_grads(pr0, ds0, b1)

        @pl.when((t >= 1) & (t < 8))
        def _():
            o_copy(t).start()

        @pl.when((t % 8 == 0) & (t > 0))
        def _():
            start(dkv_copies(t // 8))

        @pl.when(t >= 58)
        def _():
            start(dq_copies(t - 57))

        @pl.when(t >= 57)
        def _():
            pack_dq(row_slot(t - 56))
        return 0

    lax.fori_loop(0, 63, b_step, 0)
    b_grads(pr1, ds1, b_block(62, True))
    pack_dq(row_slot(7))
    for kh, qh in ((0, 0), (0, 1), (1, 1)):
        blk = (row, col, kh, qh)
        b_scores(sc0, dp0, blk)
        b_elem(sc0, dp0, pr0, ds0, blk, mask=kh == qh)
        b_grads(pr0, ds0, blk)
        if kh == 0 and qh == 0:
            start(dq_copies(6))
            start(dq_copies(7))
    pack_dq(col)

    own = [
        pltpu.make_async_copy(ot_s.at[col], o_recv.at[col], own_sem.at[0]),
        pltpu.make_async_copy(dq_s.at[col, :, :, pl.ds(0, NOPE)], dq_recv.at[col, pl.ds(0, 2)], own_sem.at[1]),
        pltpu.make_async_copy(dqr_s.at[col], dq_recv.at[col, 2], own_sem.at[2]),
        pltpu.make_async_copy(dk_s.at[row], dk_recv.at[row], own_sem.at[3]),
        pltpu.make_async_copy(dv_s.at[row], dv_recv.at[row], own_sem.at[4]),
    ]
    start(own)

    for n in range(4):
        for c in own_q(n) + own_k(n) + own_do(n):
            c.wait_send()
    for n in range(3):
        for c in pair_q(n) + pair_k(n) + pair_do(n):
            c.wait_send()
    for r in range(1, 8):
        for s in range(8):
            stats_copy(s, r).wait_send()
        o_copy(r).wait_send()
        for c in dkv_copies(r) + dq_copies(r):
            c.wait_send()
        s = row_slot(r)
        pltpu.make_async_remote_copy(ot_s.at[0], o_recv.at[s], o_send.at[r], o_recv_sem.at[s], device_id=row_dev(r)).wait_recv()
        pltpu.make_async_remote_copy(dq_s.at[0, :, :, pl.ds(0, NOPE)], dq_recv.at[s, pl.ds(0, 2)], dq_send.at[0, r], dq_recv_sem.at[0, s], device_id=row_dev(r)).wait_recv()
        pltpu.make_async_remote_copy(dqr_s.at[0], dq_recv.at[s, 2], dq_send.at[1, r], dq_recv_sem.at[1, s], device_id=row_dev(r)).wait_recv()
        s = col_slot(r)
        pltpu.make_async_remote_copy(dk_s.at[0], dk_recv.at[s], dk_send.at[0, r], dk_recv_sem.at[0, s], device_id=col_dev(r)).wait_recv()
        pltpu.make_async_remote_copy(dv_s.at[0], dv_recv.at[s], dk_send.at[1, r], dk_recv_sem.at[1, s], device_id=col_dev(r)).wait_recv()
    for c in own:
        c.wait()


T_RELAY_Q = 4
T_RELAY_K = 8
T_RELAY_DO = 40


def core_call(qn, qr, kn, kr, vt, do):
    vmem = pltpu.VMEM
    dma = pltpu.SemaphoreType.DMA
    n = 8
    scratch = [
        vmem((n, 2, HALF, QK + AUG), BF), vmem((n, HALF, 128), BF), vmem((n, 2, HALF, QK), BF), vmem((n, HALF, 128), BF),
        vmem((n, 2, VAL + AUG, HALF), BF), vmem((n, 2, HALF, VAL + AUG), BF),
        vmem((n, 2, QK, HALF), BF), vmem((n, 2, QK + AUG, HALF), BF), vmem((n, 2, VAL, HALF), BF),
        vmem((n, 2, VAL, HALF), F32), vmem((n, 2, 1, HALF), F32), vmem((n, 2, 1, HALF), F32),
        vmem((n, 2, HALF, QK), F32), vmem((n, HALF, 128), F32), vmem((n, 2, QK, HALF), F32), vmem((n, 2, VAL, HALF), F32),
        vmem((n, 24, 128), F32), vmem((n, n, 24, 128), F32),
        vmem((HALF, HALF), F32), vmem((HALF, HALF), F32), vmem((HALF, HALF), F32), vmem((HALF, HALF), F32),
        vmem((HALF, HALF), BF), vmem((HALF, HALF), BF), vmem((HALF, HALF), BF), vmem((HALF, HALF), BF),
                dma((2, 7)), dma((2, n)), dma((3, 7)), dma((3, n)), dma((7,)), dma((n,)),
        dma((n, 7)), dma((n,)), dma((n,)), dma((n,)), dma((2, n)), dma((2, n)), dma((2, n)), dma((2, n)), dma((5,)),
    ]
    return pl.pallas_call(
        core_kernel,
        out_shape=(
            jax.ShapeDtypeStruct((n, 2, VAL, HALF), F32),
            jax.ShapeDtypeStruct((n, 3, HALF, 128), F32),
            jax.ShapeDtypeStruct((n, 2, QK, HALF), F32),
            jax.ShapeDtypeStruct((n, 2, VAL, HALF), F32),
        ),
        in_specs=[pl.BlockSpec(memory_space=pltpu.VMEM)] * 6,
        out_specs=[pl.BlockSpec(memory_space=pl.ANY)] * 4,
        scratch_shapes=scratch,
        compiler_params=pltpu.CompilerParams(collective_id=0, has_side_effects=True, vmem_limit_bytes=67043328),
        name='core',
    )(qn, qr, kn, kr, vt, do)


def solution(mesh):
    token_spec = P(('pod', 'data'), 'cp', None)
    head_spec = P(('pod', 'data'), 'cp', None, None)
    weight_spec = P(None, None, None)
    sum_spec = P('pod', None, None)

    def per_device(c_latent, k_rope, queries, w_uk, w_uv, d_out):
        latent = c_latent[0]
        q = queries[0, :, 0, :]
        wk, wv = w_uk[:, 0, :], w_uv[:, 0, :]
        kn = mm(latent, wk).astype(BF).reshape(2, HALF, NOPE)
        vt = jnp.einsum('ld,htl->hdt', wv, latent.reshape(2, HALF, -1), preferred_element_type=F32).astype(BF)
        kr = jnp.concatenate([k_rope[0, :HALF], k_rope[0, HALF:]], axis=1)
        qn = q[:, :NOPE].reshape(2, HALF, NOPE)
        qr = jnp.concatenate([q[:HALF, NOPE:], q[HALF:, NOPE:]], axis=1)
        do = d_out[0, :, 0, :].reshape(2, HALF, VAL)
        o_parts, dq_parts, dk_parts, dv_parts = core_call(qn, qr, kn, kr, vt, do)
        attn_out = jnp.sum(o_parts, axis=0).transpose(0, 2, 1).astype(BF).reshape(1, 2 * HALF, 1, VAL)
        dq = jnp.sum(dq_parts, axis=0) * SCALE
        dq_rope = jnp.concatenate([dq[2, :, :ROPE], dq[2, :, ROPE:]], axis=0)
        grad_q = jnp.concatenate([dq[:2].reshape(2 * HALF, NOPE), dq_rope], axis=-1).reshape(1, 2 * HALF, 1, QK)
        dk = jnp.sum(dk_parts, axis=0) * SCALE
        dv = jnp.sum(dv_parts, axis=0)
        grad_rope = dk[:, NOPE:].transpose(0, 2, 1).reshape(1, 2 * HALF, ROPE)
        dkn = dk[:, :NOPE]
        grad_latent = (jnp.einsum('hdt,ld->htl', dkn, wk, preferred_element_type=F32) + jnp.einsum('hdt,ld->htl', dv, wv, preferred_element_type=F32)).reshape(1, 2 * HALF, -1)
        lat = latent.reshape(2, HALF, -1)
        grad_w_uk = lax.psum(jnp.einsum('htl,hdt->ld', lat, dkn, preferred_element_type=F32), ('data', 'cp'))
        grad_w_uv = lax.psum(jnp.einsum('htl,hdt->ld', lat, dv, preferred_element_type=F32), ('data', 'cp'))
        return attn_out, grad_q, grad_latent, grad_rope, grad_w_uk[:, None], grad_w_uv[:, None]

    return jax.shard_map(per_device, mesh=mesh, in_specs=(token_spec, token_spec, head_spec, weight_spec, weight_spec, head_spec), out_specs=(head_spec, head_spec, token_spec, token_spec, sum_spec, sum_spec), check_vma=False)
```

```python
import jax
import jax.numpy as jnp
from jax import lax
from jax.experimental import pallas as pl
from jax.experimental.pallas import tpu as pltpu
from jax.sharding import PartitionSpec as P

BF = jnp.bfloat16
F32 = jnp.float32
NEG_BIG = -1.0e30
HALF = 512
LATENT = 512
NOPE = 128
ROPE = 64
QK = NOPE + ROPE
VAL = 128
AUG = 16
SCALE = QK ** -0.5
EXP2_SCALE = SCALE * 1.4426950408889634
T_OWN_DO = 12
T_RELAY_Q = 9
T_RELAY_K = 9
T_RELAY_DO = 34
T_LAST = 56
T_PAIR_O = 38
T_PAIR_KV = 53


def mm(a, b):
    return jnp.dot(a, b, preferred_element_type=F32)


def mm_t(a, b):
    return lax.dot_general(a, b, (((1,), (1,)), ((), ())), preferred_element_type=F32)


def gray(r):
    return r ^ (r >> 1)


def order(n, ranks):
    out = ranks[-1]
    for i in range(len(ranks) - 2, -1, -1):
        out = jnp.where(n <= i, ranks[i], out)
    return out


def among(t, steps):
    out = t == steps[0]
    for v in steps[1:]:
        out = out | (t == v)
    return out


def at(t, steps, ranks):
    out = ranks[-1]
    for v, r in list(zip(steps, ranks))[-2::-1]:
        out = jnp.where(t <= v, r, out)
    return out


def core_kernel(c_in, kpe_in, q_in, wk_in, wv_in, do_in,
                out_o, out_q, out_c, out_r, out_uk, out_uv, xo, xq, xqv, zkv, zkvv, po, pq, pkv,
                q_s, qr_s, k_s, kr_s, vt_s, do_s, qt_s, kt_s, dot_s,
                ot_s, m_s, l_s, dq_s, dqr_s, dk_s, dv_s, st_s, st_r, stg, w_s, ws_r, wl_r, rope_s, q_out_s, wr_s, wr_r, wc_s, wc_r,
                sc0, sc1, dp0, dp1, pr0, pr1, ds0, ds1,
                q_send, q_recv, k_send, k_recv, do_send, do_recv, st_send, st_recv,
                xo_send, xo_recv, xq_send, xq_recv, xqv_send, xqv_recv, zkv_send, zkv_recv, zkvv_send, zkvv_recv, p_send, p_recv, loc, outs, w_send, w_recv):
    me = lax.axis_index('cp')
    core = lax.axis_index('data')
    x = me % 4
    y0 = (me // 4) % 2
    y1 = (me // 8) % 2
    z = me // 16
    row = me // 8
    col = me % 8

    def row_slot(rank):
        return 4 * (y0 ^ (rank // 4)) + (x + gray(rank % 4)) % 4

    def col_slot(rank):
        return 2 * ((z + gray(rank % 4)) % 4) + (y1 ^ (rank // 4))

    def row_dev(rank):
        return {'cp': 8 * row + row_slot(rank)}

    def col_dev(rank):
        return {'cp': 8 * col_slot(rank) + col}

    barrier = pltpu.get_barrier_semaphore()
    for r in range(1, 8):
        pl.semaphore_signal(barrier, inc=1, device_id=row_dev(r))
        pl.semaphore_signal(barrier, inc=1, device_id=col_dev(r))
    pl.semaphore_signal(barrier, inc=1, device_id={'data': 1 - core})

    wvt = wv_in[...].T
    for h in range(2):
        c = slice(h * HALF, (h + 1) * HALF)
        qt_s[col, h] = q_in[:, c]
        q = q_in[:, c].T
        q_s[col, h, :, 0:QK] = q
        qr_s[col, :, h * ROPE:(h + 1) * ROPE] = q[:, NOPE:QK]
        do_s[col, h, :, 0:VAL] = do_in[h]
    for h in range(2):
        k_s[row, h, :, 0:NOPE] = mm(c_in[h], wk_in[...]).astype(BF)
        rope = kpe_in[:, h * HALF:(h + 1) * HALF].T
        k_s[row, h, :, NOPE:QK + ROPE] = jnp.concatenate([rope, rope], axis=1)
        kr_s[row, :, h * ROPE:(h + 1) * ROPE] = rope
        vt_s[row, h, 0:VAL] = mm_t(wvt, c_in[h]).astype(BF)

    pl.semaphore_wait(barrier, 15)

    def q_copies(n, slot, dev):
        return [
            pltpu.make_async_remote_copy(q_s.at[slot, :, :, pl.ds(0, NOPE)], q_s.at[slot, :, :, pl.ds(0, NOPE)], q_send.at[0, n], q_recv.at[0, slot], device_id=dev),
            pltpu.make_async_remote_copy(qr_s.at[slot], qr_s.at[slot], q_send.at[1, n], q_recv.at[1, slot], device_id=dev),
        ]

    def k_copies(n, slot, dev):
        return [
            pltpu.make_async_remote_copy(k_s.at[slot, :, :, pl.ds(0, NOPE)], k_s.at[slot, :, :, pl.ds(0, NOPE)], k_send.at[0, n], k_recv.at[0, slot], device_id=dev),
            pltpu.make_async_remote_copy(kr_s.at[slot], kr_s.at[slot], k_send.at[1, n], k_recv.at[1, slot], device_id=dev),
            pltpu.make_async_remote_copy(vt_s.at[slot, :, pl.ds(0, VAL)], vt_s.at[slot, :, pl.ds(0, VAL)], k_send.at[2, n], k_recv.at[2, slot], device_id=dev),
        ]

    def do_copies(n, slot, dev):
        return [pltpu.make_async_remote_copy(do_s.at[slot, :, :, pl.ds(0, VAL)], do_s.at[slot, :, :, pl.ds(0, VAL)], do_send.at[n], do_recv.at[slot], device_id=dev)]

    def start(copies):
        for c in copies:
            c.start()

    for n in (3, 0, 1, 2):
        start(q_copies(n, col, row_dev(n + 1)))
        start(k_copies(n, row, col_dev(n + 1)))

    ones_row = jnp.where(lax.broadcasted_iota(jnp.int32, (AUG, HALF), 0) < 3, 1.0, 0.0).astype(BF)

    def clear(s, _):
        for h in range(2):
            ot_s[s, h] = jnp.zeros((VAL, HALF), F32)
            dq_s[s, h] = jnp.zeros((HALF, NOPE), F32)
            dk_s[s, h] = jnp.zeros((QK, HALF), F32)
            dv_s[s, h] = jnp.zeros((VAL, HALF), F32)
            m_s[s, h] = jnp.full((1, HALF), NEG_BIG, F32)
            l_s[s, h] = jnp.zeros((1, HALF), F32)
            kt_s[s, h, QK:QK + AUG] = ones_row
            vt_s[s, h, VAL:VAL + AUG] = ones_row
        dqr_s[s] = jnp.zeros((HALF, 128), F32)
        return 0

    def place_q(s):
        for h in range(2):
            q_s[s, h, :, NOPE:QK] = qr_s[s, :, h * ROPE:(h + 1) * ROPE]
            qt_s[s, h] = q_s[s, h, :, 0:QK].T

    def place_k(s):
        for h in range(2):
            rope = kr_s[s, :, h * ROPE:(h + 1) * ROPE]
            k_s[s, h, :, NOPE:QK + ROPE] = jnp.concatenate([rope, rope], axis=1)
            kt_s[s, h, 0:QK] = k_s[s, h, :, 0:QK].T

    def place_do(s):
        for h in range(2):
            dot_s[s, h] = do_s[s, h, :, 0:VAL].T

    for h in range(2):
        kt_s[row, h, 0:QK] = k_s[row, h, :, 0:QK].T
    place_do(col)
    lax.fori_loop(0, 8, clear, 0)

    def wait_q(rank):
        for c in q_copies(0, row_slot(rank), row_dev(1)):
            c.wait_recv()

    def wait_k(rank):
        for c in k_copies(0, col_slot(rank), col_dev(1)):
            c.wait_recv()

    def wait_do(rank):
        for c in do_copies(0, row_slot(rank), row_dev(1)):
            c.wait_recv()

    def two_blocks(ks, qs, second):
        if not second:
            return ks, qs, 0, 1
        h = jnp.where((ks < row) | ((ks == row) & (col <= qs)), 0, 1)
        return ks, qs, h, h

    f_rects = ((1, 0, 1, 1, 2, 0), (3, 1, 2, 0, 3, 0), (9, 0, 3, 3, 2, 1), (15, 3, 2, 0, 5, 0), (25, 0, 5, 5, 3, 1), (40, 5, 2, 0, 8, 0))

    def f_slots(t):
        a, b = 7, 0
        for t0, a0, na, b0, nb, inner in f_rects[::-1]:
            u = t - t0
            pa, pb = (a0 + u % na, b0 + u // na) if inner else (a0 + u // nb, b0 + u % nb)
            a = jnp.where(t < T_LAST if t0 == 40 else t < t_next, pa, a)
            b = jnp.where(t < T_LAST if t0 == 40 else t < t_next, pb, b)
            t_next = t0
        return col_slot(a), jnp.where(t < T_LAST, row_slot(b), t - T_LAST)

    def f_block(t, second):
        return two_blocks(*f_slots(t), second)

    def f_scores(sc, blk):
        ks, qs, kh, qh = blk
        sc[...] = mm(k_s[ks, kh, :, 0:QK], qt_s[qs, qh])

    def f_use(sc, blk, mask=False):
        ks, qs, kh, qh = blk
        s = sc[...]
        if mask:
            keys = lax.broadcasted_iota(jnp.int32, (HALF, HALF), 0)
            rows = lax.broadcasted_iota(jnp.int32, (HALF, HALF), 1)
            s = jnp.where(keys <= rows, s, NEG_BIG)
        m0 = m_s[qs, qh]
        m1 = jnp.maximum(m0, jnp.max(s, axis=0, keepdims=True))
        p = jnp.exp2((s - m1) * EXP2_SCALE)
        alpha = jnp.exp2((m0 - m1) * EXP2_SCALE)
        l_s[qs, qh] = l_s[qs, qh] * alpha + jnp.sum(p, axis=0, keepdims=True)
        m_s[qs, qh] = m1
        ot_s[qs, qh] = ot_s[qs, qh] * alpha + mm(vt_s[ks, kh, 0:VAL], p.astype(BF))

    def own_f():
        for kh, qh in ((0, 0), (0, 1), (1, 1)):
            blk = (row, col, kh, qh)
            f_scores(sc0, blk)
            f_use(sc0, blk, mask=kh == qh)

    own_f()

    def stats_copy(slot, n):
        return pltpu.make_async_remote_copy(st_s.at[slot], st_r.at[slot, col], st_send.at[slot, n - 1], st_recv.at[slot], device_id=row_dev(n))

    def make_stats(qs):
        for h in range(2):
            d = jnp.sum(ot_s[qs, h] * dot_s[qs, h].astype(F32), axis=0, keepdims=True)
            for j in range(4):
                c = slice(128 * j, 128 * j + 128)
                r = 4 * h + j
                st_s[qs, r:r + 1] = m_s[qs, h, :, c]
                st_s[qs, 8 + r:9 + r] = l_s[qs, h, :, c]
                st_s[qs, 16 + r:17 + r] = d[:, c]

    def start_stats(qs):
        for n in range(1, 8):
            stats_copy(qs, n).start()
        st_r[qs, col] = st_s[qs]

    q_steps, q_ranks = (1, 2, 9, 12, 25, 30, 35), (1, 2, 3, 4, 5, 6, 7)
    k_steps, k_ranks = (3, 6, 15, 20, 40, 48, T_LAST), (1, 2, 3, 4, 5, 6, 7)
    do_steps, do_ranks = (49, 50, 51, 52, 53, 54), (1, 2, 3, 5, 6, 7)

    def f_arrive(t):
        @pl.when(among(t, tuple(sorted(set(q_steps + k_steps + do_steps + (T_RELAY_Q, T_RELAY_K, T_OWN_DO, T_RELAY_DO))))))
        def _():
            @pl.when(among(t, q_steps))
            def _():
                rank = at(t, q_steps, q_ranks)

                @pl.when(rank != 4)
                def _():
                    wait_q(rank)
                place_q(row_slot(rank))

            @pl.when(among(t, k_steps))
            def _():
                rank = at(t, k_steps, k_ranks)

                @pl.when(rank != 4)
                def _():
                    wait_k(rank)
                place_k(col_slot(rank))

            @pl.when(among(t, do_steps))
            def _():
                rank = at(t, do_steps, do_ranks)
                wait_do(rank)
                place_do(row_slot(rank))

            @pl.when(t == T_RELAY_Q)
            def _():
                wait_q(4)
                for n in range(3):
                    start(q_copies(4 + n, row_slot(4), row_dev(n + 1)))

            @pl.when(t == T_RELAY_K)
            def _():
                wait_k(4)
                for n in range(3):
                    start(k_copies(4 + n, col_slot(4), col_dev(n + 1)))

            @pl.when(t == T_OWN_DO)
            def _():
                for n in (3, 0, 1, 2):
                    start(do_copies(n, col, row_dev(n + 1)))

            @pl.when(t == T_RELAY_DO)
            def _():
                wait_do(4)
                for n in range(3):
                    start(do_copies(4 + n, row_slot(4), row_dev(n + 1)))
                place_do(row_slot(4))

    f_arrive(1)
    f_scores(sc0, f_block(1, False))
    f_arrive(2)

    def f_step(t, _):
        nxt = jnp.minimum(t + 1, 63)
        b1, b2 = f_block(t, False), f_block(t, True)
        f_scores(sc1, b2)
        f_use(sc0, b1)
        f_scores(sc0, f_block(nxt, False))
        f_use(sc1, b2)

        @pl.when(t >= T_LAST)
        def _():
            @pl.when(t > T_LAST)
            def _():
                start_stats(t - T_LAST - 1)

            make_stats(t - T_LAST)

        f_arrive(t + 2)
        return 0

    lax.fori_loop(1, 64, f_step, 0)
    start_stats(7)

    def ring_dev(s):
        return {'cp': 8 * row + 4 * y0 + s % 4}

    def o_copies(s):
        d = (s // 4) ^ y0
        return [pltpu.make_async_remote_copy(ot_s.at[s, h], xo.at[d, x, pl.ds(h * VAL, VAL)], xo_send.at[h, s], xo_recv.at[h, d, x], device_id=ring_dev(s)) for h in range(2)]

    def dq_refs(s, rows):
        return [dq_s.at[s, 0, rows], dq_s.at[s, 1, rows], dqr_s.at[s, rows]]

    def dq_copies(rank):
        d, n = rank // 4, rank % 4 - 1
        srcs = dq_refs(row_slot(rank), pl.ds(0, HALF))
        return [pltpu.make_async_remote_copy(srcs[j], xq.at[d, n, :, pl.ds(128 * j, 128)], xq_send.at[j, rank], xq_recv.at[j, d, n], device_id=row_dev(n + 1)) for j in range(3)]

    def dq_via(d, p):
        srcs = dq_refs(row_slot(4 * d + 3), pl.ds(p * (HALF // 2), HALF // 2))
        return [pltpu.make_async_remote_copy(srcs[j], xqv.at[d, p, :, pl.ds(128 * j, 128)], xqv_send.at[j, d, p], xqv_recv.at[j, d, p], device_id=row_dev(p + 1)) for j in range(3)]

    def dkv_copies(rank):
        d, n = rank // 4, rank % 4 - 1
        s = col_slot(rank)
        out = []
        for h in range(2):
            out.append(pltpu.make_async_remote_copy(dk_s.at[s, h], zkv.at[d, n, h, pl.ds(0, QK)], zkv_send.at[0, h, rank], zkv_recv.at[0, h, d, n], device_id=col_dev(n + 1)))
            out.append(pltpu.make_async_remote_copy(dv_s.at[s, h], zkv.at[d, n, h, pl.ds(QK, VAL)], zkv_send.at[1, h, rank], zkv_recv.at[1, h, d, n], device_id=col_dev(n + 1)))
        return out

    def dkv_via(d, h):
        s = col_slot(4 * d + 3)
        return [
            pltpu.make_async_remote_copy(dk_s.at[s, h], zkvv.at[d, h, pl.ds(0, QK)], zkvv_send.at[0, d, h], zkvv_recv.at[0, d, h], device_id=col_dev(h + 1)),
            pltpu.make_async_remote_copy(dv_s.at[s, h], zkvv.at[d, h, pl.ds(QK, VAL)], zkvv_send.at[1, d, h], zkvv_recv.at[1, d, h], device_id=col_dev(h + 1)),
        ]

    def o_wait(d, r):
        s = (x + gray(r)) % 4
        for h in range(2):
            pltpu.make_async_remote_copy(ot_s.at[0, h], xo.at[d, s, pl.ds(h * VAL, VAL)], xo_send.at[h, r], xo_recv.at[h, d, s], device_id=row_dev(r)).wait_recv()

    def local(pairs):
        return [pltpu.make_async_copy(src, dst, loc.at[n]) for n, (src, dst) in enumerate(pairs)]

    def done(copies):
        for c in copies:
            c.wait()

    def rows(n, size):
        return stg.at[pl.ds(n, size)]

    pair_row = row_dev(4)
    pair_col = col_dev(4)

    def o_pair():
        s = row_slot(4)
        return [pltpu.make_async_remote_copy(ot_s.at[s, h], po.at[pl.ds(h * VAL, VAL)], p_send.at[h], p_recv.at[h], device_id=pair_row) for h in range(2)]

    def dq_pair():
        s = row_slot(4)
        srcs = dq_refs(s, pl.ds(0, HALF))
        return [pltpu.make_async_remote_copy(srcs[j], pq.at[:, pl.ds(128 * j, 128)], p_send.at[2 + j], p_recv.at[2 + j], device_id=pair_row) for j in range(3)]

    def dkv_pair():
        s = col_slot(4)
        out = []
        for h in range(2):
            out.append(pltpu.make_async_remote_copy(dk_s.at[s, h], pkv.at[h, pl.ds(0, QK)], p_send.at[5 + 2 * h], p_recv.at[5 + 2 * h], device_id=pair_col))
            out.append(pltpu.make_async_remote_copy(dv_s.at[s, h], pkv.at[h, pl.ds(QK, VAL)], p_send.at[6 + 2 * h], p_recv.at[6 + 2 * h], device_id=pair_col))
        return out

    KV = QK + VAL

    def o_local(d):
        return local([(xo.at[d, (x + gray(r)) % 4], rows(2 * VAL * (r - 1), 2 * VAL)) for r in range(1, 4)])

    def fetch_o(d):
        for r in range(1, 4):
            o_wait(d, r)
        start(o_local(d))

    def add_o(slot, d):
        done(o_local(d))
        for h in range(2):
            a, b, c = (stg[2 * VAL * n + h * VAL:2 * VAL * n + (h + 1) * VAL] for n in range(3))
            ot_s[slot, h] = ot_s[slot, h] + (a + b + c)

    def dkv_local(d):
        return local([(zkv.at[d, n, h], rows(KV * (2 * h + n), KV)) for h in range(2) for n in range(2)])

    def fetch_dkv(d):
        for c in dkv_copies(4 * d + 1) + dkv_copies(4 * d + 2):
            c.wait_recv()
        start(dkv_local(d))

    def add_dkv(slot, d):
        done(dkv_local(d))
        for h in range(2):
            a, b = KV * 2 * h, KV * (2 * h + 1)
            dk_s[slot, h] = dk_s[slot, h] + (stg[a:a + QK] + stg[b:b + QK])
            dv_s[slot, h] = dv_s[slot, h] + (stg[a + QK:a + KV] + stg[b + QK:b + KV])

    def via_local(d, h):
        return local([(zkvv.at[d, h], rows(0, KV))])

    def fetch_via(d, h):
        for c in dkv_via(d, h):
            c.wait_recv()
        start(via_local(d, h))

    def add_via(d, h):
        done(via_local(d, h))
        slot = col_slot(4 * d + 1 + h)
        dk_s[slot, h] = dk_s[slot, h] + stg[0:QK]
        dv_s[slot, h] = dv_s[slot, h] + stg[QK:KV]

    def add_dq_via(d):
        for p in range(2):
            for c in dq_via(d, p):
                c.wait_recv()
        copies = local([(xqv.at[d, p], stg.at[pl.ds(p * HALF, HALF // 2), pl.ds(0, 384)]) for p in range(2)])
        start(copies)
        done(copies)
        for p in range(2):
            slot = row_slot(4 * d + 1 + p)
            r = slice(p * (HALF // 2), (p + 1) * (HALF // 2))
            u = slice(p * HALF, p * HALF + HALF // 2)
            for j in range(2):
                dq_s[slot, j, r] = dq_s[slot, j, r] + stg[u, 128 * j:128 * j + 128]
            dqr_s[slot, r] = dqr_s[slot, r] + stg[u, 256:384]

    def dq_local(d):
        return local([(xq.at[d, n], stg.at[pl.ds(n * HALF, HALF), pl.ds(0, 384)]) for n in range(2)])

    def sum_dq(slot, d):
        for c in dq_copies(4 * d + 1) + dq_copies(4 * d + 2):
            c.wait_recv()
        start(dq_local(d))
        done(dq_local(d))
        for j in range(2):
            c = slice(128 * j, 128 * j + 128)
            dq_s[slot, j] = dq_s[slot, j] + (stg[0:HALF, c] + stg[HALF:2 * HALF, c])
        dqr_s[slot] = dqr_s[slot] + (stg[0:HALF, 256:384] + stg[HALF:2 * HALF, 256:384])

    def columns(v):
        flat = jnp.concatenate([v[j:j + 1] for j in range(4)], axis=1)
        hi = flat.astype(BF).astype(F32)
        mid = (flat - hi).astype(BF).astype(F32)
        lo = flat - hi - mid
        return jnp.concatenate([hi, mid, lo, jnp.zeros((AUG - 3, HALF), F32)], axis=0).T.astype(BF)

    def wait_stats(qs):
        pltpu.make_async_copy(st_r.at[qs, pl.ds(0, 7)], st_r.at[qs, pl.ds(0, 7)], st_recv.at[qs]).wait()

    def prepare(qs):
        wait_stats(qs)
        m = st_r[qs, :, 0:8]
        m_all = jnp.max(m, axis=0)
        w = jnp.exp2((m - m_all[None]) * EXP2_SCALE)
        l_all = jnp.sum(w * st_r[qs, :, 8:16], axis=0)
        inv = 1.0 / l_all
        delta = jnp.sum(w * st_r[qs, :, 16:24], axis=0) * inv
        lse = m_all + jnp.log2(l_all) * (1.0 / EXP2_SCALE)
        mine = jnp.exp2((st_s[qs, 0:8] - m_all) * EXP2_SCALE) * inv
        for h in range(2):
            q_s[qs, h, :, QK:QK + AUG] = columns(-lse[4 * h:4 * h + 4])
            do_s[qs, h, :, VAL:VAL + AUG] = columns(-delta[4 * h:4 * h + 4])
            for j in range(4):
                r = 4 * h + j
                c = slice(128 * j, 128 * j + 128)
                ot_s[qs, h, :, c] = ot_s[qs, h, :, c] * mine[r:r + 1]

    k_first, q_last = (7, 3, 5, 6, 4, 1, 2), (7, 5, 6, 3, 1, 2, 4)

    def b_slots(t):
        a = jnp.where(t < 56, order(t // 8, k_first), 0)
        return col_slot(a), jnp.where(t < 56, t % 8, row_slot(order(t - 56, q_last)))

    def b_block(t, second):
        return two_blocks(*b_slots(t), second)

    def b_scores(sc, dp, blk):
        ks, qs, kh, qh = blk
        sc[...] = mm(q_s[qs, qh], kt_s[ks, kh])
        dp[...] = mm(do_s[qs, qh], vt_s[ks, kh])

    def b_elem(sc, dp, pr, ds, blk, mask=False):
        p = jnp.exp2(sc[...] * EXP2_SCALE)
        if mask:
            rows = lax.broadcasted_iota(jnp.int32, (HALF, HALF), 0)
            keys = lax.broadcasted_iota(jnp.int32, (HALF, HALF), 1)
            p = jnp.where(keys <= rows, p, 0.0)
        pr[...] = p.astype(BF)
        ds[...] = (p * dp[...]).astype(BF)

    def b_grads(pr, ds, blk):
        ks, qs, kh, qh = blk
        p = pr[...]
        g = ds[...]
        dv_s[ks, kh] += mm(dot_s[qs, qh], p)
        dk_s[ks, kh] += mm(qt_s[qs, qh], g)
        dq = mm(g, k_s[ks, kh])
        dq_s[qs, qh] += dq[:, 0:NOPE]
        side = lax.broadcasted_iota(jnp.int32, (1, 128), 1) // ROPE
        dqr_s[qs] += jnp.where(side == qh, dq[:, NOPE:], 0.0)

    pr1[...] = jnp.zeros((HALF, HALF), BF)
    ds1[...] = jnp.zeros((HALF, HALF), BF)
    prepare(0)
    prepare(1)
    b_scores(sc0, dp0, b_block(0, False))

    fetch_steps, add_steps, send_steps = (24, 32, 48, 56), (25, 33, 49, 57), (26, 34, 50, 58)

    def b_events(t):
        @pl.when((t < 9) | among(t, (9, 17, T_PAIR_O - 1, T_PAIR_O, T_PAIR_O + 1, T_PAIR_KV - 1, T_PAIR_KV, T_PAIR_KV + 1, 61) + fetch_steps + add_steps + send_steps))
        def _():
            @pl.when(t < 7)
            def _():
                prepare(t + 1)

            @pl.when((t < 9) & ((t - 1) % 4 != x))
            def _():
                start(o_copies(t - 1))

            @pl.when((t == 9) | (t == 17))
            def _():
                for h in range(2):
                    start(dkv_via(jnp.where(t == 9, 1, 0), h))

            @pl.when(among(t, fetch_steps))
            def _():
                fetch_via(jnp.where(t < 40, 1, 0), jnp.where(among(t, fetch_steps[1::2]), 1, 0))

            @pl.when(among(t, add_steps))
            def _():
                add_via(jnp.where(t < 40, 1, 0), jnp.where(among(t, add_steps[1::2]), 1, 0))

            @pl.when(among(t, send_steps))
            def _():
                start(dkv_copies(at(t, send_steps, (5, 6, 1, 2))))

            @pl.when(t == 58)
            def _():
                for p in range(2):
                    start(dq_via(1, p))

            @pl.when(t == 61)
            def _():
                for p in range(2):
                    start(dq_via(0, p))

            @pl.when(t == T_PAIR_O - 1)
            def _():
                fetch_o(1)

            @pl.when(t == T_PAIR_O)
            def _():
                add_o(row_slot(4), 1)

            @pl.when(t == T_PAIR_O + 1)
            def _():
                start(o_pair())

            @pl.when(t == T_PAIR_KV - 1)
            def _():
                fetch_dkv(1)

            @pl.when(t == T_PAIR_KV)
            def _():
                add_dkv(col_slot(4), 1)

            @pl.when(t == T_PAIR_KV + 1)
            def _():
                start(dkv_pair())

    def b_step(t, _):
        b1, b2 = b_block(t, False), b_block(t, True)
        prev = b_block(jnp.maximum(t - 1, 0), True)
        nxt = b_block(jnp.minimum(t + 1, 62), False)
        b_scores(sc1, dp1, b2)
        b_elem(sc0, dp0, pr0, ds0, b1)
        b_grads(pr1, ds1, prev)
        b_scores(sc0, dp0, nxt)
        b_elem(sc1, dp1, pr1, ds1, b2)
        b_grads(pr0, ds0, b1)
        b_events(t + 1)
        return 0

    lax.fori_loop(0, 63, b_step, 0)
    b_grads(pr1, ds1, b_block(62, True))

    def own_b():
        for kh, qh in ((0, 0), (0, 1), (1, 1)):
            blk = (row, col, kh, qh)
            b_scores(sc0, dp0, blk)
            b_elem(sc0, dp0, pr0, ds0, blk, mask=kh == qh)
            b_grads(pr0, ds0, blk)

    fetch_o(0)
    own_b()

    def finish_o():
        add_o(col, 0)
        for c in o_pair():
            c.wait_recv()
        last_o = local([(po, sc0.at[pl.ds(0, 2 * VAL)])])
        start(last_o)
        for n in range(4):
            for c in do_copies(n, col, row_dev(n + 1)):
                c.wait_send()
        done(last_o)
        for h in range(2):
            do_s[col, h, :, 0:VAL] = (ot_s[col, h] + sc0[h * VAL:(h + 1) * VAL]).T.astype(BF)
        return pltpu.make_async_copy(do_s.at[col, :, :, pl.ds(0, VAL)], out_o, outs.at[0])

    o_out = finish_o()
    o_out.start()
    add_dq_via(1)
    for h in range(2):
        (pr0, pr1)[h][...] = c_in[h].T
    start(dq_copies(5))
    start(dq_copies(6))
    add_dq_via(0)
    w_all = jnp.concatenate([wk_in[...], wv_in[...]], axis=1).astype(F32)
    start(dq_copies(1))
    start(dq_copies(2))

    def finish_dkv():
        fetch_dkv(0)
        for c in dkv_pair():
            c.wait_recv()
        pairs = [pltpu.make_async_copy(pkv.at[h], (sc0, sc1)[h].at[pl.ds(0, KV)], loc.at[4 + h]) for h in range(2)]
        start(pairs)
        done(dkv_local(0))
        done(pairs)
        sums = None
        for h in range(2):
            a, b, other = KV * 2 * h, KV * (2 * h + 1), (sc0, sc1)[h]
            dk = (dk_s[row, h] + (stg[a:a + QK] + stg[b:b + QK]) + other[0:QK]) * SCALE
            dv = dv_s[row, h] + (stg[a + QK:a + KV] + stg[b + QK:b + KV]) + other[QK:KV]
            rope_s[:, h * HALF:(h + 1) * HALF] = dk[NOPE:QK]
            kv = jnp.concatenate([dk[0:NOPE].T, dv.T], axis=1)
            part = mm((pr0, pr1)[h][...].astype(F32), kv)
            sums = part if h == 0 else sums + part
            stg[2 * h * HALF:2 * h * HALF + HALF, 0:2 * NOPE] = kv
        w_s[0] = sums[:, 0:NOPE]
        w_s[1] = sums[:, NOPE:]

    finish_dkv()

    def w_copy(src, dst, n, m, dev):
        return pltpu.make_async_remote_copy(src, dst, w_send.at[n], w_recv.at[m], device_id=dev)

    mate = {'data': 1 - core}
    first = w_copy(w_s.at[1 - core], ws_r, 0, 0, mate)
    first.start()

    def finish_c():
        for h in range(2):
            (dp0, dp1)[h][...] = mm_t(stg[2 * h * HALF:2 * h * HALF + HALF, 0:2 * NOPE], w_all)

    finish_c()
    c_out = [pltpu.make_async_copy(dp0, out_c.at[0], outs.at[1]), pltpu.make_async_copy(dp1, out_c.at[1], outs.at[2])]
    r_out = [pltpu.make_async_copy(rope_s, out_r, outs.at[3])]
    start(c_out)
    start(r_out)

    def w_one():
        first.wait_recv()
        wr_s[...] = w_s[core] + ws_r[...]

    w_one()

    def along_col(r):
        s = col_slot(r)
        return pltpu.make_async_remote_copy(wr_s.at[pl.ds(64 * s, 64)], wr_r.at[row], w_send.at[r], w_recv.at[1], device_id=col_dev(r))

    for r in range(1, 8):
        along_col(r).start()
    strip = pl.ds(pl.multiple_of(64 * row, 64), 64)
    wr_r[row] = wr_s[strip]

    def finish_dq_pair():
        sum_dq(row_slot(4), 1)

    finish_dq_pair()

    def w_two():
        pltpu.make_async_copy(wr_r.at[pl.ds(0, 7)], wr_r.at[pl.ds(0, 7)], w_recv.at[1]).wait()
        wc_s[...] = jnp.sum(wr_r[...], axis=0)

    start(dq_pair())
    w_two()

    def along_row(r):
        return pltpu.make_async_remote_copy(wc_s, wc_r.at[col], w_send.at[7 + r], w_recv.at[2], device_id=row_dev(r))

    for r in range(1, 8):
        along_row(r).start()
    wc_r[col] = wc_s[...]

    def w_three():
        pltpu.make_async_copy(wc_r.at[pl.ds(0, 7)], wc_r.at[pl.ds(0, 7)], w_recv.at[2]).wait()
        w_s[core, strip] = jnp.sum(wc_r[...], axis=0)

    w_three()

    def back_col(r):
        return pltpu.make_async_remote_copy(w_s.at[core, strip], w_s.at[core, strip], w_send.at[14 + r], w_recv.at[3], device_id=col_dev(r))

    for r in range(1, 8):
        back_col(r).start()

    def finish_dq():
        for c in dq_copies(1) + dq_copies(2):
            c.wait_recv()
        for c in dq_pair():
            c.wait_recv()
        copies = local([(xq.at[0, 0], stg.at[pl.ds(0, HALF), pl.ds(0, 384)]), (xq.at[0, 1], stg.at[pl.ds(HALF, HALF), pl.ds(0, 384)]), (pq, stg.at[pl.ds(2 * HALF, HALF), pl.ds(0, 384)])])
        start(copies)
        done(copies)

        def total(mine, c):
            return (mine + (stg[0:HALF, c] + stg[HALF:2 * HALF, c]) + stg[2 * HALF:3 * HALF, c]) * SCALE

        for h in range(2):
            q_out_s[0:NOPE, h * HALF:(h + 1) * HALF] = total(dq_s[col, h], slice(128 * h, 128 * h + 128)).T
        rope = total(dqr_s[col], slice(256, 384)).T
        for h in range(2):
            q_out_s[NOPE:QK, h * HALF:(h + 1) * HALF] = rope[h * ROPE:(h + 1) * ROPE]
        return pltpu.make_async_copy(q_out_s, out_q, outs.at[5])

    def w_four():
        first.wait_send()
        pltpu.make_async_copy(wr_s.at[pl.ds(0, 448)], wr_s.at[pl.ds(0, 448)], w_recv.at[3]).wait()

    w_four()
    last = w_copy(w_s.at[core], wl_r, 22, 4, mate)
    last.start()
    q_out = finish_dq()
    q_out.start()

    def w_five():
        last.wait_recv()
        w_s[1 - core] = wl_r[...]

    w_five()
    w_out = [pltpu.make_async_copy(w_s.at[0], out_uk, outs.at[6]), pltpu.make_async_copy(w_s.at[1], out_uv, outs.at[7])]
    start(w_out)

    last.wait_send()
    for r in range(1, 8):
        along_row(r).wait_send()
        along_col(r).wait_send()
        back_col(r).wait_send()
        for s in range(8):
            stats_copy(s, r).wait_send()
        if r != 4:
            for c in o_copies(row_slot(r)):
                c.wait_send()
        if r % 4 in (1, 2):
            for c in dkv_copies(r) + dq_copies(r):
                c.wait_send()
        if r % 4 == 3:
            for h in range(2):
                for c in dkv_via(r // 4, h) + dq_via(r // 4, h):
                    c.wait_send()
    for c in o_pair() + dkv_pair() + dq_pair():
        c.wait_send()
    for n in range(4):
        for c in q_copies(n, col, row_dev(n + 1)) + k_copies(n, row, col_dev(n + 1)):
            c.wait_send()
    for n in range(3):
        for c in q_copies(4 + n, row_slot(4), row_dev(n + 1)) + k_copies(4 + n, col_slot(4), col_dev(n + 1)) + do_copies(4 + n, row_slot(4), row_dev(n + 1)):
            c.wait_send()
    for c in [o_out, q_out] + c_out + r_out + w_out:
        c.wait()


def core_call(c, kpe, q, wk, wv, do):
    vmem = pltpu.VMEM
    dma = pltpu.SemaphoreType.DMA
    n = 8
    shape = jax.ShapeDtypeStruct
    scratch = [
        vmem((n, 2, HALF, QK + AUG), BF), vmem((n, HALF, 128), BF), vmem((n, 2, HALF, QK + ROPE), BF), vmem((n, HALF, 128), BF),
        vmem((n, 2, VAL + AUG, HALF), BF), vmem((n, 2, HALF, VAL + AUG), BF),
        vmem((n, 2, QK, HALF), BF), vmem((n, 2, QK + AUG, HALF), BF), vmem((n, 2, VAL, HALF), BF),
        vmem((n, 2, VAL, HALF), F32), vmem((n, 2, 1, HALF), F32), vmem((n, 2, 1, HALF), F32),
        vmem((n, 2, HALF, NOPE), F32), vmem((n, HALF, 128), F32), vmem((n, 2, QK, HALF), F32), vmem((n, 2, VAL, HALF), F32),
        vmem((n, 24, 128), F32), vmem((n, n, 24, 128), F32), vmem((3 * HALF, HALF), F32),
        vmem((2, LATENT, 128), F32), vmem((LATENT, 128), F32), vmem((LATENT, 128), F32), vmem((ROPE, 2 * HALF), F32), vmem((QK, 2 * HALF), F32), vmem((LATENT, 128), F32), vmem((n, 64, 128), F32), vmem((64, 128), F32), vmem((n, 64, 128), F32),
        vmem((HALF, HALF), F32), vmem((HALF, HALF), F32), vmem((HALF, HALF), F32), vmem((HALF, HALF), F32),
        vmem((HALF, HALF), BF), vmem((HALF, HALF), BF), vmem((HALF, HALF), BF), vmem((HALF, HALF), BF),
        dma((2, 7)), dma((2, n)), dma((3, 7)), dma((3, n)), dma((7,)), dma((n,)), dma((n, 7)), dma((n,)),
        dma((2, n)), dma((2, 2, 4)), dma((3, n)), dma((3, 2, 2)), dma((3, 2, 2)), dma((3, 2, 2)), dma((2, 2, n)), dma((2, 2, 2, 2)), dma((2, 2, 2)), dma((2, 2, 2)), dma((9,)), dma((9,)), dma((6,)), dma((8,)),
        dma((23,)), dma((5,)),
    ]
    outs = (
        shape((2, HALF, VAL), BF), shape((QK, 2 * HALF), F32), shape((2, HALF, LATENT), F32), shape((ROPE, 2 * HALF), F32),
        shape((LATENT, NOPE), F32), shape((LATENT, VAL), F32),
        shape((2, 4, 2 * VAL, HALF), F32), shape((2, 2, HALF, 384), F32), shape((2, 2, HALF // 2, 384), F32),
        shape((2, 2, 2, QK + VAL, HALF), F32), shape((2, 2, QK + VAL, HALF), F32),
        shape((2 * VAL, HALF), F32), shape((HALF, 384), F32), shape((2, QK + VAL, HALF), F32),
    )
    return pl.pallas_call(
        core_kernel,
        out_shape=outs,
        in_specs=[pl.BlockSpec(memory_space=pltpu.VMEM)] * 6,
        out_specs=[pl.BlockSpec(memory_space=pl.ANY)] * len(outs),
        scratch_shapes=scratch,
        compiler_params=pltpu.CompilerParams(collective_id=0, has_side_effects=True, vmem_limit_bytes=67043328),
        name='core',
    )(c, kpe, q, wk, wv, do)[:6]


def solution(mesh):
    token_spec = P(('pod', 'data'), 'cp', None)
    head_spec = P(('pod', 'data'), 'cp', None, None)
    weight_spec = P(None, None, None)
    sum_spec = P('pod', None, None)

    def per_device(c_latent, k_rope, queries, w_uk, w_uv, d_out):
        halves = lambda a, width: a.reshape(2, HALF, width)
        o, gq, gc, gr, guk, guv = core_call(halves(c_latent, LATENT), k_rope[0].T, queries[0, :, 0].T, w_uk[:, 0], w_uv[:, 0], halves(d_out, VAL))
        return (o.reshape(1, 2 * HALF, 1, VAL), gq.T.reshape(1, 2 * HALF, 1, QK), gc.reshape(1, 2 * HALF, LATENT),
                gr.T.reshape(1, 2 * HALF, ROPE), guk[:, None], guv[:, None])

    return jax.shard_map(per_device, mesh=mesh, in_specs=(token_spec, token_spec, head_spec, weight_spec, weight_spec, head_spec), out_specs=(head_spec, head_spec, token_spec, token_spec, sum_spec, sum_spec), check_vma=False)
```

```python
import jax
import jax.numpy as jnp
from jax import lax
from jax.experimental import pallas as pl
from jax.experimental.pallas import tpu as pltpu
from jax.sharding import PartitionSpec as P

BF = jnp.bfloat16
F32 = jnp.float32
NEG_BIG = -1.0e30
HALF = 512
LATENT = 512
LANES = 128
NOPE = 128
ROPE = 64
QK = NOPE + ROPE
VAL = 128
KV = QK + VAL
AUG = 16
SCALE = QK ** -0.5
EXP2_SCALE = SCALE * 1.4426950408889634
TWO = 2
RING = 4
FAR = RING - 1
GROUP = 8
HALVES = range(TWO)
NEIGHBOURS = (1, 2)
PEERS = range(1, GROUP)
CHIPS = GROUP * GROUP
STRIP = LATENT // CHIPS
ROWS = HALF // TWO
BLOCKS = HALF // LANES
Q_STEPS = (1, 2, 9, 12, 25, 30, 35)
K_STEPS = (3, 6, 15, 20, 40, 48, 56)
DO_STEPS, DO_RANKS = (49, 50, 51, 52, 53, 54), (1, 2, 3, 5, 6, 7)
T_RELAY, T_OWN_DO, T_RELAY_DO = 9, 12, 34
T_LAST = 56
T_END = 64
RECTS = ((1, 0, 1, 1, 2, False), (3, 1, 2, 0, 3, False), (9, 0, 3, 3, 2, True), (15, 3, 2, 0, 5, False), (25, 0, 5, 5, 3, True), (40, 5, 2, 0, 8, False))
K_ORDER = (7, 3, 5, 6, 4, 1, 2)
Q_ORDER = (7, 5, 6, 3, 1, 2, 4)
T_SPLIT, T_OWN = 48, 56
T_VIA = (9, 17)
T_FETCH, T_ADD = (21, 31), (22, 32)
T_NEAR, NEAR = (25, 33, 49), (5, 6, 1)
T_NEAR_MID, T_NEAR_LAST = 53, 57
T_PAIR_O = 38
T_PAIR_KV = (46, 54)
T_VIA_Q, T_Q_FIVE, T_Q_SIX = 58, 59, 60


def mm(a, b):
    return jnp.dot(a, b, preferred_element_type=F32)


def mm_t(a, b):
    return lax.dot_general(a, b, (((1,), (1,)), ((), ())), preferred_element_type=F32)


def gray(r):
    return r ^ (r >> 1)


def part(n, size):
    return slice(n * size, (n + 1) * size)


def rows_of(n, size):
    return pl.ds(pl.multiple_of(n * size, size), size)


def order(n, ranks):
    out = ranks[-1]
    for i, r in list(enumerate(ranks))[-2::-1]:
        out = jnp.where(n <= i, r, out)
    return out


def among(t, steps):
    out = t == steps[0]
    for v in steps[1:]:
        out = out | (t == v)
    return out


def at(t, steps, ranks):
    out = ranks[-1]
    for v, r in list(zip(steps, ranks))[-2::-1]:
        out = jnp.where(t <= v, r, out)
    return out


def start(copies):
    for c in copies:
        c.start()


def done(copies):
    for c in copies:
        c.wait()


def landed(copies):
    for c in copies:
        c.wait_recv()


def left(copies):
    for c in copies:
        c.wait_send()


def remote(pairs, send, recv, dev):
    return [pltpu.make_async_remote_copy(src, dst, send.at[n], recv.at[n], device_id=dev) for n, (src, dst) in enumerate(pairs)]


def ring_sums(slot, dev, srcs, dsts, bufs, sems):
    main, via, pair = bufs
    main_send, main_recv, via_send, via_recv, pair_send, pair_recv = sems

    def near(rank, p):
        d, n = rank // RING, rank % RING - 1
        return remote(zip(srcs(slot(rank), p), dsts(main.at[d, n, p])), main_send.at[rank, p], main_recv.at[d, n, p], dev(n + 1))

    def far(d, p):
        return remote(zip(srcs(slot(RING * d + FAR), p), dsts(via.at[d, p])), via_send.at[d, p], via_recv.at[d, p], dev(p + 1))

    def across(p):
        return remote(zip(srcs(slot(RING), p), dsts(pair.at[p])), pair_send.at[p], pair_recv.at[p], dev(RING))

    return near, far, across


def core_kernel(c_in, kpe_in, q_in, wk_in, wv_in, do_in,
                out_o, out_q, out_c, out_r, out_uk, out_uv, xo, po, xq, xqv, pq, zkv, zkvv, pkv,
                q_s, qr_s, k_s, kr_s, vt_s, do_s, qt_s, kt_s, dot_s,
                ot_s, m_s, l_s, dq_s, dqr_s, dk_s, dv_s, st_s, st_r, stg, w_s, ws_r, wl_r, rope_s, q_out_s, wr_s, wr_r,
                sc0, sc1, dp0, dp1, pr0, pr1, ds0, ds1,
                q_send, q_recv, k_send, k_recv, do_send, do_recv, st_send, st_recv, xo_send, xo_recv, po_send, po_recv,
                q_sums_sems, kv_sums_sems, loc, outs, w_send, w_recv, strip_send, strip_recv):
    me = lax.axis_index('cp')
    core = lax.axis_index('data')
    row, col = me // GROUP, me % GROUP
    x, y0 = col % RING, col // RING
    y1, z = row % TWO, row // TWO

    def row_slot(rank):
        return RING * (y0 ^ (rank // RING)) + (x + gray(rank % RING)) % RING

    def col_slot(rank):
        return TWO * ((z + gray(rank % RING)) % RING) + (y1 ^ (rank // RING))

    def row_dev(rank):
        return {'cp': GROUP * row + row_slot(rank)}

    def col_dev(rank):
        return {'cp': GROUP * col_slot(rank) + col}

    mate = {'data': 1 - core}
    barrier = pltpu.get_barrier_semaphore()

    def to_others(act):
        def one(n, carry):
            act((me + n) % CHIPS)
            return carry

        lax.fori_loop(1, CHIPS, one, 0)

    to_others(lambda d: pl.semaphore_signal(barrier, inc=1, device_id={'cp': d}))
    pl.semaphore_signal(barrier, inc=1, device_id=mate)

    wvt = wv_in[:].T
    for h in HALVES:
        q = q_in[:, part(h, HALF)]
        qt_s[col, h] = q
        q_s[col, h, :, :QK] = q.T
        qr_s[col, :, part(h, ROPE)] = q[NOPE:].T
        do_s[col, h, :, :VAL] = do_in[h]
    for h in HALVES:
        k_s[row, h, :, :NOPE] = mm(c_in[h], wk_in[:]).astype(BF)
        rope = kpe_in[:, part(h, HALF)].T
        k_s[row, h, :, NOPE:] = jnp.concatenate([rope, rope], axis=1)
        kr_s[row, :, part(h, ROPE)] = rope
        vt_s[row, h, :VAL] = mm_t(wvt, c_in[h]).astype(BF)

    pl.semaphore_wait(barrier, CHIPS)

    def q_copies(n, slot, dev):
        refs = [q_s.at[slot, :, :, :NOPE], qr_s.at[slot]]
        return remote(zip(refs, refs), q_send.at[n], q_recv.at[slot], dev)

    def k_copies(n, slot, dev):
        refs = [k_s.at[slot, :, :, :NOPE], kr_s.at[slot], vt_s.at[slot, :, :VAL]]
        return remote(zip(refs, refs), k_send.at[n], k_recv.at[slot], dev)

    def do_copies(n, slot, dev):
        ref = do_s.at[slot, :, :, :VAL]
        return remote([(ref, ref)], do_send.at[n], do_recv.at[slot], dev)

    first_copies = (FAR, *range(FAR))

    def own_copies(copies, slot, dev, n):
        return copies(n, slot(0), dev(n + 1))

    def pair_copies(copies, slot, dev, n):
        return copies(RING + n, slot(RING), dev(n + 1))

    q_kind, k_kind, do_kind = (q_copies, row_slot, row_dev), (k_copies, col_slot, col_dev), (do_copies, row_slot, row_dev)

    for n in first_copies:
        start(own_copies(*q_kind, n))
        start(own_copies(*k_kind, n))

    def arrived(copies, slot, dev, rank):
        landed(copies(0, slot(rank), dev(1)))

    def wait_q(rank):
        arrived(*q_kind, rank)

    def wait_k(rank):
        arrived(*k_kind, rank)

    def wait_do(rank):
        arrived(*do_kind, rank)

    ones = jnp.where(lax.broadcasted_iota(jnp.int32, (AUG, HALF), 0) < 3, 1.0, 0.0).astype(BF)

    def clear(s, carry):
        for h in HALVES:
            for ref in (ot_s, dq_s, dk_s, dv_s, l_s):
                ref[s, h] = jnp.zeros(ref.shape[TWO:], F32)
            m_s[s, h] = jnp.full(m_s.shape[TWO:], NEG_BIG, F32)
            kt_s[s, h, QK:] = ones
            vt_s[s, h, VAL:] = ones
        dqr_s[s] = jnp.zeros((HALF, LANES), F32)
        return carry

    def place_q(s):
        for h in HALVES:
            q_s[s, h, :, NOPE:QK] = qr_s[s, :, part(h, ROPE)]
            qt_s[s, h] = q_s[s, h, :, :QK].T

    def place_k(s):
        for h in HALVES:
            rope = kr_s[s, :, part(h, ROPE)]
            k_s[s, h, :, NOPE:] = jnp.concatenate([rope, rope], axis=1)
            kt_s[s, h, :QK] = k_s[s, h, :, :QK].T

    def place_do(s):
        for h in HALVES:
            dot_s[s, h] = do_s[s, h, :, :VAL].T

    for h in HALVES:
        kt_s[row, h, :QK] = k_s[row, h, :, :QK].T
    place_do(col)
    lax.fori_loop(0, GROUP, clear, 0)

    def diagonal_half(ks, qs):
        return jnp.where((ks < row) | ((ks == row) & (col <= qs)), 0, 1)

    def two_blocks(ks, qs):
        h = diagonal_half(ks, qs)
        return (ks, qs, 0, 1), (ks, qs, h, h)

    own_blocks = [(row, col, kh, qh) for kh in HALVES for qh in HALVES if kh <= qh]

    def f_blocks(t):
        a, b = GROUP - 1, 0
        end = T_LAST
        for t0, a0, na, b0, nb, inner in RECTS[::-1]:
            u = t - t0
            pa, pb = (a0 + u % na, b0 + u // na) if inner else (a0 + u // nb, b0 + u % nb)
            a, b = jnp.where(t < end, pa, a), jnp.where(t < end, pb, b)
            end = t0
        return two_blocks(col_slot(a), jnp.where(t < T_LAST, row_slot(b), t - T_LAST))

    def f_scores(sc, blk):
        ks, qs, kh, qh = blk
        sc[:] = mm(k_s[ks, kh, :, :QK], qt_s[qs, qh])

    def f_use(sc, blk):
        ks, qs, kh, qh = blk
        s = sc[:]
        if isinstance(kh, int) and kh == qh:
            keys = lax.broadcasted_iota(jnp.int32, s.shape, 0)
            s = jnp.where(keys <= lax.broadcasted_iota(jnp.int32, s.shape, 1), s, NEG_BIG)
        m0 = m_s[qs, qh]
        m1 = jnp.maximum(m0, jnp.max(s, axis=0, keepdims=True))
        p = jnp.exp2((s - m1) * EXP2_SCALE)
        alpha = jnp.exp2((m0 - m1) * EXP2_SCALE)
        l_s[qs, qh] = l_s[qs, qh] * alpha + jnp.sum(p, axis=0, keepdims=True)
        m_s[qs, qh] = m1
        ot_s[qs, qh] = ot_s[qs, qh] * alpha + mm(vt_s[ks, kh, :VAL], p.astype(BF))

    def own_f():
        for blk in own_blocks:
            f_scores(sc0, blk)
            f_use(sc0, blk)

    own_f()

    def stats_copies(slot, n):
        return remote([(st_s.at[slot], st_r.at[slot, col])], st_send.at[slot, pl.ds(n - 1, 1)], st_recv.at[pl.ds(slot, 1)], row_dev(n))

    def make_stats(qs):
        for h in HALVES:
            d = jnp.sum(ot_s[qs, h] * dot_s[qs, h].astype(F32), axis=0, keepdims=True)
            for j in range(BLOCKS):
                c = part(j, LANES)
                for i, v in enumerate((m_s[qs, h, :, c], l_s[qs, h, :, c], d[:, c])):
                    st_s[qs, part(GROUP * i + BLOCKS * h + j, 1)] = v

    def start_stats(qs):
        for n in PEERS:
            start(stats_copies(qs, n))
        st_r[qs, col] = st_s[qs]

    def f_arrive(t):
        @pl.when(among(t, tuple(sorted({*Q_STEPS, *K_STEPS, *DO_STEPS, T_RELAY, T_OWN_DO, T_RELAY_DO}))))
        def _():
            @pl.when(among(t, Q_STEPS))
            def _():
                rank = at(t, Q_STEPS, PEERS)

                @pl.when(rank != RING)
                def _():
                    wait_q(rank)
                place_q(row_slot(rank))

            @pl.when(among(t, K_STEPS))
            def _():
                rank = at(t, K_STEPS, PEERS)

                @pl.when(rank != RING)
                def _():
                    wait_k(rank)
                place_k(col_slot(rank))

            @pl.when(among(t, DO_STEPS))
            def _():
                rank = at(t, DO_STEPS, DO_RANKS)
                wait_do(rank)
                place_do(row_slot(rank))

            @pl.when(t == T_RELAY)
            def _():
                wait_q(RING)
                for n in range(FAR):
                    start(pair_copies(*q_kind, n))
                wait_k(RING)
                for n in range(FAR):
                    start(pair_copies(*k_kind, n))

            @pl.when(t == T_OWN_DO)
            def _():
                for n in first_copies:
                    start(own_copies(*do_kind, n))

            @pl.when(t == T_RELAY_DO)
            def _():
                wait_do(RING)
                for n in range(FAR):
                    start(pair_copies(*do_kind, n))
                place_do(row_slot(RING))

    for t in NEIGHBOURS:
        f_arrive(t)
    for sc, blk in zip((sc0, sc1), f_blocks(1)):
        f_scores(sc, blk)

    def f_half(t, used, made):
        b1, b2 = f_blocks(t)
        n1, n2 = f_blocks(jnp.minimum(t + 1, T_END - 1))
        f_scores(made[0], n1)
        f_use(used[0], b1)
        f_scores(made[1], n2)
        f_use(used[1], b2)

        @pl.when(t >= T_LAST)
        def _():
            @pl.when(t > T_LAST)
            def _():
                start_stats(t - T_LAST - 1)

            make_stats(t - T_LAST)

        f_arrive(t + TWO)

    def f_step(u, carry):
        t = TWO * u + 1
        f_half(t, (sc0, sc1), (dp0, dp1))

        @pl.when(t < T_END - 1)
        def _():
            f_half(t + 1, (dp0, dp1), (sc0, sc1))
        return carry

    lax.fori_loop(0, T_END // TWO, f_step, 0)
    start_stats(GROUP - 1)

    def o_refs(slot, buf):
        return [(ot_s.at[slot, h], buf.at[pl.ds(h * VAL, VAL)]) for h in HALVES]

    def o_copies(s):
        d = (s // RING) ^ y0
        return remote(o_refs(s, xo.at[d, x]), xo_send.at[s], xo_recv.at[d, x], {'cp': GROUP * row + RING * y0 + s % RING})

    def o_pair():
        return remote(o_refs(row_slot(RING), po), po_send, po_recv, row_dev(RING))

    def dq_srcs(s, p):
        r = pl.ds(p * ROWS, ROWS)
        return [dq_s.at[s, 0, r], dq_s.at[s, 1, r], dqr_s.at[s, r]]

    def dq_dsts(buf):
        return [buf.at[:, pl.ds(LANES * j, LANES)] for j in range(3)]

    def kv_srcs(s, h):
        return [dk_s.at[s, h], dv_s.at[s, h]]

    def kv_dsts(buf):
        return [buf.at[pl.ds(0, QK)], buf.at[pl.ds(QK, VAL)]]

    dq_near, dq_far, dq_across = ring_sums(row_slot, row_dev, dq_srcs, dq_dsts, (xq, xqv, pq), q_sums_sems)
    kv_near, kv_far, kv_across = ring_sums(col_slot, col_dev, kv_srcs, kv_dsts, (zkv, zkvv, pkv), kv_sums_sems)

    def local(pairs, n=0):
        return [pltpu.make_async_copy(src, dst, loc.at[n + i]) for i, (src, dst) in enumerate(pairs)]

    def o_local(d):
        return local([(xo.at[d, (x + gray(r)) % RING], stg.at[pl.ds(HALF * (r - 1), HALF // TWO)]) for r in range(1, RING)])

    def fetch_o(d):
        for r in range(1, RING):
            s = (x + gray(r)) % RING
            landed(remote(o_refs(0, xo.at[d, s]), xo_send.at[r], xo_recv.at[d, s], row_dev(r)))
        start(o_local(d))

    def add_o(slot, d):
        done(o_local(d))
        for h in HALVES:
            ot_s[slot, h] = ot_s[slot, h] + sum(stg[HALF * n + h * VAL:HALF * n + (h + 1) * VAL] for n in range(FAR))

    def kv_local(d, h):
        return local([(zkv.at[d, n, h], stg.at[pl.ds(KV * n, KV)]) for n in HALVES])

    def fetch_kv(d, h):
        for r in NEIGHBOURS:
            landed(kv_near(RING * d + r, h))
        start(kv_local(d, h))

    def add_kv(slot, d, h):
        done(kv_local(d, h))
        dk_s[slot, h] = dk_s[slot, h] + (stg[:QK] + stg[KV:KV + QK])
        dv_s[slot, h] = dv_s[slot, h] + (stg[QK:KV] + stg[KV + QK:KV + KV])

    def kv_via_local(d):
        return local([(zkvv.at[d, h], stg.at[pl.ds(KV * h, KV)]) for h in HALVES])

    def fetch_kv_via(d):
        for h in HALVES:
            landed(kv_far(d, h))
        start(kv_via_local(d))

    def add_kv_via(d):
        done(kv_via_local(d))
        for h in HALVES:
            slot, u = col_slot(RING * d + 1 + h), KV * h
            dk_s[slot, h] = dk_s[slot, h] + stg[u:u + QK]
            dv_s[slot, h] = dv_s[slot, h] + stg[u + QK:u + KV]

    def dq_stage(n, p):
        return stg.at[pl.ds(HALF * n + ROWS * p, ROWS), pl.ds(0, 3 * LANES)]

    def add_dq(slot, p, ns):
        r = part(p, ROWS)
        for j in range(3):
            c = part(j, LANES)
            total = sum(stg[HALF * n + ROWS * p:HALF * n + ROWS * (p + 1), c] for n in ns)
            if j < TWO:
                dq_s[slot, j, r] = dq_s[slot, j, r] + total
            else:
                dqr_s[slot, r] = dqr_s[slot, r] + total

    def sum_dq_via(d):
        for p in HALVES:
            landed(dq_far(d, p))
        copies = local([(xqv.at[d, p], dq_stage(0, p)) for p in HALVES])
        start(copies)
        done(copies)
        for p in HALVES:
            add_dq(row_slot(RING * d + 1 + p), p, (0,))

    def dq_arrived(d):
        for p in HALVES:
            for r in NEIGHBOURS:
                landed(dq_near(RING * d + r, p))
        return [(xq.at[d, n, p], dq_stage(n, p)) for n in HALVES for p in HALVES]

    def columns(v):
        flat = jnp.concatenate([v[part(j, 1)] for j in range(BLOCKS)], axis=1)
        hi = flat.astype(BF).astype(F32)
        mid = (flat - hi).astype(BF).astype(F32)
        return jnp.concatenate([hi, mid, flat - hi - mid, jnp.zeros((AUG - 3, HALF), F32)], axis=0).T.astype(BF)

    def wait_stats(qs):
        others = st_r.at[qs, pl.ds(0, len(PEERS))]
        pltpu.make_async_copy(others, others, st_recv.at[qs]).wait()

    def prepare(qs):
        wait_stats(qs)
        m, l, d = (st_r[qs, :, part(i, GROUP)] for i in range(3))
        m_all = jnp.max(m, axis=0)
        w = jnp.exp2((m - m_all[None]) * EXP2_SCALE)
        l_all = jnp.sum(w * l, axis=0)
        inv = 1.0 / l_all
        delta = jnp.sum(w * d, axis=0) * inv
        lse = m_all + jnp.log2(l_all) * (1.0 / EXP2_SCALE)
        mine = jnp.exp2((st_s[qs, :GROUP] - m_all) * EXP2_SCALE) * inv
        for h in HALVES:
            q_s[qs, h, :, QK:] = columns(-lse[part(h, BLOCKS)])
            do_s[qs, h, :, VAL:] = columns(-delta[part(h, BLOCKS)])
            for j in range(BLOCKS):
                c = part(j, LANES)
                ot_s[qs, h, :, c] = ot_s[qs, h, :, c] * mine[part(BLOCKS * h + j, 1)]

    def b_blocks(t):
        ks = col_slot(jnp.where(t < T_OWN, order(t // GROUP, K_ORDER), 0))
        qs = jnp.where(t < T_OWN, t % GROUP, row_slot(order(t - T_OWN, Q_ORDER)))
        b1, b2 = two_blocks(ks, qs)
        split = (t >= T_SPLIT) & (t < T_OWN)
        u = t - T_SPLIT
        late = u >= RING
        s = TWO * (u % RING)
        h = diagonal_half(ks, 0)
        kh, qh = jnp.where(late, h, 0), jnp.where(late, h, 1)
        pick = lambda a, b: tuple(jnp.where(split, i, j) for i, j in zip(a, b))
        return pick((ks, s, kh, qh), b1), pick((ks, s + 1, kh, qh), b2)

    def b_scores(sc, dp, blk):
        ks, qs, kh, qh = blk
        sc[:] = mm(q_s[qs, qh], kt_s[ks, kh])
        dp[:] = mm(do_s[qs, qh], vt_s[ks, kh])

    def b_elem(sc, dp, pr, ds, mask=False):
        p = jnp.exp2(sc[:] * EXP2_SCALE)
        if mask:
            rows = lax.broadcasted_iota(jnp.int32, p.shape, 0)
            p = jnp.where(lax.broadcasted_iota(jnp.int32, p.shape, 1) <= rows, p, 0.0)
        pr[:] = p.astype(BF)
        ds[:] = (p * dp[:]).astype(BF)

    def b_grads(pr, ds, blk):
        ks, qs, kh, qh = blk
        p = pr[:]
        g = ds[:]
        dv_s[ks, kh] += mm(dot_s[qs, qh], p)
        dk_s[ks, kh] += mm(qt_s[qs, qh], g)
        dq = mm(g, k_s[ks, kh])
        dq_s[qs, qh] += dq[:, :NOPE]
        side = lax.broadcasted_iota(jnp.int32, (1, LANES), 1) // ROPE
        dqr_s[qs] += jnp.where(side == qh, dq[:, NOPE:], 0.0)

    early_half = 1 - diagonal_half(col_slot(K_ORDER[-1]), 0)

    def b_events(t):
        @pl.when((t <= GROUP) | among(t, (*T_VIA, *T_FETCH, *T_ADD, *T_NEAR, T_NEAR_MID, T_NEAR_LAST, T_PAIR_O - 1, T_PAIR_O, T_PAIR_O + 1, T_VIA_Q, T_Q_FIVE, T_Q_SIX)) | among(t, tuple(v + i for v in T_PAIR_KV for i in range(3))))
        def _():
            @pl.when((t < GROUP - 1) & (t % TWO == 1))
            def _():
                for n in NEIGHBOURS:
                    prepare(t + n)

            @pl.when((t <= GROUP) & ((t - 1) % RING != x))
            def _():
                start(o_copies(t - 1))

            @pl.when(among(t, T_VIA))
            def _():
                for h in HALVES:
                    start(kv_far(at(t, T_VIA, (1, 0)), h))

            @pl.when(among(t, T_FETCH))
            def _():
                fetch_kv_via(at(t, T_FETCH, (1, 0)))

            @pl.when(among(t, T_ADD))
            def _():
                add_kv_via(at(t, T_ADD, (1, 0)))

            @pl.when(among(t, T_NEAR))
            def _():
                for h in HALVES:
                    start(kv_near(at(t, T_NEAR, NEAR), h))

            @pl.when(t == T_NEAR_MID)
            def _():
                start(kv_near(K_ORDER[-1], early_half))

            @pl.when(t == T_NEAR_LAST)
            def _():
                start(kv_near(K_ORDER[-1], 1 - early_half))

            @pl.when(t == T_VIA_Q)
            def _():
                for p in HALVES:
                    start(dq_far(1, p))

            @pl.when(t == T_Q_FIVE)
            def _():
                start(dq_near(5, 1))

            @pl.when(t == T_Q_SIX)
            def _():
                start(dq_near(6, 0))

            @pl.when(t == T_PAIR_O - 1)
            def _():
                fetch_o(1)

            @pl.when(t == T_PAIR_O)
            def _():
                add_o(row_slot(RING), 1)

            @pl.when(t == T_PAIR_O + 1)
            def _():
                start(o_pair())

            for h, v in enumerate(T_PAIR_KV):
                @pl.when(t == v)
                def _():
                    fetch_kv(1, h)

                @pl.when(t == v + 1)
                def _():
                    add_kv(col_slot(RING), 1, h)

                @pl.when(t == v + TWO)
                def _():
                    start(kv_across(h))

    def b_step(t, carry):
        b1, b2 = b_blocks(t)
        b_scores(sc1, dp1, b2)
        b_elem(sc0, dp0, pr0, ds0)
        b_grads(pr1, ds1, b_blocks(jnp.maximum(t - 1, 0))[1])
        b_scores(sc0, dp0, b_blocks(jnp.minimum(t + 1, T_END - TWO))[0])
        b_elem(sc1, dp1, pr1, ds1)
        b_grads(pr0, ds0, b1)
        b_events(t + 1)
        return carry

    for ref in (pr1, ds1):
        ref[:] = jnp.zeros(ref.shape, BF)
    for s in HALVES:
        prepare(s)
    b_scores(sc0, dp0, b_blocks(0)[0])
    lax.fori_loop(0, T_END - 1, b_step, 0)
    b_grads(pr1, ds1, b_blocks(T_END - TWO)[1])

    def own_b():
        for blk in own_blocks:
            b_scores(sc0, dp0, blk)
            b_elem(sc0, dp0, pr0, ds0, mask=blk[TWO] == blk[3])
            b_grads(pr0, ds0, blk)

    fetch_o(0)
    own_b()

    def finish_o():
        add_o(col, 0)
        landed(o_pair())
        last_o = local([(po, sc0.at[pl.ds(0, HALF // TWO)])])
        start(last_o)
        for n in range(RING):
            left(own_copies(*do_kind, n))
        done(last_o)
        for h in HALVES:
            do_s[col, h, :, :VAL] = (ot_s[col, h] + sc0[part(h, VAL)]).T.astype(BF)

    finish_o()
    sum_dq_via(1)
    for pr, h in zip((pr0, pr1), HALVES):
        pr[:] = c_in[h].T
    start(dq_near(5, 0) + dq_near(6, 1))
    finals = [pltpu.make_async_copy(do_s.at[col, :, :, :VAL], out_o, outs.at[0])]
    start(finals)

    def finish_dkv():
        sums = None
        for h in HALVES:
            fetch_kv(0, h)
            landed(kv_across(h))
            pair = local([(pkv.at[h], sc0.at[pl.ds(0, KV)])], TWO)
            start(pair)
            add_kv(row, 0, h)
            done(pair)
            dk = (dk_s[row, h] + sc0[:QK]) * SCALE
            dv = dv_s[row, h] + sc0[QK:KV]
            rope_s[:, part(h, HALF)] = dk[NOPE:]
            kv = jnp.concatenate([dk[:NOPE].T, dv.T], axis=1)
            (dp0, dp1)[h][:, :NOPE + VAL] = kv
            product = mm((pr0, pr1)[h][:].astype(F32), kv)
            sums = product if sums is None else sums + product
        w_s[0] = sums[:, :NOPE]
        w_s[1] = sums[:, NOPE:]

    finish_dkv()

    def w_swap(src, dst, n):
        return remote([(src, dst)], w_send.at[pl.ds(n, 1)], w_recv.at[pl.ds(n, 1)], mate)

    def strip(d):
        return rows_of(d, STRIP)

    def to_all(n, src, dst):
        to_others(lambda d: pltpu.make_async_remote_copy(src(d), dst, strip_send.at[n], strip_recv.at[n], device_id={'cp': d}).start())

    def all_of(sem, n):
        strips = wr_r.at[pl.ds(0, CHIPS - 1)]
        pltpu.make_async_copy(strips, strips, sem.at[n]).wait()

    first = w_swap(w_s.at[1 - core], ws_r, 0)
    start(first + dq_far(0, 0) + dq_far(0, 1))

    def finish_dq_pair():
        copies = local(dq_arrived(1))
        start(copies)
        done(copies)
        for p in HALVES:
            add_dq(row_slot(RING), p, HALVES)

    finish_dq_pair()

    def finish_c():
        w_all = jnp.concatenate([wk_in[:], wv_in[:]], axis=1).astype(F32)
        for kv, out in ((dp0, sc0), (dp1, sc1)):
            out[:] = mm_t(kv[:, :NOPE + VAL], w_all)

    finish_c()
    outputs = [(sc0, out_c.at[0]), (sc1, out_c.at[1]), (rope_s, out_r)]
    more = [pltpu.make_async_copy(src, dst, outs.at[1 + n]) for n, (src, dst) in enumerate(outputs)]
    start(more)
    finals += more


    def w_one():
        landed(first)
        wr_s[:] = w_s[core] + ws_r[:]

    w_one()
    to_all(0, lambda d: wr_s.at[strip(d)], wr_r.at[me])
    start(dq_across(0) + dq_near(1, 1) + dq_near(2, 0))
    wr_r[me] = wr_s[strip(me)]
    sum_dq_via(0)
    left(first)

    def w_two():
        all_of(strip_recv, 0)
        w_s[core, strip(me)] = jnp.sum(wr_r[:], axis=0)

    w_two()
    mine = w_s.at[core, strip(me)]
    to_all(1, lambda d: mine, mine)
    start(dq_across(1) + dq_near(1, 0) + dq_near(2, 1))

    def w_three():
        all_of(strip_recv, 1)

    w_three()
    last = w_swap(w_s.at[core], wl_r, 1)
    start(last)

    def finish_dq():
        pairs = dq_arrived(0)
        for p in HALVES:
            landed(dq_across(p))
        copies = local(pairs + [(pq.at[p], dq_stage(TWO, p)) for p in HALVES])
        start(copies)
        done(copies)
        for p in HALVES:
            add_dq(col, p, range(3))
        for h in HALVES:
            q_out_s[:NOPE, part(h, HALF)] = (dq_s[col, h] * SCALE).T
        rope = (dqr_s[col] * SCALE).T
        for h in HALVES:
            q_out_s[NOPE:, part(h, HALF)] = rope[part(h, ROPE)]

    def w_five():
        landed(last)
        w_s[1 - core] = wl_r[:]

    w_five()
    more = [pltpu.make_async_copy(src, dst, outs.at[RING + n]) for n, (src, dst) in enumerate([(w_s.at[0], out_uk), (w_s.at[1], out_uv)])]
    start(more)
    finals += more
    finish_dq()
    q_out = pltpu.make_async_copy(q_out_s, out_q, outs.at[RING + TWO])
    q_out.start()

    left(last)
    for n in HALVES:
        all_of(strip_send, n)
    for r in PEERS:
        for s in range(GROUP):
            left(stats_copies(s, r))
        if r != RING:
            left(o_copies(row_slot(r)))
        if r % RING in NEIGHBOURS:
            for p in HALVES:
                left(dq_near(r, p) + kv_near(r, p))
    for p in HALVES:
        left(dq_across(p) + kv_across(p))
        for d in HALVES:
            left(dq_far(d, p) + kv_far(d, p))
    left(o_pair())
    for n in range(RING):
        left(own_copies(*q_kind, n) + own_copies(*k_kind, n))
    for n in range(FAR):
        left(pair_copies(*q_kind, n) + pair_copies(*k_kind, n) + pair_copies(*do_kind, n))
    done(finals + [q_out])


def core_call(c, kpe, q, wk, wv, do):
    dma = lambda *s: pltpu.SemaphoreType.DMA(s)
    shape = jax.ShapeDtypeStruct
    per = (GROUP, TWO)
    wide = lambda *s: pltpu.VMEM(per + s, BF)
    sums = lambda *s: pltpu.VMEM(per + s, F32)
    f32 = lambda *s: pltpu.VMEM(s, F32)
    packed = pltpu.VMEM((GROUP, HALF, LANES), BF)

    def sum_sems(n):
        return (dma(GROUP, TWO, n), dma(TWO, TWO, TWO, n), dma(TWO, TWO, n), dma(TWO, TWO, n), dma(TWO, n), dma(TWO, n))

    def sum_bufs(*s):
        return [shape((TWO, TWO, TWO, *s), F32), shape((TWO, TWO, *s), F32), shape((TWO, *s), F32)]

    square = (HALF, HALF)
    scratch = [
        wide(HALF, QK + AUG), packed, wide(HALF, QK + ROPE), packed, wide(VAL + AUG, HALF), wide(HALF, VAL + AUG),
        wide(QK, HALF), wide(QK + AUG, HALF), wide(VAL, HALF),
        sums(VAL, HALF), sums(1, HALF), sums(1, HALF),
        sums(HALF, NOPE), f32(GROUP, HALF, LANES), sums(QK, HALF), sums(VAL, HALF),
        f32(GROUP, 3 * GROUP, LANES), f32(GROUP, GROUP, 3 * GROUP, LANES), f32(3 * HALF, HALF),
        f32(TWO, LATENT, NOPE), f32(LATENT, NOPE), f32(LATENT, NOPE), f32(ROPE, TWO * HALF), f32(QK, TWO * HALF),
        f32(LATENT, NOPE), f32(CHIPS, STRIP, NOPE),
        *[f32(*square)] * RING, *[pltpu.VMEM(square, BF)] * RING,
        dma(len(PEERS), TWO), dma(GROUP, TWO), dma(len(PEERS), 3), dma(GROUP, 3), dma(len(PEERS), 1), dma(GROUP, 1),
        dma(GROUP, len(PEERS)), dma(GROUP), dma(GROUP, TWO), dma(TWO, RING, TWO), dma(TWO), dma(TWO),
        sum_sems(3), sum_sems(TWO), dma(GROUP), dma(GROUP), dma(TWO), dma(TWO), dma(TWO), dma(TWO),
    ]
    results = [
        shape((TWO, HALF, VAL), BF), shape((QK, TWO * HALF), F32), shape((TWO, HALF, LATENT), F32), shape((ROPE, TWO * HALF), F32),
        shape((LATENT, NOPE), F32), shape((LATENT, VAL), F32),
    ]
    landing = [shape((TWO, RING, TWO * VAL, HALF), F32), shape((TWO * VAL, HALF), F32), *sum_bufs(ROWS, 3 * LANES), *sum_bufs(KV, HALF)]
    anywhere = pl.BlockSpec(memory_space=pl.ANY)
    return pl.pallas_call(
        core_kernel,
        out_shape=results + landing,
        in_specs=[pl.BlockSpec(memory_space=pltpu.VMEM)] * 6,
        out_specs=[anywhere] * len(results + landing),
        scratch_shapes=scratch,
        compiler_params=pltpu.CompilerParams(collective_id=0, has_side_effects=True, vmem_limit_bytes=67043328),
        name='core',
    )(c, kpe, q, wk, wv, do)[:len(results)]


def solution(mesh):
    batch = ('pod', 'data')
    token_spec = P(batch, 'cp')
    sum_spec = P('pod')

    def per_device(c_latent, k_rope, queries, w_uk, w_uv, d_out):
        halves = lambda a: a.reshape(TWO, HALF, a.shape[-1])
        o, gq, gc, gr, guk, guv = core_call(halves(c_latent), k_rope[0].T, queries[0, :, 0].T, w_uk[:, 0], w_uv[:, 0], halves(d_out))
        return o.reshape(d_out.shape), gq.T.reshape(queries.shape), gc.reshape(c_latent.shape), gr.T.reshape(k_rope.shape), guk[:, None], guv[:, None]

    return jax.shard_map(per_device, mesh=mesh, in_specs=(token_spec, token_spec, token_spec, P(), P(), token_spec), out_specs=(token_spec, token_spec, token_spec, token_spec, sum_spec, sum_spec), check_vma=False)
```

```python
import jax
import jax.numpy as jnp
from jax import lax
from jax.experimental import pallas as pl
from jax.experimental.pallas import tpu as pltpu
from jax.sharding import PartitionSpec as P

BF = jnp.bfloat16
F32 = jnp.float32
NEG_BIG = -1.0e30
HALF = 512
LATENT = 512
LANES = 128
NOPE = 128
ROPE = 64
QK = NOPE + ROPE
VAL = 128
KV = QK + VAL
AUG = 16
SCALE = QK ** -0.5
EXP2_SCALE = SCALE * 1.4426950408889634
TWO = 2
RING = 4
FAR = RING - 1
GROUP = 8
HALVES = range(TWO)
NEIGHBOURS = (1, 2)
PEERS = range(1, GROUP)
CHIPS = GROUP * GROUP
STRIP = LATENT // CHIPS
ROWS = HALF // TWO
BLOCKS = HALF // LANES
Q_STEPS = (1, 2, 9, 12, 25, 30, 35)
K_STEPS = (3, 6, 15, 20, 40, 48, 56)
DO_STEPS, DO_RANKS = (49, 50, 51, 52, 53, 54), (1, 2, 3, 5, 6, 7)
T_RELAY, T_OWN_DO, T_RELAY_DO = 9, 12, 34
T_LAST = 56
T_END = 64
RECTS = ((1, 0, 1, 1, 2, False), (3, 1, 2, 0, 3, False), (9, 0, 3, 3, 2, True), (15, 3, 2, 0, 5, False), (25, 0, 5, 5, 3, True), (40, 5, 2, 0, 8, False))
K_ORDER = (7, 5, 6, 4, 3, 1, 2)
Q_FIRST, Q_REST = (7, 5, 6), (3, 1, 2, 4, 0)
T_SPLIT, T_MIX = 48, 52
M_REST, M_OWN = 9, 14
T_VIA = (9, 41)
T_FETCH, T_ADD = (21, 53), (22, 54)
T_NEAR, NEAR = (23, 25), (5, 6)
T_ONE = (49, 55)
T_NEAR_MID, T_NEAR_LAST = 55, 60
T_PAIR_O = 56
T_PAIR_KV = (36, 45)
T_VIA_Q, T_Q_FIVE, T_Q_SIX = 54, 56, 57


def mm(a, b):
    return jnp.dot(a, b, preferred_element_type=F32)


def mm_t(a, b):
    return lax.dot_general(a, b, (((1,), (1,)), ((), ())), preferred_element_type=F32)


def gray(r):
    return r ^ (r >> 1)


def part(n, size):
    return slice(n * size, (n + 1) * size)


def rows_of(n, size):
    return pl.ds(pl.multiple_of(n * size, size), size)


def order(n, ranks):
    out = ranks[-1]
    for i, r in list(enumerate(ranks))[-2::-1]:
        out = jnp.where(n <= i, r, out)
    return out


def among(t, steps):
    out = t == steps[0]
    for v in steps[1:]:
        out = out | (t == v)
    return out


def at(t, steps, ranks):
    out = ranks[-1]
    for v, r in list(zip(steps, ranks))[-2::-1]:
        out = jnp.where(t <= v, r, out)
    return out


def start(copies):
    for c in copies:
        c.start()


def done(copies):
    for c in copies:
        c.wait()


class Remote:
    def __init__(self, pairs, send, recv, dev, ref):
        self.pairs, self.send, self.recv, self.dev, self.ref = pairs, send, recv, dev, ref

    def start(self):
        for src, dst in self.pairs:
            pltpu.make_async_remote_copy(src, dst, self.send, self.recv, device_id=self.dev).start()

    def wait_recv(self):
        pltpu.make_async_copy(self.ref, self.ref, self.recv).wait()

    def wait_send(self):
        pltpu.make_async_copy(self.ref, self.ref, self.send).wait()


def landed(copies):
    for c in copies:
        c.wait_recv()


def left(copies):
    for c in copies:
        c.wait_send()


def remote(pairs, send, recv, dev, ref):
    return [Remote(pairs, send, recv, dev, ref)]


def ring_sums(slot, dev, far_rank, srcs, dsts, bufs, sems, ref):
    main, via, pair = bufs
    main_send, main_recv, via_send, via_recv, pair_send, pair_recv = sems

    def near(rank, p):
        d, n = rank // RING, rank % RING - 1
        return remote(zip(srcs(slot(rank), p), dsts(main.at[d, n, p])), main_send.at[rank, p], main_recv.at[d, n, p], dev(n + 1), ref)

    def far(d, p):
        return remote(zip(srcs(slot(RING * d + FAR), p), dsts(via.at[d, p])), via_send.at[d, p], via_recv.at[d, p], dev(far_rank(d, p)), ref)

    def across(p):
        return remote(zip(srcs(slot(RING), p), dsts(pair.at[p])), pair_send.at[p], pair_recv.at[p], dev(RING), ref)

    return near, far, across


def core_kernel(c_in, kpe_in, q_in, wk_in, wv_in, do_in,
                out_o, out_q, out_c, out_r, out_uk, out_uv, xo, po, xq, xqv, pq, zkv, zkvv, pkv,
                q_s, qr_s, k_s, kr_s, vt_s, do_s, qt_s, kt_s, dot_s,
                ot_s, m_s, l_s, dq_s, dqr_s, dk_s, dv_s, st_s, st_r, stg, w_s, ws_r, wl_r, rope_s, q_out_s, wr_s, wr_r,
                sc0, sc1, dp0, dp1, pr0, pr1, ds0, ds1,
                q_send, q_recv, k_send, k_recv, do_send, do_recv, st_send, st_recv, xo_send, xo_recv, po_send, po_recv,
                q_sums_sems, kv_sums_sems, loc, outs, w_send, w_recv, strip_send, strip_recv):
    me = lax.axis_index('cp')
    core = lax.axis_index('data')
    row, col = me // GROUP, me % GROUP
    x, y0 = col % RING, col // RING
    y1, z = row % TWO, row // TWO

    def row_slot(rank):
        return RING * (y0 ^ (rank // RING)) + (x + gray(rank % RING)) % RING

    def col_slot(rank):
        return TWO * ((z + gray(rank % RING)) % RING) + (y1 ^ (rank // RING))

    def row_dev(rank):
        return {'cp': GROUP * row + row_slot(rank)}

    def col_dev(rank):
        return {'cp': GROUP * col_slot(rank) + col}

    mate = {'data': 1 - core}
    barrier = pltpu.get_barrier_semaphore()

    def to_others(act):
        def one(n, carry):
            act((me + n) % CHIPS)
            return carry

        lax.fori_loop(1, CHIPS, one, 0)

    to_others(lambda d: pl.semaphore_signal(barrier, inc=1, device_id={'cp': d}))
    pl.semaphore_signal(barrier, inc=1, device_id=mate)

    wvt = wv_in[:].T
    for h in HALVES:
        q = q_in[:, part(h, HALF)]
        qt_s[col, h] = q
        q_s[col, h, :, :QK] = q.T
        qr_s[col, :, part(h, ROPE)] = q[NOPE:].T
        do_s[col, h, :, :VAL] = do_in[h]
    for h in HALVES:
        k_s[row, h, :, :NOPE] = mm(c_in[h], wk_in[:]).astype(BF)
        rope = kpe_in[:, part(h, HALF)].T
        k_s[row, h, :, NOPE:] = jnp.concatenate([rope, rope], axis=1)
        kr_s[row, :, part(h, ROPE)] = rope
        vt_s[row, h, :VAL] = mm_t(wvt, c_in[h]).astype(BF)

    pl.semaphore_wait(barrier, CHIPS)

    def like(n):
        return qr_s.at[pl.ds(0, n)]

    def q_copies(n, slot, dev):
        refs = [q_s.at[slot, :, :, :NOPE], qr_s.at[slot]]
        return remote(zip(refs, refs), q_send.at[n], q_recv.at[slot], dev, like(3))

    def k_copies(n, slot, dev):
        refs = [k_s.at[slot, :, :, :NOPE], kr_s.at[slot], vt_s.at[slot, :, :VAL]]
        return remote(zip(refs, refs), k_send.at[n], k_recv.at[slot], dev, like(5))

    def do_copies(n, slot, dev):
        ref = do_s.at[slot, :, :, :VAL]
        return remote([(ref, ref)], do_send.at[n], do_recv.at[slot], dev, like(TWO))

    first_copies = (FAR, 0, 1)

    def own_copies(copies, slot, dev, n):
        return copies(n, slot(0), dev(n + 1))

    def pair_copies(copies, slot, dev, n):
        return copies(RING + n, slot(RING), dev(n + 1))

    q_kind, k_kind, do_kind = (q_copies, row_slot, row_dev), (k_copies, col_slot, col_dev), (do_copies, row_slot, row_dev)

    for n in first_copies:
        start(own_copies(*q_kind, n))
        start(own_copies(*k_kind, n))

    def arrived(copies, slot, dev, rank):
        landed(copies(0, slot(rank), dev(1)))

    def wait_q(rank):
        arrived(*q_kind, rank)

    def wait_k(rank):
        arrived(*k_kind, rank)

    def wait_do(rank):
        arrived(*do_kind, rank)

    ones = jnp.where(lax.broadcasted_iota(jnp.int32, (AUG, HALF), 0) < 3, 1.0, 0.0).astype(BF)

    def clear(s, carry):
        for h in HALVES:
            for ref in (ot_s, dq_s, dk_s, dv_s, l_s):
                ref[s, h] = jnp.zeros(ref.shape[TWO:], F32)
            m_s[s, h] = jnp.full(m_s.shape[TWO:], NEG_BIG, F32)
            kt_s[s, h, QK:] = ones
            vt_s[s, h, VAL:] = ones
        dqr_s[s] = jnp.zeros((HALF, LANES), F32)
        return carry

    def place_q(s):
        for h in HALVES:
            q_s[s, h, :, NOPE:QK] = qr_s[s, :, part(h, ROPE)]
            qt_s[s, h] = q_s[s, h, :, :QK].T

    def place_k(s):
        for h in HALVES:
            rope = kr_s[s, :, part(h, ROPE)]
            k_s[s, h, :, NOPE:] = jnp.concatenate([rope, rope], axis=1)
            kt_s[s, h, :QK] = k_s[s, h, :, :QK].T

    def place_do(s):
        for h in HALVES:
            dot_s[s, h] = do_s[s, h, :, :VAL].T

    for h in HALVES:
        kt_s[row, h, :QK] = k_s[row, h, :, :QK].T
    place_do(col)
    lax.fori_loop(0, GROUP, clear, 0)

    def diagonal_half(ks, qs):
        return jnp.where((ks < row) | ((ks == row) & (col <= qs)), 0, 1)

    def two_blocks(ks, qs):
        h = diagonal_half(ks, qs)
        return (ks, qs, 0, 1), (ks, qs, h, h)

    own_blocks = [(row, col, kh, qh) for kh in HALVES for qh in HALVES if kh <= qh]

    def f_blocks(t):
        a, b = GROUP - 1, 0
        end = T_LAST
        for t0, a0, na, b0, nb, inner in RECTS[::-1]:
            u = t - t0
            pa, pb = (a0 + u % na, b0 + u // na) if inner else (a0 + u // nb, b0 + u % nb)
            a, b = jnp.where(t < end, pa, a), jnp.where(t < end, pb, b)
            end = t0
        return two_blocks(col_slot(a), jnp.where(t < T_LAST, row_slot(b), t - T_LAST))

    def f_scores(sc, blk):
        ks, qs, kh, qh = blk
        sc[:] = mm(k_s[ks, kh, :, :QK], qt_s[qs, qh])

    def f_use(sc, blk):
        ks, qs, kh, qh = blk
        s = sc[:]
        if isinstance(kh, int) and kh == qh:
            keys = lax.broadcasted_iota(jnp.int32, s.shape, 0)
            s = jnp.where(keys <= lax.broadcasted_iota(jnp.int32, s.shape, 1), s, NEG_BIG)
        m0 = m_s[qs, qh]
        m1 = jnp.maximum(m0, jnp.max(s, axis=0, keepdims=True))
        p = jnp.exp2((s - m1) * EXP2_SCALE)
        alpha = jnp.exp2((m0 - m1) * EXP2_SCALE)
        l_s[qs, qh] = l_s[qs, qh] * alpha + jnp.sum(p, axis=0, keepdims=True)
        m_s[qs, qh] = m1
        ot_s[qs, qh] = ot_s[qs, qh] * alpha + mm(vt_s[ks, kh, :VAL], p.astype(BF))

    def own_f():
        for blk in own_blocks:
            f_scores(sc0, blk)
            f_use(sc0, blk)

    own_f()

    def stats_copies(slot, n):
        return remote([(st_s.at[slot], st_r.at[slot, col])], st_send.at[slot], st_recv.at[slot], row_dev(n), st_r.at[slot, pl.ds(0, len(PEERS))])

    def make_stats(qs):
        for h in HALVES:
            d = jnp.sum(ot_s[qs, h] * dot_s[qs, h].astype(F32), axis=0, keepdims=True)
            for j in range(BLOCKS):
                c = part(j, LANES)
                for i, v in enumerate((m_s[qs, h, :, c], l_s[qs, h, :, c], d[:, c])):
                    st_s[qs, part(GROUP * i + BLOCKS * h + j, 1)] = v

    def start_stats(qs):
        for n in PEERS:
            start(stats_copies(qs, n))
        st_r[qs, col] = st_s[qs]

    def f_arrive(t):
        @pl.when(among(t, tuple(sorted({*Q_STEPS, *K_STEPS, *DO_STEPS, T_RELAY, T_OWN_DO, T_RELAY_DO}))))
        def _():
            @pl.when(among(t, Q_STEPS))
            def _():
                rank = at(t, Q_STEPS, PEERS)

                @pl.when(rank != RING)
                def _():
                    wait_q(rank)

                @pl.when(rank == 1)
                def _():
                    start(own_copies(*q_kind, TWO))
                place_q(row_slot(rank))

            @pl.when(among(t, K_STEPS))
            def _():
                rank = at(t, K_STEPS, PEERS)

                @pl.when(rank != RING)
                def _():
                    wait_k(rank)

                @pl.when(rank == 1)
                def _():
                    start(own_copies(*k_kind, TWO))
                place_k(col_slot(rank))

            @pl.when(among(t, DO_STEPS))
            def _():
                rank = at(t, DO_STEPS, DO_RANKS)
                wait_do(rank)
                place_do(row_slot(rank))

            @pl.when(t == T_RELAY)
            def _():
                wait_q(RING)
                for n in range(FAR):
                    start(pair_copies(*q_kind, n))
                wait_k(RING)
                for n in range(FAR):
                    start(pair_copies(*k_kind, n))

            @pl.when(t == T_OWN_DO)
            def _():
                for n in (*first_copies, TWO):
                    start(own_copies(*do_kind, n))

            @pl.when(t == T_RELAY_DO)
            def _():
                wait_do(RING)
                for n in range(FAR):
                    start(pair_copies(*do_kind, n))
                place_do(row_slot(RING))

    for t in NEIGHBOURS:
        f_arrive(t)
    blocks = f_blocks(jnp.int32(1))
    for sc, blk in zip((sc0, sc1), blocks):
        f_scores(sc, blk)

    def f_half(t, used, made, b1, b2):
        n1, n2 = after = f_blocks(jnp.minimum(t + 1, T_END - 1))
        f_scores(made[0], n1)
        f_use(used[0], b1)
        f_scores(made[1], n2)
        f_use(used[1], b2)

        @pl.when(t >= T_LAST)
        def _():
            @pl.when(t > T_LAST)
            def _():
                start_stats(t - T_LAST - 1)

            make_stats(t - T_LAST)

        f_arrive(t + TWO)
        return after

    def f_step(u, carry):
        t = TWO * u + 1
        after = f_half(t, (sc0, sc1), (dp0, dp1), *carry)

        @pl.when(t < T_END - 1)
        def _():
            f_half(t + 1, (dp0, dp1), (sc0, sc1), *after)
        return f_blocks(jnp.minimum(t + TWO, T_END - 1))

    lax.fori_loop(0, T_END // TWO, f_step, blocks)
    start_stats(GROUP - 1)

    o_all = stg.at[pl.ds(0, TWO * VAL)]

    def o_refs(slot, buf):
        return [(ot_s.at[slot, h], buf.at[pl.ds(h * VAL, VAL)]) for h in HALVES]

    def o_copies(s):
        d = (s // RING) ^ y0
        return remote(o_refs(s, xo.at[d, x]), xo_send.at[s], xo_recv.at[d, x], {'cp': GROUP * row + RING * y0 + s % RING}, o_all)

    def o_pair():
        return remote(o_refs(row_slot(RING), po), po_send.at[0], po_recv.at[0], row_dev(RING), o_all)

    def dq_srcs(s, p):
        r = pl.ds(p * ROWS, ROWS)
        return [dq_s.at[s, 0, r], dq_s.at[s, 1, r], dqr_s.at[s, r]]

    def dq_dsts(buf):
        return [buf.at[:, pl.ds(LANES * j, LANES)] for j in range(3)]

    def kv_srcs(s, h):
        return [dk_s.at[s, h], dv_s.at[s, h]]

    def kv_dsts(buf):
        return [buf.at[pl.ds(0, QK)], buf.at[pl.ds(QK, VAL)]]

    dq_near, dq_far, dq_across = ring_sums(row_slot, row_dev, lambda d, p: RING if d else p + 1, dq_srcs, dq_dsts, (xq, xqv, pq), q_sums_sems, stg.at[pl.ds(0, ROWS * 3 * LANES // HALF)])
    kv_near, kv_far, kv_across = ring_sums(col_slot, col_dev, lambda d, p: p + 1, kv_srcs, kv_dsts, (zkv, zkvv, pkv), kv_sums_sems, stg.at[pl.ds(0, KV)])

    def local(pairs, n=0):
        return [pltpu.make_async_copy(src, dst, loc.at[n + i]) for i, (src, dst) in enumerate(pairs)]

    def o_local(d):
        return local([(xo.at[d, (x + gray(r)) % RING], stg.at[pl.ds(HALF * (r - 1), HALF // TWO)]) for r in range(1, RING)])

    def fetch_o(d):
        for r in range(1, RING):
            s = (x + gray(r)) % RING
            landed(remote(o_refs(0, xo.at[d, s]), xo_send.at[r], xo_recv.at[d, s], row_dev(r), o_all))
        start(o_local(d))

    def add_o(slot, d):
        done(o_local(d))
        for h in HALVES:
            ot_s[slot, h] = ot_s[slot, h] + sum(stg[HALF * n + h * VAL:HALF * n + (h + 1) * VAL] for n in range(FAR))

    def kv_local(d, h):
        return local([(zkv.at[d, n, h], stg.at[pl.ds(KV * n, KV)]) for n in HALVES])

    def fetch_kv(d, h):
        for r in NEIGHBOURS:
            landed(kv_near(RING * d + r, h))
        start(kv_local(d, h))

    def add_kv(slot, d, h):
        done(kv_local(d, h))
        dk_s[slot, h] = dk_s[slot, h] + (stg[:QK] + stg[KV:KV + QK])
        dv_s[slot, h] = dv_s[slot, h] + (stg[QK:KV] + stg[KV + QK:KV + KV])

    def kv_via_local(d):
        return local([(zkvv.at[d, h], stg.at[pl.ds(KV * h, KV)]) for h in HALVES])

    def fetch_kv_via(d):
        for h in HALVES:
            landed(kv_far(d, h))
        start(kv_via_local(d))

    def add_kv_via(d):
        done(kv_via_local(d))
        for h in HALVES:
            slot, u = col_slot(RING * d + 1 + h), KV * h
            dk_s[slot, h] = dk_s[slot, h] + stg[u:u + QK]
            dv_s[slot, h] = dv_s[slot, h] + stg[u + QK:u + KV]

    def dq_stage(n, p):
        return stg.at[pl.ds(HALF * n + ROWS * p, ROWS), pl.ds(0, 3 * LANES)]

    def add_dq(slot, p, ns):
        r = part(p, ROWS)
        for j in range(3):
            c = part(j, LANES)
            total = sum(stg[HALF * n + ROWS * p:HALF * n + ROWS * (p + 1), c] for n in ns)
            if j < TWO:
                dq_s[slot, j, r] = dq_s[slot, j, r] + total
            else:
                dqr_s[slot, r] = dqr_s[slot, r] + total

    def sum_dq_via(d):
        for p in HALVES:
            landed(dq_far(d, p))
        copies = local([(xqv.at[d, p], dq_stage(0, p)) for p in HALVES])
        start(copies)
        done(copies)
        for p in HALVES:
            add_dq(row_slot(FAR if d else 1 + p), p, (0,))

    def dq_arrived(d):
        for p in HALVES:
            for r in NEIGHBOURS:
                landed(dq_near(RING * d + r, p))
        return [(xq.at[d, n, p], dq_stage(n, p)) for n in HALVES for p in HALVES]

    def columns(v):
        flat = jnp.concatenate([v[part(j, 1)] for j in range(BLOCKS)], axis=1)
        hi = flat.astype(BF).astype(F32)
        mid = (flat - hi).astype(BF).astype(F32)
        return jnp.concatenate([hi, mid, flat - hi - mid, jnp.zeros((AUG - 3, HALF), F32)], axis=0).T.astype(BF)

    def wait_stats(qs):
        landed(stats_copies(qs, 1))

    def prepare(qs):
        wait_stats(qs)
        m, l, d = (st_r[qs, :, part(i, GROUP)] for i in range(3))
        m_all = jnp.max(m, axis=0)
        w = jnp.exp2((m - m_all[None]) * EXP2_SCALE)
        l_all = jnp.sum(w * l, axis=0)
        inv = 1.0 / l_all
        delta = jnp.sum(w * d, axis=0) * inv
        lse = m_all + jnp.log2(l_all) * (1.0 / EXP2_SCALE)
        mine = jnp.exp2((st_s[qs, :GROUP] - m_all) * EXP2_SCALE) * inv
        for h in HALVES:
            q_s[qs, h, :, QK:] = columns(-lse[part(h, BLOCKS)])
            do_s[qs, h, :, VAL:] = columns(-delta[part(h, BLOCKS)])
            for j in range(BLOCKS):
                c = part(j, LANES)
                ot_s[qs, h, :, c] = ot_s[qs, h, :, c] * mine[part(BLOCKS * h + j, 1)]

    def b_mixed(m):
        first, rest = m < M_REST, m < M_OWN
        rank = jnp.where(first, order(m // 3, Q_FIRST), order(jnp.where(rest, m - M_REST, (m - M_OWN) // TWO), Q_REST))
        ring = jnp.where(first, m % 3, jnp.where(rest, 0, 1)) == 0
        same = ring | (jnp.where(first, m % 3, 1 + m % TWO) == TWO)
        ks, qs = jnp.where(ring, col_slot(K_ORDER[-1]), row), row_slot(rank)
        h = diagonal_half(ks, qs)
        return ks, qs, jnp.where(same, h, 0), jnp.where(same, h, 1)

    def b_blocks(t):
        b1, b2 = two_blocks(col_slot(order(t // GROUP, K_ORDER)), t % GROUP)
        pick = lambda c, a, b: tuple(jnp.where(c, i, j) for i, j in zip(a, b))
        last = col_slot(K_ORDER[-1])
        u = TWO * (t - T_SPLIT)
        m = TWO * (t - T_MIX)
        return tuple(pick(t < T_SPLIT, b, pick(t < T_MIX, (last, u + n, 0, 1), b_mixed(m + n))) for n, b in enumerate((b1, b2)))

    def b_scores(sc, dp, blk):
        ks, qs, kh, qh = blk
        sc[:] = mm(q_s[qs, qh], kt_s[ks, kh])
        dp[:] = mm(do_s[qs, qh], vt_s[ks, kh])

    def b_elem(sc, dp, pr, ds, mask=False):
        p = jnp.exp2(sc[:] * EXP2_SCALE)
        if mask:
            rows = lax.broadcasted_iota(jnp.int32, p.shape, 0)
            p = jnp.where(lax.broadcasted_iota(jnp.int32, p.shape, 1) <= rows, p, 0.0)
        pr[:] = p.astype(BF)
        ds[:] = (p * dp[:]).astype(BF)

    def b_grads(pr, ds, blk):
        ks, qs, kh, qh = blk
        p = pr[:]
        g = ds[:]
        dv_s[ks, kh] += mm(dot_s[qs, qh], p)
        dk_s[ks, kh] += mm(qt_s[qs, qh], g)
        dq = mm(g, k_s[ks, kh])
        dq_s[qs, qh] += dq[:, :NOPE]
        side = lax.broadcasted_iota(jnp.int32, (1, LANES), 1) // ROPE
        dqr_s[qs] += jnp.where(side == qh, dq[:, NOPE:], 0.0)

    early_half = 1 - diagonal_half(col_slot(K_ORDER[-1]), 0)

    def b_events(t):
        @pl.when((t <= GROUP) | among(t, (*T_VIA, *T_FETCH, *T_ADD, *T_NEAR, *T_ONE, T_NEAR_MID, T_NEAR_LAST, T_PAIR_O - 1, T_PAIR_O, T_PAIR_O + 1, T_VIA_Q, T_Q_FIVE, T_Q_SIX)) | among(t, tuple(v + i for v in T_PAIR_KV for i in range(3))))
        def _():
            @pl.when((t < GROUP - 1) & (t % TWO == 1))
            def _():
                for n in NEIGHBOURS:
                    prepare(t + n)

            @pl.when((t <= GROUP) & ((t - 1) % RING != x))
            def _():
                start(o_copies(t - 1))

            @pl.when(among(t, T_VIA))
            def _():
                for h in HALVES:
                    start(kv_far(at(t, T_VIA, (1, 0)), h))

            @pl.when(among(t, T_FETCH))
            def _():
                fetch_kv_via(at(t, T_FETCH, (1, 0)))

            @pl.when(among(t, T_ADD))
            def _():
                add_kv_via(at(t, T_ADD, (1, 0)))

            @pl.when(among(t, T_NEAR))
            def _():
                for h in HALVES:
                    start(kv_near(at(t, T_NEAR, NEAR), h))

            @pl.when(among(t, T_ONE))
            def _():
                start(kv_near(1, at(t, T_ONE, (1, 0))))

            @pl.when(t == T_NEAR_MID)
            def _():
                start(kv_near(K_ORDER[-1], early_half))

            @pl.when(t == T_NEAR_LAST)
            def _():
                start(kv_near(K_ORDER[-1], 1 - early_half))

            @pl.when(t == T_VIA_Q)
            def _():
                for p in HALVES:
                    start(dq_far(1, p))

            @pl.when(t == T_Q_FIVE)
            def _():
                start(dq_near(5, 0) + dq_near(5, 1))

            @pl.when(t == T_Q_SIX)
            def _():
                start(dq_near(6, 0) + dq_near(6, 1))

            @pl.when(t == T_PAIR_O - 1)
            def _():
                fetch_o(1)

            @pl.when(t == T_PAIR_O)
            def _():
                add_o(row_slot(RING), 1)

            @pl.when(t == T_PAIR_O + 1)
            def _():
                start(o_pair())

            for h, v in enumerate(T_PAIR_KV):
                @pl.when(t == v)
                def _():
                    fetch_kv(1, h)

                @pl.when(t == v + 1)
                def _():
                    add_kv(col_slot(RING), 1, h)

                @pl.when(t == v + TWO)
                def _():
                    start(kv_across(h))

    def b_step(t, carry):
        before, (b1, b2) = carry
        after = b_blocks(jnp.minimum(t + 1, T_END - TWO))
        b_scores(sc1, dp1, b2)
        b_elem(sc0, dp0, pr0, ds0)
        b_grads(pr1, ds1, before)
        b_scores(sc0, dp0, after[0])
        b_elem(sc1, dp1, pr1, ds1)
        b_grads(pr0, ds0, b1)
        b_events(t + 1)
        return b2, after

    for ref in (pr1, ds1):
        ref[:] = jnp.zeros(ref.shape, BF)
    for s in HALVES:
        prepare(s)
    blocks = b_blocks(jnp.int32(0))
    b_scores(sc0, dp0, blocks[0])
    before, _ = lax.fori_loop(0, T_END - 1, b_step, (blocks[1], blocks))
    b_grads(pr1, ds1, before)

    def own_b():
        for blk in own_blocks:
            b_scores(sc0, dp0, blk)
            b_elem(sc0, dp0, pr0, ds0, mask=blk[TWO] == blk[3])
            b_grads(pr0, ds0, blk)

    own_b()

    def finish_o():
        fetch_o(0)
        add_o(col, 0)
        landed(o_pair())
        last_o = local([(po, stg.at[pl.ds(HALF // TWO, HALF // TWO)])])
        start(last_o)
        for n in range(RING):
            left(own_copies(*do_kind, n))
        done(last_o)
        for h in HALVES:
            do_s[col, h, :, :VAL] = (ot_s[col, h] + stg[part(TWO + h, VAL)]).T.astype(BF)

    sum_dq_via(1)
    start(dq_far(0, 0) + dq_far(0, 1))
    for pr, h in zip((pr0, pr1), HALVES):
        pr[:] = c_in[h].T

    def finish_dq_pair():
        copies = local(dq_arrived(1))
        start(copies)
        done(copies)
        for p in HALVES:
            add_dq(row_slot(RING), p, HALVES)

    finish_dq_pair()
    start(dq_across(0))

    def finish_dkv():
        sums = None
        for h in HALVES:
            fetch_kv(0, h)
            landed(kv_across(h))
            pair = local([(pkv.at[h], sc0.at[pl.ds(0, KV)])], TWO)
            start(pair)
            add_kv(row, 0, h)
            done(pair)
            dk = (dk_s[row, h] + sc0[:QK]) * SCALE
            dv = dv_s[row, h] + sc0[QK:KV]
            rope_s[:, part(h, HALF)] = dk[NOPE:]
            kv = jnp.concatenate([dk[:NOPE].T, dv.T], axis=1)
            (dp0, dp1)[h][:, :NOPE + VAL] = kv
            product = mm((pr0, pr1)[h][:].astype(F32), kv)
            sums = product if sums is None else sums + product
        w_s[0] = sums[:, :NOPE]
        w_s[1] = sums[:, NOPE:]

    finish_dkv()

    def w_swap(src, dst, n):
        return remote([(src, dst)], w_send.at[n], w_recv.at[n], mate, src)

    def strip(d):
        return rows_of(d, STRIP)

    def to_all(n, src, dst):
        to_others(lambda d: pltpu.make_async_remote_copy(src(d), dst, strip_send.at[n], strip_recv.at[n], device_id={'cp': d}).start())

    def all_of(sem, n):
        strips = wr_r.at[pl.ds(0, CHIPS - 1)]
        pltpu.make_async_copy(strips, strips, sem.at[n]).wait()

    first = w_swap(w_s.at[1 - core], ws_r, 0)
    start(first)

    def left_early():
        left(stats_copies(0, 1))
        for r in PEERS:
            left(stats_copies(r, 1))
            if r != RING:
                left(o_copies(row_slot(r)))
            if r % RING in NEIGHBOURS:
                for p in HALVES:
                    left(kv_near(r, p))
        for p in HALVES:
            left(kv_across(p) + dq_far(1, p))
            for r in NEIGHBOURS:
                left(dq_near(RING + r, p))
            for d in HALVES:
                left(kv_far(d, p))
        left(o_pair())
        for n in range(RING):
            left(own_copies(*q_kind, n) + own_copies(*k_kind, n))
        for n in range(FAR):
            left(pair_copies(*q_kind, n) + pair_copies(*k_kind, n) + pair_copies(*do_kind, n))

    def finish_c():
        w_all = jnp.concatenate([wk_in[:], wv_in[:]], axis=1).astype(F32)
        for kv, out in ((dp0, sc0), (dp1, sc1)):
            out[:] = mm_t(kv[:, :NOPE + VAL], w_all)

    finish_c()
    outputs = [(sc0, out_c.at[0]), (sc1, out_c.at[1]), (rope_s, out_r)]
    more = [pltpu.make_async_copy(src, dst, outs.at[1 + n]) for n, (src, dst) in enumerate(outputs)]
    start(more)
    finals = more

    def w_one():
        landed(first)
        wr_s[:] = w_s[core] + ws_r[:]

    w_one()
    to_all(0, lambda d: wr_s.at[strip(d)], wr_r.at[me])
    start(dq_across(1) + dq_near(1, 1) + dq_near(2, 0))
    wr_r[me] = wr_s[strip(me)]
    finish_o()
    o_out = [pltpu.make_async_copy(do_s.at[col, :, :, :VAL], out_o, outs.at[0])]
    start(o_out)
    finals += o_out
    sum_dq_via(0)
    left(first)

    left_early()

    def w_two():
        all_of(strip_recv, 0)
        w_s[core, strip(me)] = jnp.sum(wr_r[:], axis=0)

    w_two()
    mine = w_s.at[core, strip(me)]
    to_all(1, lambda d: mine, mine)
    start(dq_near(1, 0) + dq_near(2, 1))

    def w_three():
        all_of(strip_recv, 1)

    w_three()
    last = w_swap(w_s.at[core], wl_r, 1)
    start(last)

    def finish_dq():
        pairs = dq_arrived(0)
        for p in HALVES:
            landed(dq_across(p))
        copies = local(pairs + [(pq.at[p], dq_stage(TWO, p)) for p in HALVES])
        start(copies)
        done(copies)
        for p in HALVES:
            add_dq(col, p, range(3))
        for h in HALVES:
            q_out_s[:NOPE, part(h, HALF)] = (dq_s[col, h] * SCALE).T
        rope = (dqr_s[col] * SCALE).T
        for h in HALVES:
            q_out_s[NOPE:, part(h, HALF)] = rope[part(h, ROPE)]

    def w_five():
        landed(last)
        w_s[1 - core] = wl_r[:]

    w_five()
    more = [pltpu.make_async_copy(src, dst, outs.at[RING + n]) for n, (src, dst) in enumerate([(w_s.at[0], out_uk), (w_s.at[1], out_uv)])]
    start(more)
    finals += more
    finish_dq()
    q_out = pltpu.make_async_copy(q_out_s, out_q, outs.at[RING + TWO])
    q_out.start()

    def left_late():
        left(last)
        for n in HALVES:
            all_of(strip_send, n)
        for p in HALVES:
            left(dq_across(p) + dq_far(0, p))
            for r in NEIGHBOURS:
                left(dq_near(r, p))

    left_late()

    def out_done():
        done(finals + [q_out])

    out_done()


def core_call(c, kpe, q, wk, wv, do):
    dma = lambda *s: pltpu.SemaphoreType.DMA(s)
    shape = jax.ShapeDtypeStruct
    per = (GROUP, TWO)
    wide = lambda *s: pltpu.VMEM(per + s, BF)
    sums = lambda *s: pltpu.VMEM(per + s, F32)
    f32 = lambda *s: pltpu.VMEM(s, F32)
    packed = pltpu.VMEM((GROUP, HALF, LANES), BF)

    def sum_sems():
        return [dma(*s) for s in ((GROUP, TWO), (TWO, TWO, TWO), (TWO, TWO), (TWO, TWO), (TWO,), (TWO,))]

    def sum_bufs(*s):
        return [shape((TWO, TWO, TWO, *s), F32), shape((TWO, TWO, *s), F32), shape((TWO, *s), F32)]

    square = (HALF, HALF)
    scratch = [
        wide(HALF, QK + AUG), packed, wide(HALF, QK + ROPE), packed, wide(VAL + AUG, HALF), wide(HALF, VAL + AUG),
        wide(QK, HALF), wide(QK + AUG, HALF), wide(VAL, HALF),
        sums(VAL, HALF), sums(1, HALF), sums(1, HALF),
        sums(HALF, NOPE), f32(GROUP, HALF, LANES), sums(QK, HALF), sums(VAL, HALF),
        f32(GROUP, 3 * GROUP, LANES), f32(GROUP, GROUP, 3 * GROUP, LANES), f32(3 * HALF, HALF),
        f32(TWO, LATENT, NOPE), f32(LATENT, NOPE), f32(LATENT, NOPE), f32(ROPE, TWO * HALF), f32(QK, TWO * HALF),
        f32(LATENT, NOPE), f32(CHIPS, STRIP, NOPE),
        *[f32(*square)] * RING, *[pltpu.VMEM(square, BF)] * RING,
        *[dma(GROUP)] * GROUP, dma(GROUP), dma(TWO, RING), dma(1), dma(1),
        sum_sems(), sum_sems(), dma(GROUP), dma(GROUP), dma(TWO), dma(TWO), dma(TWO), dma(TWO),
    ]
    results = [
        shape((TWO, HALF, VAL), BF), shape((QK, TWO * HALF), F32), shape((TWO, HALF, LATENT), F32), shape((ROPE, TWO * HALF), F32),
        shape((LATENT, NOPE), F32), shape((LATENT, VAL), F32),
    ]
    landing = [shape((TWO, RING, TWO * VAL, HALF), F32), shape((TWO * VAL, HALF), F32), *sum_bufs(ROWS, 3 * LANES), *sum_bufs(KV, HALF)]
    anywhere = pl.BlockSpec(memory_space=pl.ANY)
    return pl.pallas_call(
        core_kernel,
        out_shape=results + landing,
        in_specs=[pl.BlockSpec(memory_space=pltpu.VMEM)] * 6,
        out_specs=[anywhere] * len(results + landing),
        scratch_shapes=scratch,
        compiler_params=pltpu.CompilerParams(collective_id=0, has_side_effects=True, vmem_limit_bytes=67043328),
        name='core',
    )(c, kpe, q, wk, wv, do)[:len(results)]


def solution(mesh):
    batch = ('pod', 'data')
    token_spec = P(batch, 'cp')
    sum_spec = P('pod')

    def per_device(c_latent, k_rope, queries, w_uk, w_uv, d_out):
        halves = lambda a: a.reshape(TWO, HALF, a.shape[-1])
        o, gq, gc, gr, guk, guv = core_call(halves(c_latent), k_rope[0].T, queries[0, :, 0].T, w_uk[:, 0], w_uv[:, 0], halves(d_out))
        return o.reshape(d_out.shape), gq.T.reshape(queries.shape), gc.reshape(c_latent.shape), gr.T.reshape(k_rope.shape), guk[:, None], guv[:, None]

    return jax.shard_map(per_device, mesh=mesh, in_specs=(token_spec, token_spec, token_spec, P(), P(), token_spec), out_specs=(token_spec, token_spec, token_spec, token_spec, sum_spec, sum_spec), check_vma=False)
```

```python
import jax
import jax.numpy as jnp
from jax import lax
from jax.experimental import pallas as pl
from jax.experimental.pallas import tpu as pltpu
from jax.sharding import PartitionSpec as P

BF = jnp.bfloat16
F32 = jnp.float32
NEG_BIG = -1.0e30
HALF = 512
LATENT = 512
LANES = 128
NOPE = 128
ROPE = 64
QK = NOPE + ROPE
VAL = 128
KV = QK + VAL
AUG = 16
SCALE = QK ** -0.5
EXP2_SCALE = SCALE * 1.4426950408889634
TWO = 2
RING = 4
FAR = RING - 1
GROUP = 8
HALVES = range(TWO)
NEIGHBOURS = (1, 2)
PEERS = range(1, GROUP)
CHIPS = GROUP * GROUP
STRIP = LATENT // CHIPS
ROWS = HALF // TWO
BLOCKS = HALF // LANES
Q_STEPS = (1, 2, 9, 12, 25, 30, 35)
K_STEPS = (3, 6, 15, 20, 40, 48, 56)
DO_STEPS, DO_RANKS = (49, 50, 51, 52, 53, 54), (1, 2, 3, 5, 6, 7)
K_RANKS = (1, 2, 4, 3, 5, 6, 7)
T_RELAY, T_RELAY_K, T_OWN_DO, T_RELAY_DO = 4, 11, 18, 36
T_LAST = 56
T_END = 64
RECTS = ((1, 0, 1, 1, 2, False), (3, 1, 2, 0, 3, False), (9, 0, 3, 3, 2, True), (15, 3, 2, 0, 5, False), (25, 0, 5, 5, 3, True), (40, 5, 2, 0, 8, False))
K_ORDER = (7, 5, 6, 4, 3, 1, 2)
Q_FIRST, Q_REST = (7, 5, 6), (3, 1, 2, 4, 0)
T_SPLIT, T_MIX = 48, 52
M_REST, M_OWN = 9, 14
T_VIA = (9, 41)
T_FETCH, T_ADD = (21, 53), (22, 54)
T_NEAR, NEAR = (23, 25), (5, 6)
T_ONE = (49, 55)
T_NEAR_MID, T_NEAR_LAST = 55, 60
T_PAIR_O = 56
T_PAIR_KV = (36, 45)
T_VIA_Q, T_Q_FIVE, T_Q_SIX = 54, 56, 57


def mm(a, b):
    return jnp.dot(a, b, preferred_element_type=F32)


def mm_t(a, b):
    return lax.dot_general(a, b, (((1,), (1,)), ((), ())), preferred_element_type=F32)


def gray(r):
    return r ^ (r >> 1)


def part(n, size):
    return slice(n * size, (n + 1) * size)


def rows_of(n, size):
    return pl.ds(pl.multiple_of(n * size, size), size)


def order(n, ranks):
    out = ranks[-1]
    for i, r in list(enumerate(ranks))[-2::-1]:
        out = jnp.where(n <= i, r, out)
    return out


def among(t, steps):
    out = t == steps[0]
    for v in steps[1:]:
        out = out | (t == v)
    return out


def at(t, steps, ranks):
    out = ranks[-1]
    for v, r in list(zip(steps, ranks))[-2::-1]:
        out = jnp.where(t <= v, r, out)
    return out


def start(copies):
    for c in copies:
        c.start()


def done(copies):
    for c in copies:
        c.wait()


class Remote:
    def __init__(self, pairs, send, recv, dev, ref):
        self.pairs, self.send, self.recv, self.dev, self.ref = pairs, send, recv, dev, ref

    def start(self):
        for src, dst in self.pairs:
            pltpu.make_async_remote_copy(src, dst, self.send, self.recv, device_id=self.dev).start()

    def wait_recv(self):
        pltpu.make_async_copy(self.ref, self.ref, self.recv).wait()

    def wait_send(self):
        pltpu.make_async_copy(self.ref, self.ref, self.send).wait()


def landed(copies):
    for c in copies:
        c.wait_recv()


def left(copies):
    for c in copies:
        c.wait_send()


def remote(pairs, send, recv, dev, ref):
    return [Remote(pairs, send, recv, dev, ref)]


def ring_sums(slot, dev, far_rank, srcs, dsts, bufs, sems, ref):
    main, via, pair = bufs
    main_send, main_recv, via_send, via_recv, pair_send, pair_recv = sems

    def near(rank, p):
        d, n = rank // RING, rank % RING - 1
        return remote(zip(srcs(slot(rank), p), dsts(main.at[d, n, p])), main_send.at[rank, p], main_recv.at[d, n, p], dev(n + 1), ref)

    def far(d, p):
        return remote(zip(srcs(slot(RING * d + FAR), p), dsts(via.at[d, p])), via_send.at[d, p], via_recv.at[d, p], dev(far_rank(d, p)), ref)

    def across(p):
        return remote(zip(srcs(slot(RING), p), dsts(pair.at[p])), pair_send.at[p], pair_recv.at[p], dev(RING), ref)

    return near, far, across


def core_kernel(c_arg, kpe_arg, q_arg, wk_arg, wv_arg, do_arg,
                out_o, out_q, out_c, out_r, out_uk, out_uv, xo, po, xq, xqv, pq, zkv, zkvv, pkv,
                c_in, kpe_in, q_in, wk_in, wv_in, do_in, q_s, qr_s, k_s, kr_s, vt_s, do_s, qt_s, kt_s, dot_s,
                ot_s, m_s, l_s, dq_s, dqr_s, dk_s, dv_s, st_s, st_r, stg, w_s, ws_r, wl_r, rope_s, q_out_s, wr_s, wr_r,
                sc0, sc1, dp0, dp1, pr0, pr1, ds0, ds1,
                q_send, q_recv, k_send, k_recv, do_send, do_recv, st_send, st_recv, xo_send, xo_recv, po_send, po_recv,
                q_sums_sems, kv_sums_sems, loc, outs, w_send, w_recv, strip_send, strip_recv):
    me = lax.axis_index('cp')
    core = lax.axis_index('data')
    row, col = me // GROUP, me % GROUP
    x, y0 = col % RING, col // RING
    y1, z = row % TWO, row // TWO

    def row_slot(rank):
        return RING * (y0 ^ (rank // RING)) + (x + gray(rank % RING)) % RING

    def col_slot(rank):
        return TWO * ((z + gray(rank % RING)) % RING) + (y1 ^ (rank // RING))

    def row_dev(rank):
        return {'cp': GROUP * row + row_slot(rank)}

    def col_dev(rank):
        return {'cp': GROUP * col_slot(rank) + col}

    args = [pltpu.make_async_copy(src, dst, loc.at[n]) for n, (src, dst) in enumerate(((q_arg, q_in), (do_arg, do_in), (kpe_arg, kpe_in), (wv_arg, wv_in), (wk_arg, wk_in), (c_arg, c_in)))]
    start(args)
    mate = {'data': 1 - core}
    barrier = pltpu.get_barrier_semaphore()

    def to_others(act):
        def one(n, carry):
            act((me + n) % CHIPS)
            return carry

        lax.fori_loop(1, CHIPS, one, 0)

    to_others(lambda d: pl.semaphore_signal(barrier, inc=1, device_id={'cp': d}))
    pl.semaphore_signal(barrier, inc=1, device_id=mate)

    done(args)
    wvt = wv_in[:].T
    for h in HALVES:
        q = q_in[:, part(h, HALF)]
        qt_s[col, h] = q
        q_s[col, h, :, :QK] = q.T
        qr_s[col, :, part(h, ROPE)] = q[NOPE:].T
        do_s[col, h, :, :VAL] = do_in[h]
    for h in HALVES:
        k_s[row, h, :, :NOPE] = mm(c_in[h], wk_in[:]).astype(BF)
        rope = kpe_in[:, part(h, HALF)].T
        k_s[row, h, :, NOPE:] = jnp.concatenate([rope, rope], axis=1)
        kr_s[row, :, part(h, ROPE)] = rope
        vt_s[row, h, :VAL] = mm_t(wvt, c_in[h]).astype(BF)

    pl.semaphore_wait(barrier, CHIPS)

    def like(n):
        return qr_s.at[pl.ds(0, n)]

    def q_copies(n, slot, dev):
        refs = [q_s.at[slot, :, :, :NOPE], qr_s.at[slot]]
        return remote(zip(refs, refs), q_send.at[n], q_recv.at[slot], dev, like(3))

    def k_copies(n, slot, dev):
        refs = [k_s.at[slot, :, :, :NOPE], kr_s.at[slot], vt_s.at[slot, :, :VAL]]
        return remote(zip(refs, refs), k_send.at[n], k_recv.at[slot], dev, like(5))

    def do_copies(n, slot, dev):
        ref = do_s.at[slot, :, :, :VAL]
        return remote([(ref, ref)], do_send.at[n], do_recv.at[slot], dev, like(TWO))

    first_copies = (FAR, 0, 1)

    def own_copies(copies, slot, dev, n):
        return copies(n, slot(0), dev(n + 1))

    def pair_copies(copies, slot, dev, n):
        return copies(RING + n, slot(RING), dev(n + 1))

    q_kind, k_kind, do_kind = (q_copies, row_slot, row_dev), (k_copies, col_slot, col_dev), (do_copies, row_slot, row_dev)

    for n in first_copies:
        start(own_copies(*q_kind, n))
        start(own_copies(*k_kind, n))

    def arrived(copies, slot, dev, rank):
        landed(copies(0, slot(rank), dev(1)))

    def wait_q(rank):
        arrived(*q_kind, rank)

    def wait_k(rank):
        arrived(*k_kind, rank)

    def wait_do(rank):
        arrived(*do_kind, rank)

    ones = jnp.where(lax.broadcasted_iota(jnp.int32, (AUG, HALF), 0) < 3, 1.0, 0.0).astype(BF)

    def clear(s, carry):
        for h in HALVES:
            for ref in (ot_s, dq_s, dk_s, dv_s, l_s):
                ref[s, h] = jnp.zeros(ref.shape[TWO:], F32)
            m_s[s, h] = jnp.full(m_s.shape[TWO:], NEG_BIG, F32)
            kt_s[s, h, QK:] = ones
            vt_s[s, h, VAL:] = ones
        dqr_s[s] = jnp.zeros((HALF, LANES), F32)
        return carry

    def place_q(s):
        for h in HALVES:
            q_s[s, h, :, NOPE:QK] = qr_s[s, :, part(h, ROPE)]
            qt_s[s, h] = q_s[s, h, :, :QK].T

    def place_k(s):
        for h in HALVES:
            rope = kr_s[s, :, part(h, ROPE)]
            k_s[s, h, :, NOPE:] = jnp.concatenate([rope, rope], axis=1)
            kt_s[s, h, :QK] = k_s[s, h, :, :QK].T

    def place_do(s):
        for h in HALVES:
            dot_s[s, h] = do_s[s, h, :, :VAL].T

    for h in HALVES:
        kt_s[row, h, :QK] = k_s[row, h, :, :QK].T
    place_do(col)
    lax.fori_loop(0, GROUP, clear, 0)

    def diagonal_half(ks, qs):
        return jnp.where((ks < row) | ((ks == row) & (col <= qs)), 0, 1)

    def two_blocks(ks, qs):
        h = diagonal_half(ks, qs)
        return (ks, qs, 0, 1), (ks, qs, h, h)

    own_blocks = [(row, col, kh, qh) for kh in HALVES for qh in HALVES if kh <= qh]

    def f_blocks(t):
        a, b = GROUP - 1, 0
        end = T_LAST
        for t0, a0, na, b0, nb, inner in RECTS[::-1]:
            u = t - t0
            pa, pb = (a0 + u % na, b0 + u // na) if inner else (a0 + u // nb, b0 + u % nb)
            a, b = jnp.where(t < end, pa, a), jnp.where(t < end, pb, b)
            end = t0
        a = jnp.where(a == FAR, RING, jnp.where(a == RING, FAR, a))
        return two_blocks(col_slot(a), jnp.where(t < T_LAST, row_slot(b), t - T_LAST))

    def f_scores(sc, blk):
        ks, qs, kh, qh = blk
        sc[:] = mm(k_s[ks, kh, :, :QK], qt_s[qs, qh])

    def f_use(sc, blk):
        ks, qs, kh, qh = blk
        s = sc[:]
        if isinstance(kh, int) and kh == qh:
            keys = lax.broadcasted_iota(jnp.int32, s.shape, 0)
            s = jnp.where(keys <= lax.broadcasted_iota(jnp.int32, s.shape, 1), s, NEG_BIG)
        m0 = m_s[qs, qh]
        m1 = jnp.maximum(m0, jnp.max(s, axis=0, keepdims=True))
        p = jnp.exp2((s - m1) * EXP2_SCALE)
        alpha = jnp.exp2((m0 - m1) * EXP2_SCALE)
        l_s[qs, qh] = l_s[qs, qh] * alpha + jnp.sum(p, axis=0, keepdims=True)
        m_s[qs, qh] = m1
        ot_s[qs, qh] = ot_s[qs, qh] * alpha + mm(vt_s[ks, kh, :VAL], p.astype(BF))

    def own_f():
        for blk in own_blocks:
            f_scores(sc0, blk)
            f_use(sc0, blk)

    own_f()

    def stats_copies(slot, n):
        return remote([(st_s.at[slot], st_r.at[slot, col])], st_send.at[slot], st_recv.at[slot], row_dev(n), st_r.at[slot, pl.ds(0, len(PEERS))])

    def make_stats(qs):
        for h in HALVES:
            d = jnp.sum(ot_s[qs, h] * dot_s[qs, h].astype(F32), axis=0, keepdims=True)
            for j in range(BLOCKS):
                c = part(j, LANES)
                for i, v in enumerate((m_s[qs, h, :, c], l_s[qs, h, :, c], d[:, c])):
                    st_s[qs, part(GROUP * i + BLOCKS * h + j, 1)] = v

    def start_stats(qs):
        for n in PEERS:
            start(stats_copies(qs, n))
        st_r[qs, col] = st_s[qs]

    def f_arrive(t):
        @pl.when(among(t, tuple(sorted({*Q_STEPS, *K_STEPS, *DO_STEPS, T_RELAY, T_RELAY_K, T_OWN_DO, T_RELAY_DO}))))
        def _():
            @pl.when(among(t, Q_STEPS))
            def _():
                rank = at(t, Q_STEPS, PEERS)

                @pl.when(rank != RING)
                def _():
                    wait_q(rank)

                @pl.when(rank == 1)
                def _():
                    start(own_copies(*q_kind, TWO))
                place_q(row_slot(rank))

            @pl.when(among(t, K_STEPS))
            def _():
                rank = at(t, K_STEPS, K_RANKS)

                @pl.when(rank != RING)
                def _():
                    wait_k(rank)

                @pl.when(rank == 1)
                def _():
                    start(own_copies(*k_kind, TWO))
                place_k(col_slot(rank))

            @pl.when(among(t, DO_STEPS))
            def _():
                rank = at(t, DO_STEPS, DO_RANKS)
                wait_do(rank)
                place_do(row_slot(rank))

            @pl.when(t == T_RELAY)
            def _():
                wait_q(RING)
                for n in range(FAR):
                    start(pair_copies(*q_kind, n))

            @pl.when(t == T_RELAY_K)
            def _():
                wait_k(RING)
                for n in range(FAR):
                    start(pair_copies(*k_kind, n))

            @pl.when(t == T_OWN_DO)
            def _():
                for n in (*first_copies, TWO):
                    start(own_copies(*do_kind, n))

            @pl.when(t == T_RELAY_DO)
            def _():
                wait_do(RING)
                for n in range(FAR):
                    start(pair_copies(*do_kind, n))
                place_do(row_slot(RING))

    for t in NEIGHBOURS:
        f_arrive(t)
    blocks = f_blocks(jnp.int32(1))
    for sc, blk in zip((sc0, sc1), blocks):
        f_scores(sc, blk)

    def f_half(t, used, made, b1, b2):
        n1, n2 = after = f_blocks(jnp.minimum(t + 1, T_END - 1))
        f_scores(made[0], n1)
        f_use(used[0], b1)
        f_scores(made[1], n2)
        f_use(used[1], b2)

        @pl.when(t >= T_LAST)
        def _():
            @pl.when(t > T_LAST)
            def _():
                start_stats(t - T_LAST - 1)

            make_stats(t - T_LAST)

        f_arrive(t + TWO)
        return after

    def f_step(u, carry):
        t = TWO * u + 1
        after = f_half(t, (sc0, sc1), (dp0, dp1), *carry)

        @pl.when(t < T_END - 1)
        def _():
            f_half(t + 1, (dp0, dp1), (sc0, sc1), *after)
        return f_blocks(jnp.minimum(t + TWO, T_END - 1))

    lax.fori_loop(0, T_END // TWO, f_step, blocks)
    start_stats(GROUP - 1)

    o_all = stg.at[pl.ds(0, TWO * VAL)]

    def o_refs(slot, buf):
        return [(ot_s.at[slot, h], buf.at[pl.ds(h * VAL, VAL)]) for h in HALVES]

    def o_copies(s):
        d = (s // RING) ^ y0
        return remote(o_refs(s, xo.at[d, x]), xo_send.at[s], xo_recv.at[d, x], {'cp': GROUP * row + RING * y0 + s % RING}, o_all)

    def o_pair():
        return remote(o_refs(row_slot(RING), po), po_send.at[0], po_recv.at[0], row_dev(RING), o_all)

    def dq_srcs(s, p):
        r = pl.ds(p * ROWS, ROWS)
        return [dq_s.at[s, 0, r], dq_s.at[s, 1, r], dqr_s.at[s, r]]

    def dq_dsts(buf):
        return [buf.at[:, pl.ds(LANES * j, LANES)] for j in range(3)]

    def kv_srcs(s, h):
        return [dk_s.at[s, h], dv_s.at[s, h]]

    def kv_dsts(buf):
        return [buf.at[pl.ds(0, QK)], buf.at[pl.ds(QK, VAL)]]

    dq_near, dq_far, dq_across = ring_sums(row_slot, row_dev, lambda d, p: RING if d else p + 1, dq_srcs, dq_dsts, (xq, xqv, pq), q_sums_sems, stg.at[pl.ds(0, ROWS * 3 * LANES // HALF)])
    kv_near, kv_far, kv_across = ring_sums(col_slot, col_dev, lambda d, p: p + 1, kv_srcs, kv_dsts, (zkv, zkvv, pkv), kv_sums_sems, stg.at[pl.ds(0, KV)])

    def local(pairs, n=0):
        return [pltpu.make_async_copy(src, dst, loc.at[n + i]) for i, (src, dst) in enumerate(pairs)]

    def o_local(d):
        return local([(xo.at[d, (x + gray(r)) % RING], stg.at[pl.ds(HALF * (r - 1), HALF // TWO)]) for r in range(1, RING)])

    def fetch_o(d):
        for r in range(1, RING):
            s = (x + gray(r)) % RING
            landed(remote(o_refs(0, xo.at[d, s]), xo_send.at[r], xo_recv.at[d, s], row_dev(r), o_all))
        start(o_local(d))

    def add_o(slot, d):
        done(o_local(d))
        for h in HALVES:
            ot_s[slot, h] = ot_s[slot, h] + sum(stg[HALF * n + h * VAL:HALF * n + (h + 1) * VAL] for n in range(FAR))

    def kv_local(d, h):
        return local([(zkv.at[d, n, h], stg.at[pl.ds(KV * (TWO * h + n), KV)]) for n in HALVES], TWO * h)

    def fetch_kv(d, h):
        for r in NEIGHBOURS:
            landed(kv_near(RING * d + r, h))
        start(kv_local(d, h))

    def add_kv(slot, d, h):
        done(kv_local(d, h))
        u = KV * TWO * h
        v = u + KV
        dk_s[slot, h] = dk_s[slot, h] + (stg[u:u + QK] + stg[v:v + QK])
        dv_s[slot, h] = dv_s[slot, h] + (stg[u + QK:v] + stg[v + QK:v + KV])

    def kv_via_local(d):
        return local([(zkvv.at[d, h], stg.at[pl.ds(KV * h, KV)]) for h in HALVES])

    def fetch_kv_via(d):
        for h in HALVES:
            landed(kv_far(d, h))
        start(kv_via_local(d))

    def add_kv_via(d):
        done(kv_via_local(d))
        for h in HALVES:
            slot, u = col_slot(RING * d + 1 + h), KV * h
            dk_s[slot, h] = dk_s[slot, h] + stg[u:u + QK]
            dv_s[slot, h] = dv_s[slot, h] + stg[u + QK:u + KV]

    def dq_stage(n, p):
        return stg.at[pl.ds(HALF * n + ROWS * p, ROWS), pl.ds(0, 3 * LANES)]

    def add_dq(slot, p, ns):
        r = part(p, ROWS)
        for j in range(3):
            c = part(j, LANES)
            total = sum(stg[HALF * n + ROWS * p:HALF * n + ROWS * (p + 1), c] for n in ns)
            if j < TWO:
                dq_s[slot, j, r] = dq_s[slot, j, r] + total
            else:
                dqr_s[slot, r] = dqr_s[slot, r] + total

    def sum_dq_via(d):
        for p in HALVES:
            landed(dq_far(d, p))
        copies = local([(xqv.at[d, p], dq_stage(0, p)) for p in HALVES])
        start(copies)
        done(copies)
        for p in HALVES:
            add_dq(row_slot(FAR if d else 1 + p), p, (0,))

    def dq_arrived(d):
        for p in HALVES:
            for r in NEIGHBOURS:
                landed(dq_near(RING * d + r, p))
        return [(xq.at[d, n, p], dq_stage(n, p)) for n in HALVES for p in HALVES]

    def columns(v):
        flat = jnp.concatenate([v[part(j, 1)] for j in range(BLOCKS)], axis=1)
        hi = flat.astype(BF).astype(F32)
        mid = (flat - hi).astype(BF).astype(F32)
        return jnp.concatenate([hi, mid, flat - hi - mid, jnp.zeros((AUG - 3, HALF), F32)], axis=0).T.astype(BF)

    def wait_stats(qs):
        landed(stats_copies(qs, 1))

    def prepare_two(qs):
        for n in HALVES:
            wait_stats(qs + n)
        for n in HALVES:
            prepare(qs + n)

    def prepare(qs):
        m, l, d = (st_r[qs, :, part(i, GROUP)] for i in range(3))
        m_all = jnp.max(m, axis=0)
        w = jnp.exp2((m - m_all[None]) * EXP2_SCALE)
        l_all = jnp.sum(w * l, axis=0)
        inv = 1.0 / l_all
        delta = jnp.sum(w * d, axis=0) * inv
        lse = m_all + jnp.log2(l_all) * (1.0 / EXP2_SCALE)
        mine = jnp.exp2((st_s[qs, :GROUP] - m_all) * EXP2_SCALE) * inv
        for h in HALVES:
            q_s[qs, h, :, QK:] = columns(-lse[part(h, BLOCKS)])
            do_s[qs, h, :, VAL:] = columns(-delta[part(h, BLOCKS)])
            for j in range(BLOCKS):
                c = part(j, LANES)
                ot_s[qs, h, :, c] = ot_s[qs, h, :, c] * mine[part(BLOCKS * h + j, 1)]

    def b_mixed(m):
        first, rest = m < M_REST, m < M_OWN
        rank = jnp.where(first, order(m // 3, Q_FIRST), order(jnp.where(rest, m - M_REST, (m - M_OWN) // TWO), Q_REST))
        ring = jnp.where(first, m % 3, jnp.where(rest, 0, 1)) == 0
        same = ring | (jnp.where(first, m % 3, 1 + m % TWO) == TWO)
        ks, qs = jnp.where(ring, col_slot(K_ORDER[-1]), row), row_slot(rank)
        h = diagonal_half(ks, qs)
        return ks, qs, jnp.where(same, h, 0), jnp.where(same, h, 1)

    def b_blocks(t):
        b1, b2 = two_blocks(col_slot(order(t // GROUP, K_ORDER)), t % GROUP)
        pick = lambda c, a, b: tuple(jnp.where(c, i, j) for i, j in zip(a, b))
        last = col_slot(K_ORDER[-1])
        u = TWO * (t - T_SPLIT)
        m = TWO * (t - T_MIX)
        return tuple(pick(t < T_SPLIT, b, pick(t < T_MIX, (last, u + n, 0, 1), b_mixed(m + n))) for n, b in enumerate((b1, b2)))

    def b_scores(sc, dp, blk):
        ks, qs, kh, qh = blk
        sc[:] = mm(q_s[qs, qh], kt_s[ks, kh])
        dp[:] = mm(do_s[qs, qh], vt_s[ks, kh])

    def b_elem(sc, dp, pr, ds, mask=False):
        p = jnp.exp2(sc[:] * EXP2_SCALE)
        if mask:
            rows = lax.broadcasted_iota(jnp.int32, p.shape, 0)
            p = jnp.where(lax.broadcasted_iota(jnp.int32, p.shape, 1) <= rows, p, 0.0)
        pr[:] = p.astype(BF)
        ds[:] = (p * dp[:]).astype(BF)

    def b_grads(pr, ds, blk):
        ks, qs, kh, qh = blk
        p = pr[:]
        g = ds[:]
        dv_s[ks, kh] += mm(dot_s[qs, qh], p)
        dk_s[ks, kh] += mm(qt_s[qs, qh], g)
        dq = mm(g, k_s[ks, kh])
        dq_s[qs, qh] += dq[:, :NOPE]
        side = lax.broadcasted_iota(jnp.int32, (1, LANES), 1) // ROPE
        dqr_s[qs] += jnp.where(side == qh, dq[:, NOPE:], 0.0)

    early_half = 1 - diagonal_half(col_slot(K_ORDER[-1]), 0)

    def b_events(t):
        @pl.when((t <= GROUP) | among(t, (*T_VIA, *T_FETCH, *T_ADD, *T_NEAR, *T_ONE, T_NEAR_MID, T_NEAR_LAST, T_PAIR_O - 1, T_PAIR_O, T_PAIR_O + 1, T_VIA_Q, T_Q_FIVE, T_Q_SIX)) | among(t, tuple(v + i for v in T_PAIR_KV for i in range(3))))
        def _():
            @pl.when((t < GROUP - 1) & (t % TWO == 1))
            def _():
                prepare_two(t + 1)

            @pl.when((t <= GROUP) & ((t - 1) % RING != x))
            def _():
                start(o_copies(t - 1))

            @pl.when(among(t, T_VIA))
            def _():
                for h in HALVES:
                    start(kv_far(at(t, T_VIA, (1, 0)), h))

            @pl.when(among(t, T_FETCH))
            def _():
                fetch_kv_via(at(t, T_FETCH, (1, 0)))

            @pl.when(among(t, T_ADD))
            def _():
                add_kv_via(at(t, T_ADD, (1, 0)))

            @pl.when(among(t, T_NEAR))
            def _():
                for h in HALVES:
                    start(kv_near(at(t, T_NEAR, NEAR), h))

            @pl.when(among(t, T_ONE))
            def _():
                start(kv_near(1, at(t, T_ONE, (1, 0))))

            @pl.when(t == T_NEAR_MID)
            def _():
                start(kv_near(K_ORDER[-1], early_half))

            @pl.when(t == T_NEAR_LAST)
            def _():
                start(kv_near(K_ORDER[-1], 1 - early_half))

            @pl.when(t == T_VIA_Q)
            def _():
                for p in HALVES:
                    start(dq_far(1, p))

            @pl.when(t == T_Q_FIVE)
            def _():
                start(dq_near(5, 0) + dq_near(5, 1))

            @pl.when(t == T_Q_SIX)
            def _():
                start(dq_near(6, 0) + dq_near(6, 1))

            @pl.when(t == T_PAIR_O - 1)
            def _():
                fetch_o(1)

            @pl.when(t == T_PAIR_O)
            def _():
                add_o(row_slot(RING), 1)

            @pl.when(t == T_PAIR_O + 1)
            def _():
                start(o_pair())

            for h, v in enumerate(T_PAIR_KV):
                @pl.when(t == v)
                def _():
                    fetch_kv(1, h)

                @pl.when(t == v + 1)
                def _():
                    add_kv(col_slot(RING), 1, h)

                @pl.when(t == v + TWO)
                def _():
                    start(kv_across(h))

    def b_step(t, carry):
        before, (b1, b2) = carry
        after = b_blocks(jnp.minimum(t + 1, T_END - TWO))
        b_scores(sc1, dp1, b2)
        b_elem(sc0, dp0, pr0, ds0)
        b_grads(pr1, ds1, before)
        b_scores(sc0, dp0, after[0])
        b_elem(sc1, dp1, pr1, ds1)
        b_grads(pr0, ds0, b1)
        b_events(t + 1)
        return b2, after

    for ref in (pr1, ds1):
        ref[:] = jnp.zeros(ref.shape, BF)
    prepare_two(0)
    blocks = b_blocks(jnp.int32(0))
    b_scores(sc0, dp0, blocks[0])
    before, _ = lax.fori_loop(0, T_END - 1, b_step, (blocks[1], blocks))
    b_grads(pr1, ds1, before)

    def own_b():
        for blk in own_blocks:
            b_scores(sc0, dp0, blk)
            b_elem(sc0, dp0, pr0, ds0, mask=blk[TWO] == blk[3])
            b_grads(pr0, ds0, blk)

    own_b()

    def finish_o():
        fetch_o(0)
        add_o(col, 0)
        landed(o_pair())
        last_o = local([(po, stg.at[pl.ds(HALF // TWO, HALF // TWO)])])
        start(last_o)
        for n in range(RING):
            left(own_copies(*do_kind, n))
        done(last_o)
        for h in HALVES:
            do_s[col, h, :, :VAL] = (ot_s[col, h] + stg[part(TWO + h, VAL)]).T.astype(BF)

    sum_dq_via(1)
    start(dq_far(0, 0) + dq_far(0, 1) + dq_near(1, 1) + dq_near(2, 0))
    for pr, h in zip((pr0, pr1), HALVES):
        pr[:] = c_in[h].T

    def finish_dq_pair():
        copies = local(dq_arrived(1))
        start(copies)
        done(copies)
        for p in HALVES:
            add_dq(row_slot(RING), p, HALVES)

    finish_dq_pair()
    start(dq_across(0))

    def finish_dkv():
        sums = None
        pair = local([(pkv.at[h], sc.at[pl.ds(0, KV)]) for h, sc in enumerate((sc0, sc1))], RING)
        for h in HALVES:
            landed(kv_across(h))
        start(pair)
        for h in HALVES:
            fetch_kv(0, h)
        done(pair)
        for h, sc in enumerate((sc0, sc1)):
            add_kv(row, 0, h)
            dk = (dk_s[row, h] + sc[:QK]) * SCALE
            dv = dv_s[row, h] + sc[QK:KV]
            rope_s[:, part(h, HALF)] = dk[NOPE:]
            kv = jnp.concatenate([dk[:NOPE].T, dv.T], axis=1)
            (dp0, dp1)[h][:, :NOPE + VAL] = kv
            product = mm((pr0, pr1)[h][:].astype(F32), kv)
            sums = product if sums is None else sums + product
        w_s[0] = sums[:, :NOPE]
        w_s[1] = sums[:, NOPE:]

    finish_dkv()

    def w_swap(src, dst, n):
        return remote([(src, dst)], w_send.at[n], w_recv.at[n], mate, src)

    def strip(d):
        return rows_of(d, STRIP)

    def to_all(n, src, dst):
        to_others(lambda d: pltpu.make_async_remote_copy(src(d), dst, strip_send.at[n], strip_recv.at[n], device_id={'cp': d}).start())

    def all_of(sem, n):
        strips = wr_r.at[pl.ds(0, CHIPS - 1)]
        pltpu.make_async_copy(strips, strips, sem.at[n]).wait()

    first = w_swap(w_s.at[1 - core], ws_r, 0)
    start(first)

    def left_early():
        left(stats_copies(0, 1))
        for r in PEERS:
            left(stats_copies(r, 1))
            if r != RING:
                left(o_copies(row_slot(r)))
            if r % RING in NEIGHBOURS:
                for p in HALVES:
                    left(kv_near(r, p))
        for p in HALVES:
            left(kv_across(p) + dq_far(1, p))
            for r in NEIGHBOURS:
                left(dq_near(RING + r, p))
            for d in HALVES:
                left(kv_far(d, p))
        left(o_pair())
        for n in range(RING):
            left(own_copies(*q_kind, n) + own_copies(*k_kind, n))
        for n in range(FAR):
            left(pair_copies(*q_kind, n) + pair_copies(*k_kind, n) + pair_copies(*do_kind, n))

    def finish_c():
        w_all = jnp.concatenate([wk_in[:], wv_in[:]], axis=1).astype(F32)
        for kv, out in ((dp0, sc0), (dp1, sc1)):
            out[:] = mm_t(kv[:, :NOPE + VAL], w_all)

    finish_c()
    outputs = [(sc0, out_c.at[0]), (sc1, out_c.at[1]), (rope_s, out_r)]
    more = [pltpu.make_async_copy(src, dst, outs.at[1 + n]) for n, (src, dst) in enumerate(outputs)]
    start(more)
    finals = more

    def w_one():
        landed(first)
        wr_s[:] = w_s[core] + ws_r[:]

    w_one()
    to_all(0, lambda d: wr_s.at[strip(d)], wr_r.at[me])
    start(dq_across(1))
    wr_r[me] = wr_s[strip(me)]
    sum_dq_via(0)
    start(dq_near(1, 0) + dq_near(2, 1))
    finish_o()
    o_out = [pltpu.make_async_copy(do_s.at[col, :, :, :VAL], out_o, outs.at[0])]
    start(o_out)
    finals += o_out
    left(first)

    left_early()

    def w_two():
        all_of(strip_recv, 0)
        w_s[core, strip(me)] = jnp.sum(wr_r[:], axis=0)

    w_two()
    mine = w_s.at[core, strip(me)]
    to_all(1, lambda d: mine, mine)

    def w_three():
        all_of(strip_recv, 1)

    w_three()
    last = w_swap(w_s.at[core], wl_r, 1)
    start(last)

    def finish_dq():
        pairs = dq_arrived(0)
        for p in HALVES:
            landed(dq_across(p))
        copies = local(pairs + [(pq.at[p], dq_stage(TWO, p)) for p in HALVES])
        start(copies)
        done(copies)
        for p in HALVES:
            add_dq(col, p, range(3))
        for h in HALVES:
            q_out_s[:NOPE, part(h, HALF)] = (dq_s[col, h] * SCALE).T
        rope = (dqr_s[col] * SCALE).T
        for h in HALVES:
            q_out_s[NOPE:, part(h, HALF)] = rope[part(h, ROPE)]

    def w_five():
        landed(last)
        w_s[1 - core] = wl_r[:]

    w_five()
    more = [pltpu.make_async_copy(src, dst, outs.at[RING + n]) for n, (src, dst) in enumerate([(w_s.at[0], out_uk), (w_s.at[1], out_uv)])]
    start(more)
    finals += more
    finish_dq()
    q_out = pltpu.make_async_copy(q_out_s, out_q, outs.at[RING + TWO])
    q_out.start()

    def left_late():
        left(last)
        for n in HALVES:
            all_of(strip_send, n)
        for p in HALVES:
            left(dq_across(p) + dq_far(0, p))
            for r in NEIGHBOURS:
                left(dq_near(r, p))

    left_late()

    def out_done():
        done(finals + [q_out])

    out_done()


def core_call(c, kpe, q, wk, wv, do):
    dma = lambda *s: pltpu.SemaphoreType.DMA(s)
    shape = jax.ShapeDtypeStruct
    per = (GROUP, TWO)
    wide = lambda *s: pltpu.VMEM(per + s, BF)
    sums = lambda *s: pltpu.VMEM(per + s, F32)
    f32 = lambda *s: pltpu.VMEM(s, F32)
    packed = pltpu.VMEM((GROUP, HALF, LANES), BF)

    def sum_sems():
        return [dma(*s) for s in ((GROUP, TWO), (TWO, TWO, TWO), (TWO, TWO), (TWO, TWO), (TWO,), (TWO,))]

    def sum_bufs(*s):
        return [shape((TWO, TWO, TWO, *s), F32), shape((TWO, TWO, *s), F32), shape((TWO, *s), F32)]

    square = (HALF, HALF)
    scratch = [pltpu.VMEM(a.shape, a.dtype) for a in (c, kpe, q, wk, wv, do)] + [
        wide(HALF, QK + AUG), packed, wide(HALF, QK + ROPE), packed, wide(VAL + AUG, HALF), wide(HALF, VAL + AUG),
        wide(QK, HALF), wide(QK + AUG, HALF), wide(VAL, HALF),
        sums(VAL, HALF), sums(1, HALF), sums(1, HALF),
        sums(HALF, NOPE), f32(GROUP, HALF, LANES), sums(QK, HALF), sums(VAL, HALF),
        f32(GROUP, 3 * GROUP, LANES), f32(GROUP, GROUP, 3 * GROUP, LANES), f32(3 * HALF, HALF),
        f32(TWO, LATENT, NOPE), f32(LATENT, NOPE), f32(LATENT, NOPE), f32(ROPE, TWO * HALF), f32(QK, TWO * HALF),
        f32(LATENT, NOPE), f32(CHIPS, STRIP, NOPE),
        *[f32(*square)] * RING, *[pltpu.VMEM(square, BF)] * RING,
        *[dma(GROUP)] * GROUP, dma(GROUP), dma(TWO, RING), dma(1), dma(1),
        sum_sems(), sum_sems(), dma(GROUP), dma(GROUP), dma(TWO), dma(TWO), dma(TWO), dma(TWO),
    ]
    results = [
        shape((TWO, HALF, VAL), BF), shape((QK, TWO * HALF), F32), shape((TWO, HALF, LATENT), F32), shape((ROPE, TWO * HALF), F32),
        shape((LATENT, NOPE), F32), shape((LATENT, VAL), F32),
    ]
    landing = [shape((TWO, RING, TWO * VAL, HALF), F32), shape((TWO * VAL, HALF), F32), *sum_bufs(ROWS, 3 * LANES), *sum_bufs(KV, HALF)]
    anywhere = pl.BlockSpec(memory_space=pl.ANY)
    return pl.pallas_call(
        core_kernel,
        out_shape=results + landing,
        in_specs=[anywhere] * 6,
        out_specs=[anywhere] * len(results + landing),
        scratch_shapes=scratch,
        compiler_params=pltpu.CompilerParams(collective_id=0, has_side_effects=True, vmem_limit_bytes=67043328),
        name='core',
    )(c, kpe, q, wk, wv, do)[:len(results)]


def solution(mesh):
    batch = ('pod', 'data')
    token_spec = P(batch, 'cp')
    sum_spec = P('pod')

    def per_device(c_latent, k_rope, queries, w_uk, w_uv, d_out):
        halves = lambda a: a.reshape(TWO, HALF, a.shape[-1])
        o, gq, gc, gr, guk, guv = core_call(halves(c_latent), k_rope[0].T, queries[0, :, 0].T, w_uk[:, 0], w_uv[:, 0], halves(d_out))
        return o.reshape(d_out.shape), gq.T.reshape(queries.shape), gc.reshape(c_latent.shape), gr.T.reshape(k_rope.shape), guk[:, None], guv[:, None]

    return jax.shard_map(per_device, mesh=mesh, in_specs=(token_spec, token_spec, token_spec, P(), P(), token_spec), out_specs=(token_spec, token_spec, token_spec, token_spec, sum_spec, sum_spec), check_vma=False)
```

```python
import jax
import jax.numpy as jnp
from jax import lax
from jax.experimental import pallas as pl
from jax.experimental.pallas import tpu as pltpu
from jax.sharding import PartitionSpec as P

BF = jnp.bfloat16
F32 = jnp.float32
NEG_BIG = -1.0e30
HALF = 512
LATENT = 512
LANES = 128
NOPE = 128
ROPE = 64
QK = NOPE + ROPE
VAL = 128
KV = QK + VAL
AUG = 16
SCALE = QK ** -0.5
EXP2_SCALE = SCALE * 1.4426950408889634
TWO = 2
RING = 4
FAR = RING - 1
GROUP = 8
HALVES = range(TWO)
NEIGHBOURS = (1, 2)
PEERS = range(1, GROUP)
CHIPS = GROUP * GROUP
STRIP = LATENT // CHIPS
ROWS = HALF // TWO
BLOCKS = HALF // LANES
Q_STEPS = (1, 2, 9, 12, 25, 30, 35)
K_STEPS = (3, 6, 15, 20, 40, 48, 56)
DO_STEPS, DO_RANKS = (49, 50, 51, 52, 53, 54), (1, 2, 3, 5, 6, 7)
K_RANKS = (1, 2, 4, 3, 5, 6, 7)
T_RELAY, T_RELAY_K, T_OWN_DO, T_RELAY_DO = 4, 11, 18, 36
T_LAST = 56
T_END = 64
RECTS = ((1, 0, 1, 1, 2, False), (3, 1, 2, 0, 3, False), (9, 0, 3, 3, 2, True), (15, 3, 2, 0, 5, False), (25, 0, 5, 5, 3, True), (40, 5, 2, 0, 8, False))
K_ORDER = (7, 5, 6, 4, 3, 1, 2)
Q_FIRST, Q_REST = (7, 5, 6), (3, 1, 2, 4, 0)
T_MIX = 48
M_NEAR, M_FAR, M_OWN = 12, 17, 22
T_VIA = (9, 41)
T_FETCH, T_ADD = (21, 53), (22, 54)
T_NEAR, NEAR = (23, 25), (5, 6)
T_ONE = (49, 55)
T_NEAR_MID, T_NEAR_LAST = 57, 60
T_PAIR_O = 56
T_PAIR_KV = (36, 45)
T_VIA_Q, T_Q_FIVE, T_Q_SIX = 51, 53, 55


def mm(a, b):
    return jnp.dot(a, b, preferred_element_type=F32)


def mm_t(a, b):
    return lax.dot_general(a, b, (((1,), (1,)), ((), ())), preferred_element_type=F32)


def gray(r):
    return r ^ (r >> 1)


def part(n, size):
    return slice(n * size, (n + 1) * size)


def rows_of(n, size):
    return pl.ds(pl.multiple_of(n * size, size), size)


def order(n, ranks):
    out = ranks[-1]
    for i, r in list(enumerate(ranks))[-2::-1]:
        out = jnp.where(n <= i, r, out)
    return out


def among(t, steps):
    out = t == steps[0]
    for v in steps[1:]:
        out = out | (t == v)
    return out


def at(t, steps, ranks):
    out = ranks[-1]
    for v, r in list(zip(steps, ranks))[-2::-1]:
        out = jnp.where(t <= v, r, out)
    return out


def start(copies):
    for c in copies:
        c.start()


def done(copies):
    for c in copies:
        c.wait()


class Remote:
    def __init__(self, pairs, send, recv, dev, ref):
        self.pairs, self.send, self.recv, self.dev, self.ref = pairs, send, recv, dev, ref

    def start(self):
        for src, dst in self.pairs:
            pltpu.make_async_remote_copy(src, dst, self.send, self.recv, device_id=self.dev).start()

    def wait_recv(self):
        pltpu.make_async_copy(self.ref, self.ref, self.recv).wait()

    def wait_send(self):
        pltpu.make_async_copy(self.ref, self.ref, self.send).wait()


def landed(copies):
    for c in copies:
        c.wait_recv()


def left(copies):
    for c in copies:
        c.wait_send()


def remote(pairs, send, recv, dev, ref):
    return [Remote(pairs, send, recv, dev, ref)]


def ring_sums(slot, dev, far_rank, srcs, dsts, bufs, sems, ref):
    main, via, pair = bufs
    main_send, main_recv, via_send, via_recv, pair_send, pair_recv = sems

    def near(rank, p):
        d, n = rank // RING, rank % RING - 1
        return remote(zip(srcs(slot(rank), p), dsts(main.at[d, n, p])), main_send.at[rank, p], main_recv.at[d, n, p], dev(n + 1), ref)

    def far(d, p):
        return remote(zip(srcs(slot(RING * d + FAR), p), dsts(via.at[d, p])), via_send.at[d, p], via_recv.at[d, p], dev(far_rank(d, p)), ref)

    def across(p):
        return remote(zip(srcs(slot(RING), p), dsts(pair.at[p])), pair_send.at[p], pair_recv.at[p], dev(RING), ref)

    return near, far, across


def core_kernel(c_arg, kpe_arg, q_arg, wk_arg, wv_arg, do_arg,
                out_o, out_q, out_c, out_r, out_w, xo, po, xq, xqv, pq, zkv, zkvv, pkv,
                c_in, kpe_in, q_in, wk_in, wv_in, do_in, q_s, qr_s, k_s, kr_s, vt_s, do_s, qt_s, kt_s, dot_s,
                ot_s, m_s, l_s, dq_s, dqr_s, dk_s, dv_s, st_s, st_r, stg, w_s, ws_r, wl_r, rope_s, q_out_s, wr_s, wr_r,
                sc0, sc1, dp0, dp1, pr0, pr1, ds0, ds1,
                q_send, q_recv, k_send, k_recv, do_send, do_recv, st_send, st_recv, xo_send, xo_recv, po_send, po_recv,
                q_sums_sems, kv_sums_sems, loc, outs, w_send, w_recv, strip_send, strip_recv):
    me = lax.axis_index('cp')
    core = lax.axis_index('data')
    row, col = me // GROUP, me % GROUP
    x, y0 = col % RING, col // RING
    y1, z = row % TWO, row // TWO

    def row_slot(rank):
        return RING * (y0 ^ (rank // RING)) + (x + gray(rank % RING)) % RING

    def col_slot(rank):
        return TWO * ((z + gray(rank % RING)) % RING) + (y1 ^ (rank // RING))

    def row_dev(rank):
        return {'cp': GROUP * row + row_slot(rank)}

    def col_dev(rank):
        return {'cp': GROUP * col_slot(rank) + col}

    args = [pltpu.make_async_copy(src, dst, loc.at[n]) for n, (src, dst) in enumerate(((q_arg, q_in), (do_arg, do_in), (kpe_arg, kpe_in), (wv_arg, wv_in), (wk_arg, wk_in), (c_arg, c_in)))]
    start(args)
    mate = {'data': 1 - core}
    barrier = pltpu.get_barrier_semaphore()

    def to_others(act):
        def one(n, carry):
            act((me + n) % CHIPS)
            return carry

        lax.fori_loop(1, CHIPS, one, 0)

    to_others(lambda d: pl.semaphore_signal(barrier, inc=1, device_id={'cp': d}))
    pl.semaphore_signal(barrier, inc=1, device_id=mate)

    done(args)
    wvt = wv_in[:].T
    for h in HALVES:
        q = q_in[:, part(h, HALF)]
        qt_s[col, h] = q
        q_s[col, h, :, :QK] = q.T
        qr_s[col, :, part(h, ROPE)] = q[NOPE:].T
        do_s[col, h, :, :VAL] = do_in[h]
    for h in HALVES:
        k_s[row, h, :, :NOPE] = mm(c_in[h], wk_in[:]).astype(BF)
        rope = kpe_in[:, part(h, HALF)].T
        k_s[row, h, :, NOPE:] = jnp.concatenate([rope, rope], axis=1)
        kr_s[row, :, part(h, ROPE)] = rope
        vt_s[row, h, :VAL] = mm_t(wvt, c_in[h]).astype(BF)

    pl.semaphore_wait(barrier, CHIPS)

    def like(n):
        return qr_s.at[pl.ds(0, n)]

    def q_copies(n, slot, dev):
        refs = [q_s.at[slot, :, :, :NOPE], qr_s.at[slot]]
        return remote(zip(refs, refs), q_send.at[n], q_recv.at[slot], dev, like(3))

    def k_copies(n, slot, dev):
        refs = [k_s.at[slot, :, :, :NOPE], kr_s.at[slot], vt_s.at[slot, :, :VAL]]
        return remote(zip(refs, refs), k_send.at[n], k_recv.at[slot], dev, like(5))

    def do_copies(n, slot, dev):
        ref = do_s.at[slot, :, :, :VAL]
        return remote([(ref, ref)], do_send.at[n], do_recv.at[slot], dev, like(TWO))

    first_copies = (FAR, 0, 1)

    def own_copies(copies, slot, dev, n):
        return copies(n, slot(0), dev(n + 1))

    def pair_copies(copies, slot, dev, n):
        return copies(RING + n, slot(RING), dev(n + 1))

    q_kind, k_kind, do_kind = (q_copies, row_slot, row_dev), (k_copies, col_slot, col_dev), (do_copies, row_slot, row_dev)

    for n in first_copies:
        start(own_copies(*q_kind, n))
        start(own_copies(*k_kind, n))

    def arrived(copies, slot, dev, rank):
        landed(copies(0, slot(rank), dev(1)))

    def wait_q(rank):
        arrived(*q_kind, rank)

    def wait_k(rank):
        arrived(*k_kind, rank)

    def wait_do(rank):
        arrived(*do_kind, rank)

    ones = jnp.where(lax.broadcasted_iota(jnp.int32, (AUG, HALF), 0) < 3, 1.0, 0.0).astype(BF)

    def clear(s, carry):
        for h in HALVES:
            for ref in (ot_s, dq_s, dk_s, dv_s, l_s):
                ref[s, h] = jnp.zeros(ref.shape[TWO:], F32)
            m_s[s, h] = jnp.full(m_s.shape[TWO:], NEG_BIG, F32)
            kt_s[s, h, QK:] = ones
            vt_s[s, h, VAL:] = ones
        dqr_s[s] = jnp.zeros((HALF, LANES), F32)
        return carry

    def place_q(s):
        for h in HALVES:
            q_s[s, h, :, NOPE:QK] = qr_s[s, :, part(h, ROPE)]
            qt_s[s, h] = q_s[s, h, :, :QK].T

    def place_k(s):
        for h in HALVES:
            rope = kr_s[s, :, part(h, ROPE)]
            k_s[s, h, :, NOPE:] = jnp.concatenate([rope, rope], axis=1)
            kt_s[s, h, :QK] = k_s[s, h, :, :QK].T

    def place_do(s):
        for h in HALVES:
            dot_s[s, h] = do_s[s, h, :, :VAL].T

    for h in HALVES:
        kt_s[row, h, :QK] = k_s[row, h, :, :QK].T
    place_do(col)
    lax.fori_loop(0, GROUP, clear, 0)

    def diagonal_half(ks, qs):
        return jnp.where((ks < row) | ((ks == row) & (col <= qs)), 0, 1)

    def two_blocks(ks, qs):
        h = diagonal_half(ks, qs)
        return (ks, qs, 0, 1), (ks, qs, h, h)

    own_blocks = [(row, col, kh, qh) for kh in HALVES for qh in HALVES if kh <= qh]

    def f_blocks(t):
        a, b = GROUP - 1, 0
        end = T_LAST
        for t0, a0, na, b0, nb, inner in RECTS[::-1]:
            u = t - t0
            pa, pb = (a0 + u % na, b0 + u // na) if inner else (a0 + u // nb, b0 + u % nb)
            a, b = jnp.where(t < end, pa, a), jnp.where(t < end, pb, b)
            end = t0
        a = jnp.where(a == FAR, RING, jnp.where(a == RING, FAR, a))
        return two_blocks(col_slot(a), jnp.where(t < T_LAST, row_slot(b), t - T_LAST))

    def f_scores(sc, blk):
        ks, qs, kh, qh = blk
        sc[:] = mm(k_s[ks, kh, :, :QK], qt_s[qs, qh])

    def f_use(sc, blk):
        ks, qs, kh, qh = blk
        s = sc[:]
        if isinstance(kh, int) and kh == qh:
            keys = lax.broadcasted_iota(jnp.int32, s.shape, 0)
            s = jnp.where(keys <= lax.broadcasted_iota(jnp.int32, s.shape, 1), s, NEG_BIG)
        m0 = m_s[qs, qh]
        m1 = jnp.maximum(m0, jnp.max(s, axis=0, keepdims=True))
        p = jnp.exp2((s - m1) * EXP2_SCALE)
        alpha = jnp.exp2((m0 - m1) * EXP2_SCALE)
        l_s[qs, qh] = l_s[qs, qh] * alpha + jnp.sum(p, axis=0, keepdims=True)
        m_s[qs, qh] = m1
        ot_s[qs, qh] = ot_s[qs, qh] * alpha + mm(vt_s[ks, kh, :VAL], p.astype(BF))

    def own_f():
        for blk in own_blocks:
            f_scores(sc0, blk)
            f_use(sc0, blk)

    own_f()

    def stats_copies(slot, n):
        return remote([(st_s.at[slot], st_r.at[slot, col])], st_send.at[slot], st_recv.at[slot], row_dev(n), st_r.at[slot, pl.ds(0, len(PEERS))])

    def make_stats(qs):
        for h in HALVES:
            d = jnp.sum(ot_s[qs, h] * dot_s[qs, h].astype(F32), axis=0, keepdims=True)
            for j in range(BLOCKS):
                c = part(j, LANES)
                for i, v in enumerate((m_s[qs, h, :, c], l_s[qs, h, :, c], d[:, c])):
                    st_s[qs, part(GROUP * i + BLOCKS * h + j, 1)] = v

    def start_stats(qs):
        for n in PEERS:
            start(stats_copies(qs, n))
        st_r[qs, col] = st_s[qs]

    def f_arrive(t):
        @pl.when(among(t, tuple(sorted({*Q_STEPS, *K_STEPS, *DO_STEPS, T_RELAY, T_RELAY_K, T_OWN_DO, T_RELAY_DO}))))
        def _():
            @pl.when(among(t, Q_STEPS))
            def _():
                rank = at(t, Q_STEPS, PEERS)

                @pl.when(rank != RING)
                def _():
                    wait_q(rank)

                @pl.when(rank == 1)
                def _():
                    start(own_copies(*q_kind, TWO))
                place_q(row_slot(rank))

            @pl.when(among(t, K_STEPS))
            def _():
                rank = at(t, K_STEPS, K_RANKS)

                @pl.when(rank != RING)
                def _():
                    wait_k(rank)

                @pl.when(rank == 1)
                def _():
                    start(own_copies(*k_kind, TWO))
                place_k(col_slot(rank))

            @pl.when(among(t, DO_STEPS))
            def _():
                rank = at(t, DO_STEPS, DO_RANKS)
                wait_do(rank)
                place_do(row_slot(rank))

            @pl.when(t == T_RELAY)
            def _():
                wait_q(RING)
                for n in range(FAR):
                    start(pair_copies(*q_kind, n))

            @pl.when(t == T_RELAY_K)
            def _():
                wait_k(RING)
                for n in range(FAR):
                    start(pair_copies(*k_kind, n))

            @pl.when(t == T_OWN_DO)
            def _():
                for n in (*first_copies, TWO):
                    start(own_copies(*do_kind, n))

            @pl.when(t == T_RELAY_DO)
            def _():
                wait_do(RING)
                for n in range(FAR):
                    start(pair_copies(*do_kind, n))
                place_do(row_slot(RING))

    for t in NEIGHBOURS:
        f_arrive(t)
    blocks = f_blocks(jnp.int32(1))
    for sc, blk in zip((sc0, sc1), blocks):
        f_scores(sc, blk)

    def f_half(t, used, made, b1, b2):
        n1, n2 = after = f_blocks(jnp.minimum(t + 1, T_END - 1))
        f_scores(made[0], n1)
        f_use(used[0], b1)
        f_scores(made[1], n2)
        f_use(used[1], b2)

        @pl.when(t >= T_LAST)
        def _():
            @pl.when(t > T_LAST)
            def _():
                start_stats(t - T_LAST - 1)

            make_stats(t - T_LAST)

        f_arrive(t + TWO)
        return after

    def f_step(u, carry):
        t = TWO * u + 1
        after = f_half(t, (sc0, sc1), (dp0, dp1), *carry)

        @pl.when(t < T_END - 1)
        def _():
            f_half(t + 1, (dp0, dp1), (sc0, sc1), *after)
        return f_blocks(jnp.minimum(t + TWO, T_END - 1))

    lax.fori_loop(0, T_END // TWO, f_step, blocks)
    start_stats(GROUP - 1)

    o_all = stg.at[pl.ds(0, TWO * VAL)]

    def o_refs(slot, buf):
        return [(ot_s.at[slot, h], buf.at[pl.ds(h * VAL, VAL)]) for h in HALVES]

    def o_copies(s):
        d = (s // RING) ^ y0
        return remote(o_refs(s, xo.at[d, x]), xo_send.at[s], xo_recv.at[d, x], {'cp': GROUP * row + RING * y0 + s % RING}, o_all)

    def o_pair():
        return remote(o_refs(row_slot(RING), po), po_send.at[0], po_recv.at[0], row_dev(RING), o_all)

    def dq_srcs(s, p):
        r = pl.ds(p * ROWS, ROWS)
        return [dq_s.at[s, 0, r], dq_s.at[s, 1, r], dqr_s.at[s, r]]

    def dq_dsts(buf):
        return [buf.at[:, pl.ds(LANES * j, LANES)] for j in range(3)]

    def kv_srcs(s, h):
        return [dk_s.at[s, h], dv_s.at[s, h]]

    def kv_dsts(buf):
        return [buf.at[pl.ds(0, QK)], buf.at[pl.ds(QK, VAL)]]

    dq_near, dq_far, dq_across = ring_sums(row_slot, row_dev, lambda d, p: RING if d else p + 1, dq_srcs, dq_dsts, (xq, xqv, pq), q_sums_sems, stg.at[pl.ds(0, ROWS * 3 * LANES // HALF)])
    kv_near, kv_far, kv_across = ring_sums(col_slot, col_dev, lambda d, p: p + 1, kv_srcs, kv_dsts, (zkv, zkvv, pkv), kv_sums_sems, stg.at[pl.ds(0, KV)])

    def local(pairs, n=0):
        return [pltpu.make_async_copy(src, dst, loc.at[n + i]) for i, (src, dst) in enumerate(pairs)]

    def o_local(d):
        return local([(xo.at[d, (x + gray(r)) % RING], stg.at[pl.ds(HALF * (r - 1), HALF // TWO)]) for r in range(1, RING)])

    def fetch_o(d):
        for r in range(1, RING):
            s = (x + gray(r)) % RING
            landed(remote(o_refs(0, xo.at[d, s]), xo_send.at[r], xo_recv.at[d, s], row_dev(r), o_all))
        start(o_local(d))

    def add_o(slot, d):
        done(o_local(d))
        for h in HALVES:
            ot_s[slot, h] = ot_s[slot, h] + sum(stg[HALF * n + h * VAL:HALF * n + (h + 1) * VAL] for n in range(FAR))

    def kv_local(d, h):
        return local([(zkv.at[d, n, h], stg.at[pl.ds(KV * (TWO * h + n), KV)]) for n in HALVES], TWO * h)

    def fetch_kv(d, h):
        for r in NEIGHBOURS:
            landed(kv_near(RING * d + r, h))
        start(kv_local(d, h))

    def add_kv(slot, d, h):
        done(kv_local(d, h))
        u = KV * TWO * h
        v = u + KV
        dk_s[slot, h] = dk_s[slot, h] + (stg[u:u + QK] + stg[v:v + QK])
        dv_s[slot, h] = dv_s[slot, h] + (stg[u + QK:v] + stg[v + QK:v + KV])

    def kv_via_local(d):
        return local([(zkvv.at[d, h], stg.at[pl.ds(KV * h, KV)]) for h in HALVES])

    def fetch_kv_via(d):
        for h in HALVES:
            landed(kv_far(d, h))
        start(kv_via_local(d))

    def add_kv_via(d):
        done(kv_via_local(d))
        for h in HALVES:
            slot, u = col_slot(RING * d + 1 + h), KV * h
            dk_s[slot, h] = dk_s[slot, h] + stg[u:u + QK]
            dv_s[slot, h] = dv_s[slot, h] + stg[u + QK:u + KV]

    def dq_stage(n, p):
        return stg.at[pl.ds(HALF * n + ROWS * p, ROWS), pl.ds(0, 3 * LANES)]

    def add_dq(slot, p, ns):
        r = part(p, ROWS)
        for j in range(3):
            c = part(j, LANES)
            total = sum(stg[HALF * n + ROWS * p:HALF * n + ROWS * (p + 1), c] for n in ns)
            if j < TWO:
                dq_s[slot, j, r] = dq_s[slot, j, r] + total
            else:
                dqr_s[slot, r] = dqr_s[slot, r] + total

    def sum_dq_via(d):
        for p in HALVES:
            landed(dq_far(d, p))
        copies = local([(xqv.at[d, p], dq_stage(0, p)) for p in HALVES])
        start(copies)
        done(copies)
        for p in HALVES:
            add_dq(row_slot(FAR if d else 1 + p), p, (0,))

    def dq_arrived(d):
        for p in HALVES:
            for r in NEIGHBOURS:
                landed(dq_near(RING * d + r, p))
        return [(xq.at[d, n, p], dq_stage(n, p)) for n in HALVES for p in HALVES]

    def columns(v):
        flat = jnp.concatenate([v[part(j, 1)] for j in range(BLOCKS)], axis=1)
        hi = flat.astype(BF).astype(F32)
        mid = (flat - hi).astype(BF).astype(F32)
        return jnp.concatenate([hi, mid, flat - hi - mid, jnp.zeros((AUG - 3, HALF), F32)], axis=0).T.astype(BF)

    def wait_stats(qs):
        landed(stats_copies(qs, 1))

    def prepare_two(qs):
        for n in HALVES:
            wait_stats(qs + n)
        for n in HALVES:
            prepare(qs + n)

    def prepare(qs):
        m, l, d = (st_r[qs, :, part(i, GROUP)] for i in range(3))
        m_all = jnp.max(m, axis=0)
        w = jnp.exp2((m - m_all[None]) * EXP2_SCALE)
        l_all = jnp.sum(w * l, axis=0)
        inv = 1.0 / l_all
        delta = jnp.sum(w * d, axis=0) * inv
        lse = m_all + jnp.log2(l_all) * (1.0 / EXP2_SCALE)
        mine = jnp.exp2((st_s[qs, :GROUP] - m_all) * EXP2_SCALE) * inv
        for h in HALVES:
            q_s[qs, h, :, QK:] = columns(-lse[part(h, BLOCKS)])
            do_s[qs, h, :, VAL:] = columns(-delta[part(h, BLOCKS)])
            for j in range(BLOCKS):
                c = part(j, LANES)
                ot_s[qs, h, :, c] = ot_s[qs, h, :, c] * mine[part(BLOCKS * h + j, 1)]

    def b_mixed(m):
        first, near, far = m < M_NEAR, m < M_FAR, m < M_OWN
        rest = jnp.where(near, m - M_NEAR, jnp.where(far, m - M_FAR, (m - M_OWN) // TWO))
        qs = row_slot(jnp.where(first, order(m // RING, Q_FIRST), order(rest, Q_REST)))
        kind = jnp.where(first, m % RING, jnp.where(near, 0, jnp.where(far, 1, TWO + m % TWO)))
        ks = jnp.where(kind < TWO, col_slot(K_ORDER[-1]), row)
        same = kind % TWO == 1
        h = diagonal_half(ks, qs)
        return ks, qs, jnp.where(same, h, 0), jnp.where(same, h, 1)

    def b_blocks(t):
        pick = lambda a, b: tuple(jnp.where(t < T_MIX, i, j) for i, j in zip(a, b))
        plain = two_blocks(col_slot(order(t // GROUP, K_ORDER)), t % GROUP)
        return tuple(pick(b, b_mixed(TWO * (t - T_MIX) + n)) for n, b in enumerate(plain))

    def b_scores(sc, dp, blk):
        ks, qs, kh, qh = blk
        sc[:] = mm(q_s[qs, qh], kt_s[ks, kh])
        dp[:] = mm(do_s[qs, qh], vt_s[ks, kh])

    def b_elem(sc, dp, pr, ds, mask=False):
        p = jnp.exp2(sc[:] * EXP2_SCALE)
        if mask:
            rows = lax.broadcasted_iota(jnp.int32, p.shape, 0)
            p = jnp.where(lax.broadcasted_iota(jnp.int32, p.shape, 1) <= rows, p, 0.0)
        pr[:] = p.astype(BF)
        ds[:] = (p * dp[:]).astype(BF)

    def b_grads(pr, ds, blk):
        ks, qs, kh, qh = blk
        p = pr[:]
        g = ds[:]
        dv_s[ks, kh] += mm(dot_s[qs, qh], p)
        dk_s[ks, kh] += mm(qt_s[qs, qh], g)
        dq = mm(g, k_s[ks, kh])
        dq_s[qs, qh] += dq[:, :NOPE]
        side = lax.broadcasted_iota(jnp.int32, (1, LANES), 1) // ROPE
        dqr_s[qs] += jnp.where(side == qh, dq[:, NOPE:], 0.0)

    early_half = 1 - diagonal_half(col_slot(K_ORDER[-1]), 0)

    def b_events(t):
        @pl.when((t <= GROUP) | among(t, (*T_VIA, *T_FETCH, *T_ADD, *T_NEAR, *T_ONE, T_NEAR_MID, T_NEAR_LAST, T_PAIR_O - 1, T_PAIR_O, T_PAIR_O + 1, T_VIA_Q, T_Q_FIVE, T_Q_SIX)) | among(t, tuple(v + i for v in T_PAIR_KV for i in range(3))))
        def _():
            @pl.when((t < GROUP - 1) & (t % TWO == 1))
            def _():
                prepare_two(t + 1)

            @pl.when((t <= GROUP) & ((t - 1) % RING != x))
            def _():
                start(o_copies(t - 1))

            @pl.when(among(t, T_VIA))
            def _():
                for h in HALVES:
                    start(kv_far(at(t, T_VIA, (1, 0)), h))

            @pl.when(among(t, T_FETCH))
            def _():
                fetch_kv_via(at(t, T_FETCH, (1, 0)))

            @pl.when(among(t, T_ADD))
            def _():
                add_kv_via(at(t, T_ADD, (1, 0)))

            @pl.when(among(t, T_NEAR))
            def _():
                for h in HALVES:
                    start(kv_near(at(t, T_NEAR, NEAR), h))

            @pl.when(among(t, T_ONE))
            def _():
                start(kv_near(1, at(t, T_ONE, (1, 0))))

            @pl.when(t == T_NEAR_MID)
            def _():
                start(kv_near(K_ORDER[-1], early_half))

            @pl.when(t == T_NEAR_LAST)
            def _():
                start(kv_near(K_ORDER[-1], 1 - early_half))

            @pl.when(t == T_VIA_Q)
            def _():
                for p in HALVES:
                    start(dq_far(1, p))

            @pl.when(t == T_Q_FIVE)
            def _():
                start(dq_near(5, 0) + dq_near(5, 1))

            @pl.when(t == T_Q_SIX)
            def _():
                start(dq_near(6, 0) + dq_near(6, 1))

            @pl.when(t == T_PAIR_O - 1)
            def _():
                fetch_o(1)

            @pl.when(t == T_PAIR_O)
            def _():
                add_o(row_slot(RING), 1)

            @pl.when(t == T_PAIR_O + 1)
            def _():
                start(o_pair())

            for h, v in enumerate(T_PAIR_KV):
                @pl.when(t == v)
                def _():
                    fetch_kv(1, h)

                @pl.when(t == v + 1)
                def _():
                    add_kv(col_slot(RING), 1, h)

                @pl.when(t == v + TWO)
                def _():
                    start(kv_across(h))

    def b_step(t, carry):
        before, (b1, b2) = carry
        after = b_blocks(jnp.minimum(t + 1, T_END - TWO))
        b_scores(sc1, dp1, b2)
        b_elem(sc0, dp0, pr0, ds0)
        b_grads(pr1, ds1, before)
        b_scores(sc0, dp0, after[0])
        b_elem(sc1, dp1, pr1, ds1)
        b_grads(pr0, ds0, b1)
        b_events(t + 1)
        return b2, after

    for ref in (pr1, ds1):
        ref[:] = jnp.zeros(ref.shape, BF)
    prepare_two(0)
    blocks = b_blocks(jnp.int32(0))
    b_scores(sc0, dp0, blocks[0])
    before, _ = lax.fori_loop(0, T_END - 1, b_step, (blocks[1], blocks))
    start(dq_near(1, 1) + dq_near(2, 0))
    b_grads(pr1, ds1, before)

    def own_b():
        for blk in own_blocks:
            b_scores(sc0, dp0, blk)
            b_elem(sc0, dp0, pr0, ds0, mask=blk[TWO] == blk[3])
            b_grads(pr0, ds0, blk)

    own_b()

    def finish_o():
        fetch_o(0)
        add_o(col, 0)
        landed(o_pair())
        last_o = local([(po, stg.at[pl.ds(HALF // TWO, HALF // TWO)])])
        start(last_o)
        for n in range(RING):
            left(own_copies(*do_kind, n))
        done(last_o)
        for h in HALVES:
            do_s[col, h, :, :VAL] = (ot_s[col, h] + stg[part(TWO + h, VAL)]).T.astype(BF)

    sum_dq_via(1)
    start(dq_far(0, 0) + dq_far(0, 1))
    for pr, h in zip((pr0, pr1), HALVES):
        pr[:] = c_in[h].T

    def finish_dq_pair():
        copies = local(dq_arrived(1))
        start(copies)
        done(copies)
        for p in HALVES:
            add_dq(row_slot(RING), p, HALVES)

    finish_dq_pair()
    start(dq_across(0))

    def finish_dkv():
        sums = None
        pair = local([(pkv.at[h], sc.at[pl.ds(0, KV)]) for h, sc in enumerate((sc0, sc1))], RING)
        for h in HALVES:
            landed(kv_across(h))
        start(pair)
        for h in HALVES:
            fetch_kv(0, h)
        done(pair)
        for h, sc in enumerate((sc0, sc1)):
            add_kv(row, 0, h)
            dk = (dk_s[row, h] + sc[:QK]) * SCALE
            dv = dv_s[row, h] + sc[QK:KV]
            rope_s[:, part(h, HALF)] = dk[NOPE:]
            kv = jnp.concatenate([dk[:NOPE].T, dv.T], axis=1)
            (dp0, dp1)[h][:, :NOPE + VAL] = kv
            product = mm((pr0, pr1)[h][:].astype(F32), kv)
            sums = product if sums is None else sums + product
        w_s[0] = sums[:, :NOPE]
        w_s[1] = sums[:, NOPE:]

    finish_dkv()

    def w_swap(src, dst, n):
        return remote([(src, dst)], w_send.at[n], w_recv.at[n], mate, src)

    def strip(d):
        return rows_of(d, STRIP)

    def to_all(n, src, dst):
        to_others(lambda d: pltpu.make_async_remote_copy(src(d), dst, strip_send.at[n], strip_recv.at[n], device_id={'cp': d}).start())

    def all_of(sem, n):
        strips = wr_r.at[pl.ds(0, CHIPS - 1)]
        pltpu.make_async_copy(strips, strips, sem.at[n]).wait()

    first = w_swap(w_s.at[1 - core], ws_r, 0)
    start(first)

    def left_early():
        left(stats_copies(0, 1))
        for r in PEERS:
            left(stats_copies(r, 1))
            if r != RING:
                left(o_copies(row_slot(r)))
            if r % RING in NEIGHBOURS:
                for p in HALVES:
                    left(kv_near(r, p))
        for p in HALVES:
            left(kv_across(p) + dq_far(1, p))
            for r in NEIGHBOURS:
                left(dq_near(RING + r, p))
            for d in HALVES:
                left(kv_far(d, p))
        left(o_pair())
        for n in range(RING):
            left(own_copies(*q_kind, n) + own_copies(*k_kind, n))
        for n in range(FAR):
            left(pair_copies(*q_kind, n) + pair_copies(*k_kind, n) + pair_copies(*do_kind, n))

    def finish_c():
        w_all = jnp.concatenate([wk_in[:], wv_in[:]], axis=1).astype(F32)
        for kv, out in ((dp0, sc0), (dp1, sc1)):
            out[:] = mm_t(kv[:, :NOPE + VAL], w_all)

    def w_one():
        landed(first)
        wr_s[:] = w_s[core] + ws_r[:]

    w_one()
    to_all(0, lambda d: wr_s.at[strip(d)], wr_r.at[me])
    start(dq_across(1))
    wr_r[me] = wr_s[strip(me)]
    sum_dq_via(0)
    start(dq_near(1, 0) + dq_near(2, 1))
    finish_o()
    finish_c()
    outputs = [(do_s.at[col, :, :, :VAL], out_o), (sc0, out_c.at[0]), (sc1, out_c.at[1]), (rope_s, out_r)]
    finals = [pltpu.make_async_copy(src, dst, outs.at[n]) for n, (src, dst) in enumerate(outputs)]
    start(finals)
    left(first)

    left_early()

    def w_two():
        all_of(strip_recv, 0)
        w_s[core, strip(me)] = jnp.sum(wr_r[:], axis=0)

    w_two()
    mine = w_s.at[core, strip(me)]
    to_all(1, lambda d: mine, mine)

    def finish_dq():
        pairs = dq_arrived(0)
        for p in HALVES:
            landed(dq_across(p))
        copies = local(pairs + [(pq.at[p], dq_stage(TWO, p)) for p in HALVES])
        start(copies)
        done(copies)
        for p in HALVES:
            add_dq(col, p, range(3))
        for h in HALVES:
            q_out_s[:NOPE, part(h, HALF)] = (dq_s[col, h] * SCALE).T
        rope = (dqr_s[col] * SCALE).T
        for h in HALVES:
            q_out_s[NOPE:, part(h, HALF)] = rope[part(h, ROPE)]

    finish_dq()
    q_out = [pltpu.make_async_copy(q_out_s, out_q, outs.at[RING])]
    start(q_out)

    def w_three():
        all_of(strip_recv, 1)

    w_three()
    last = w_swap(w_s.at[core], wl_r, 1)
    own_w = [pltpu.make_async_copy(w_s.at[core], out_w.at[core], outs.at[RING + 1])]
    start(last + own_w)

    def left_late():
        for n in HALVES:
            all_of(strip_send, n)
        for p in HALVES:
            left(dq_across(p) + dq_far(0, p))
            for r in NEIGHBOURS:
                left(dq_near(r, p))

    left_late()

    def out_done():
        landed(last)
        mate_w = [pltpu.make_async_copy(wl_r, out_w.at[1 - core], outs.at[RING + TWO])]
        start(mate_w)
        left(last)
        done(finals + q_out + own_w + mate_w)

    out_done()


def core_call(c, kpe, q, wk, wv, do):
    dma = lambda *s: pltpu.SemaphoreType.DMA(s)
    shape = jax.ShapeDtypeStruct
    per = (GROUP, TWO)
    wide = lambda *s: pltpu.VMEM(per + s, BF)
    sums = lambda *s: pltpu.VMEM(per + s, F32)
    f32 = lambda *s: pltpu.VMEM(s, F32)
    packed = pltpu.VMEM((GROUP, HALF, LANES), BF)

    def sum_sems():
        return [dma(*s) for s in ((GROUP, TWO), (TWO, TWO, TWO), (TWO, TWO), (TWO, TWO), (TWO,), (TWO,))]

    def sum_bufs(*s):
        return [shape((TWO, TWO, TWO, *s), F32), shape((TWO, TWO, *s), F32), shape((TWO, *s), F32)]

    square = (HALF, HALF)
    scratch = [pltpu.VMEM(a.shape, a.dtype) for a in (c, kpe, q, wk, wv, do)] + [
        wide(HALF, QK + AUG), packed, wide(HALF, QK + ROPE), packed, wide(VAL + AUG, HALF), wide(HALF, VAL + AUG),
        wide(QK, HALF), wide(QK + AUG, HALF), wide(VAL, HALF),
        sums(VAL, HALF), sums(1, HALF), sums(1, HALF),
        sums(HALF, NOPE), f32(GROUP, HALF, LANES), sums(QK, HALF), sums(VAL, HALF),
        f32(GROUP, 3 * GROUP, LANES), f32(GROUP, GROUP, 3 * GROUP, LANES), f32(3 * HALF, HALF),
        f32(TWO, LATENT, NOPE), f32(LATENT, NOPE), f32(LATENT, NOPE), f32(ROPE, TWO * HALF), f32(QK, TWO * HALF),
        f32(LATENT, NOPE), f32(CHIPS, STRIP, NOPE),
        *[f32(*square)] * RING, *[pltpu.VMEM(square, BF)] * RING,
        *[dma(GROUP)] * GROUP, dma(GROUP), dma(TWO, RING), dma(1), dma(1),
        sum_sems(), sum_sems(), dma(GROUP), dma(GROUP), dma(TWO), dma(TWO), dma(TWO), dma(TWO),
    ]
    results = [
        shape((TWO, HALF, VAL), BF), shape((QK, TWO * HALF), F32), shape((TWO, HALF, LATENT), F32), shape((ROPE, TWO * HALF), F32),
        shape((TWO, LATENT, NOPE), F32),
    ]
    landing = [shape((TWO, RING, TWO * VAL, HALF), F32), shape((TWO * VAL, HALF), F32), *sum_bufs(ROWS, 3 * LANES), *sum_bufs(KV, HALF)]
    anywhere = pl.BlockSpec(memory_space=pl.ANY)
    return pl.pallas_call(
        core_kernel,
        out_shape=results + landing,
        in_specs=[anywhere] * 6,
        out_specs=[anywhere] * len(results + landing),
        scratch_shapes=scratch,
        compiler_params=pltpu.CompilerParams(collective_id=0, has_side_effects=True, vmem_limit_bytes=67043328),
        name='core',
    )(c, kpe, q, wk, wv, do)[:len(results)]


def solution(mesh):
    batch = ('pod', 'data')
    token_spec = P(batch, 'cp')
    sum_spec = P('pod')

    def per_device(c_latent, k_rope, queries, w_uk, w_uv, d_out):
        halves = lambda a: a.reshape(TWO, HALF, a.shape[-1])
        o, gq, gc, gr, gw = core_call(halves(c_latent), k_rope[0].T, queries[0, :, 0].T, w_uk[:, 0], w_uv[:, 0], halves(d_out))
        return o.reshape(d_out.shape), gq.T.reshape(queries.shape), gc.reshape(c_latent.shape), gr.T.reshape(k_rope.shape), gw[0, :, None], gw[1, :, None]

    return jax.shard_map(per_device, mesh=mesh, in_specs=(token_spec, token_spec, token_spec, P(), P(), token_spec), out_specs=(token_spec, token_spec, token_spec, token_spec, sum_spec, sum_spec), check_vma=False)
```

```python
import jax
import jax.numpy as jnp
from jax import lax
from jax.experimental import pallas as pl
from jax.experimental.pallas import tpu as pltpu
from jax.sharding import PartitionSpec as P

BF = jnp.bfloat16
F32 = jnp.float32
NEG_BIG = -1.0e30
HALF = 512
LATENT = 512
LANES = 128
NOPE = 128
ROPE = 64
QK = NOPE + ROPE
VAL = 128
KV = QK + VAL
AUG = 16
SCALE = QK ** -0.5
EXP2_SCALE = SCALE * 1.4426950408889634
TWO = 2
RING = 4
FAR = RING - 1
GROUP = 8
HALVES = range(TWO)
NEIGHBOURS = (1, 2)
PEERS = range(1, GROUP)
CHIPS = GROUP * GROUP
STRIP = LATENT // CHIPS
ROWS = HALF // TWO
BLOCKS = HALF // LANES
Q_STEPS = (1, 2, 9, 12, 25, 30, 35)
K_STEPS = (3, 6, 15, 20, 40, 48, 56)
DO_STEPS, DO_RANKS = (49, 50, 51, 52, 53, 54), (1, 2, 3, 5, 6, 7)
K_RANKS = (1, 2, 4, 3, 5, 6, 7)
T_RELAY, T_RELAY_K, T_OWN_DO, T_RELAY_DO = 4, 11, 18, 36
T_LAST = 56
T_END = 64
RECTS = ((1, 0, 1, 1, 2, False), (3, 1, 2, 0, 3, False), (9, 0, 3, 3, 2, True), (15, 3, 2, 0, 5, False), (25, 0, 5, 5, 3, True), (40, 5, 2, 0, 8, False))
K_ORDER = (7, 5, 6, 4, 3, 1, 2)
Q_FIRST, Q_REST = (7, 5, 6), (3, 1, 2, 4, 0)
T_MIX = 48
M_NEAR, M_FAR, M_OWN = 12, 17, 22
T_VIA = (9, 41)
T_FETCH, T_ADD = (21, 53), (22, 54)
T_NEAR, NEAR = (23, 25), (5, 6)
T_ONE = (49, 55)
T_NEAR_MID, T_NEAR_LAST = 57, 60
T_PAIR_O = 56
T_PAIR_KV = (36, 45)
T_VIA_Q, T_Q_FIVE, T_Q_SIX = 51, 53, 55


def mm(a, b):
    return jnp.dot(a, b, preferred_element_type=F32)


def mm_t(a, b):
    return lax.dot_general(a, b, (((1,), (1,)), ((), ())), preferred_element_type=F32)


def gray(r):
    return r ^ (r >> 1)


def part(n, size):
    return slice(n * size, (n + 1) * size)


def rows_of(n, size):
    return pl.ds(pl.multiple_of(n * size, size), size)


def order(n, ranks):
    out = ranks[-1]
    for i, r in list(enumerate(ranks))[-2::-1]:
        out = jnp.where(n <= i, r, out)
    return out


def among(t, steps):
    out = t == steps[0]
    for v in steps[1:]:
        out = out | (t == v)
    return out


def at(t, steps, ranks):
    out = ranks[-1]
    for v, r in list(zip(steps, ranks))[-2::-1]:
        out = jnp.where(t <= v, r, out)
    return out


def start(copies):
    for c in copies:
        c.start()


def done(copies):
    for c in copies:
        c.wait()


class Remote:
    def __init__(self, pairs, send, recv, dev, ref):
        self.pairs, self.send, self.recv, self.dev, self.ref = pairs, send, recv, dev, ref

    def start(self):
        for src, dst in self.pairs:
            pltpu.make_async_remote_copy(src, dst, self.send, self.recv, device_id=self.dev).start()

    def wait_recv(self):
        pltpu.make_async_copy(self.ref, self.ref, self.recv).wait()

    def wait_send(self):
        pltpu.make_async_copy(self.ref, self.ref, self.send).wait()


def landed(copies):
    for c in copies:
        c.wait_recv()


def left(copies):
    for c in copies:
        c.wait_send()


def remote(pairs, send, recv, dev, ref):
    return [Remote(pairs, send, recv, dev, ref)]


def ring_sums(slot, dev, far_rank, srcs, dsts, bufs, sems, ref):
    main, via, pair = bufs
    main_send, main_recv, via_send, via_recv, pair_send, pair_recv = sems

    def near(rank, p):
        d, n = rank // RING, rank % RING - 1
        return remote(zip(srcs(slot(rank), p), dsts(main.at[d, n, p])), main_send.at[rank, p], main_recv.at[d, n, p], dev(n + 1), ref)

    def far(d, p):
        return remote(zip(srcs(slot(RING * d + FAR), p), dsts(via.at[d, p])), via_send.at[d, p], via_recv.at[d, p], dev(far_rank(d, p)), ref)

    def across(p):
        return remote(zip(srcs(slot(RING), p), dsts(pair.at[p])), pair_send.at[p], pair_recv.at[p], dev(RING), ref)

    return near, far, across


def core_kernel(c_arg, kpe_arg, q_arg, wk_arg, wv_arg, do_arg,
                out_o, out_q, out_c, out_r, out_w, xo, po, xq, xqv, pq, zkv, zkvv, pkv,
                c_in, kpe_in, q_in, wk_in, wv_in, do_in, q_s, qr_s, k_s, kr_s, vt_s, do_s, qt_s, kt_s, dot_s,
                ot_s, m_s, l_s, dq_s, dqr_s, dk_s, dv_s, st_s, st_r, stg, w_s, ws_r, wl_r, rope_s, q_out_s, wr_s, wr_r,
                sc0, sc1, dp0, dp1, pr0, pr1, ds0, ds1,
                q_send, q_recv, k_send, k_recv, do_send, do_recv, st_send, st_recv, xo_send, xo_recv, po_send, po_recv,
                q_sums_sems, kv_sums_sems, loc, outs, w_send, w_recv, strip_send, strip_recv):
    me = lax.axis_index('cp')
    core = lax.axis_index('data')
    row, col = me // GROUP, me % GROUP
    x, y0 = col % RING, col // RING
    y1, z = row % TWO, row // TWO

    def row_slot(rank):
        return RING * (y0 ^ (rank // RING)) + (x + gray(rank % RING)) % RING

    def col_slot(rank):
        return TWO * ((z + gray(rank % RING)) % RING) + (y1 ^ (rank // RING))

    def row_dev(rank):
        return {'cp': GROUP * row + row_slot(rank)}

    def col_dev(rank):
        return {'cp': GROUP * col_slot(rank) + col}

    args = [pltpu.make_async_copy(src, dst, loc.at[n]) for n, (src, dst) in enumerate(((q_arg, q_in), (do_arg, do_in), (kpe_arg, kpe_in), (wv_arg, wv_in), (wk_arg, wk_in), (c_arg, c_in)))]
    start(args)
    mate = {'data': 1 - core}
    barrier = pltpu.get_barrier_semaphore()

    def to_others(act):
        def one(n, carry):
            act((me + n) % CHIPS)
            return carry

        lax.fori_loop(1, CHIPS, one, 0)

    to_others(lambda d: pl.semaphore_signal(barrier, inc=1, device_id={'cp': d}))
    pl.semaphore_signal(barrier, inc=1, device_id=mate)

    done(args)
    wvt = wv_in[:].T
    for h in HALVES:
        q = q_in[:, part(h, HALF)]
        qt_s[col, h] = q
        q_s[col, h, :, :QK] = q.T
        qr_s[col, :, part(h, ROPE)] = q[NOPE:].T
    for h in HALVES:
        k_s[row, h, :, :NOPE] = mm(c_in[h], wk_in[:]).astype(BF)
        rope = kpe_in[:, part(h, HALF)].T
        k_s[row, h, :, NOPE:] = jnp.concatenate([rope, rope], axis=1)
        kr_s[row, :, part(h, ROPE)] = rope
        vt_s[row, h, :VAL] = mm_t(wvt, c_in[h]).astype(BF)

    pl.semaphore_wait(barrier, CHIPS)

    def like(n):
        return qr_s.at[pl.ds(0, n)]

    def q_copies(n, slot, dev):
        refs = [q_s.at[slot, :, :, :NOPE], qr_s.at[slot]]
        return remote(zip(refs, refs), q_send.at[n], q_recv.at[slot], dev, like(3))

    def k_copies(n, slot, dev):
        refs = [k_s.at[slot, :, :, :NOPE], kr_s.at[slot], vt_s.at[slot, :, :VAL]]
        return remote(zip(refs, refs), k_send.at[n], k_recv.at[slot], dev, like(5))

    def do_copies(n, slot, dev):
        ref = do_s.at[slot, :, :, :VAL]
        return remote([(ref, ref)], do_send.at[n], do_recv.at[slot], dev, like(TWO))

    first_copies = (FAR, 0, 1)

    def own_copies(copies, slot, dev, n):
        return copies(n, slot(0), dev(n + 1))

    def pair_copies(copies, slot, dev, n):
        return copies(RING + n, slot(RING), dev(n + 1))

    q_kind, k_kind, do_kind = (q_copies, row_slot, row_dev), (k_copies, col_slot, col_dev), (do_copies, row_slot, row_dev)

    for n in first_copies:
        start(own_copies(*q_kind, n))
        start(own_copies(*k_kind, n))

    def arrived(copies, slot, dev, rank):
        landed(copies(0, slot(rank), dev(1)))

    def wait_q(rank):
        arrived(*q_kind, rank)

    def wait_k(rank):
        arrived(*k_kind, rank)

    def wait_do(rank):
        arrived(*do_kind, rank)

    ones = jnp.where(lax.broadcasted_iota(jnp.int32, (AUG, HALF), 0) < 3, 1.0, 0.0).astype(BF)

    def clear(s, carry):
        for h in HALVES:
            for ref in (ot_s, dq_s, dk_s, dv_s, l_s):
                ref[s, h] = jnp.zeros(ref.shape[TWO:], F32)
            m_s[s, h] = jnp.full(m_s.shape[TWO:], NEG_BIG, F32)
            kt_s[s, h, QK:] = ones
            vt_s[s, h, VAL:] = ones
        dqr_s[s] = jnp.zeros((HALF, LANES), F32)
        return carry

    def place_q(s):
        for h in HALVES:
            q_s[s, h, :, NOPE:QK] = qr_s[s, :, part(h, ROPE)]
            qt_s[s, h] = q_s[s, h, :, :QK].T

    def place_k(s):
        for h in HALVES:
            rope = kr_s[s, :, part(h, ROPE)]
            k_s[s, h, :, NOPE:] = jnp.concatenate([rope, rope], axis=1)
            kt_s[s, h, :QK] = k_s[s, h, :, :QK].T

    def place_do(s):
        for h in HALVES:
            dot_s[s, h] = do_s[s, h, :, :VAL].T

    for h in HALVES:
        kt_s[row, h, :QK] = k_s[row, h, :, :QK].T
    for h in HALVES:
        do_s[col, h, :, :VAL] = do_in[h]
    place_do(col)
    lax.fori_loop(0, GROUP, clear, 0)

    def diagonal_half(ks, qs):
        return jnp.where((ks < row) | ((ks == row) & (col <= qs)), 0, 1)

    def two_blocks(ks, qs):
        h = diagonal_half(ks, qs)
        return (ks, qs, 0, 1), (ks, qs, h, h)

    own_blocks = [(row, col, kh, qh) for kh in HALVES for qh in HALVES if kh <= qh]

    def f_blocks(t):
        a, b = GROUP - 1, 0
        end = T_LAST
        for t0, a0, na, b0, nb, inner in RECTS[::-1]:
            u = t - t0
            pa, pb = (a0 + u % na, b0 + u // na) if inner else (a0 + u // nb, b0 + u % nb)
            a, b = jnp.where(t < end, pa, a), jnp.where(t < end, pb, b)
            end = t0
        a = jnp.where(a == FAR, RING, jnp.where(a == RING, FAR, a))
        return two_blocks(col_slot(a), jnp.where(t < T_LAST, row_slot(b), t - T_LAST))

    def f_scores(sc, blk):
        ks, qs, kh, qh = blk
        sc[:] = mm(k_s[ks, kh, :, :QK], qt_s[qs, qh])

    def f_use(sc, blk):
        ks, qs, kh, qh = blk
        s = sc[:]
        if isinstance(kh, int) and kh == qh:
            keys = lax.broadcasted_iota(jnp.int32, s.shape, 0)
            s = jnp.where(keys <= lax.broadcasted_iota(jnp.int32, s.shape, 1), s, NEG_BIG)
        m0 = m_s[qs, qh]
        m1 = jnp.maximum(m0, jnp.max(s, axis=0, keepdims=True))
        p = jnp.exp2((s - m1) * EXP2_SCALE)
        alpha = jnp.exp2((m0 - m1) * EXP2_SCALE)
        l_s[qs, qh] = l_s[qs, qh] * alpha + jnp.sum(p, axis=0, keepdims=True)
        m_s[qs, qh] = m1
        ot_s[qs, qh] = ot_s[qs, qh] * alpha + mm(vt_s[ks, kh, :VAL], p.astype(BF))

    def own_f():
        for blk in own_blocks:
            f_scores(sc0, blk)
            f_use(sc0, blk)

    own_f()

    def stats_copies(slot, n):
        return remote([(st_s.at[slot], st_r.at[slot, col])], st_send.at[slot], st_recv.at[slot], row_dev(n), st_r.at[slot, pl.ds(0, len(PEERS))])

    def make_stats(qs):
        for h in HALVES:
            d = jnp.sum(ot_s[qs, h] * dot_s[qs, h].astype(F32), axis=0, keepdims=True)
            for j in range(BLOCKS):
                c = part(j, LANES)
                for i, v in enumerate((m_s[qs, h, :, c], l_s[qs, h, :, c], d[:, c])):
                    st_s[qs, part(GROUP * i + BLOCKS * h + j, 1)] = v

    def start_stats(qs):
        for n in PEERS:
            start(stats_copies(qs, n))
        st_r[qs, col] = st_s[qs]

    def f_event(t):
        return among(t, tuple(sorted({*Q_STEPS, *K_STEPS, *DO_STEPS, T_RELAY, T_RELAY_K, T_OWN_DO, T_RELAY_DO})))

    def f_arrive(t):
        @pl.when(f_event(t))
        def _():
            @pl.when(among(t, Q_STEPS))
            def _():
                rank = at(t, Q_STEPS, PEERS)

                @pl.when(rank != RING)
                def _():
                    wait_q(rank)

                @pl.when(rank == 1)
                def _():
                    start(own_copies(*q_kind, TWO))
                place_q(row_slot(rank))

            @pl.when(among(t, K_STEPS))
            def _():
                rank = at(t, K_STEPS, K_RANKS)

                @pl.when(rank != RING)
                def _():
                    wait_k(rank)

                @pl.when(rank == 1)
                def _():
                    start(own_copies(*k_kind, TWO))
                place_k(col_slot(rank))

            @pl.when(among(t, DO_STEPS))
            def _():
                rank = at(t, DO_STEPS, DO_RANKS)
                wait_do(rank)
                place_do(row_slot(rank))

            @pl.when(t == T_RELAY)
            def _():
                wait_q(RING)
                for n in range(FAR):
                    start(pair_copies(*q_kind, n))

            @pl.when(t == T_RELAY_K)
            def _():
                wait_k(RING)
                for n in range(FAR):
                    start(pair_copies(*k_kind, n))

            @pl.when(t == T_OWN_DO)
            def _():
                for n in (*first_copies, TWO):
                    start(own_copies(*do_kind, n))

            @pl.when(t == T_RELAY_DO)
            def _():
                wait_do(RING)
                for n in range(FAR):
                    start(pair_copies(*do_kind, n))
                place_do(row_slot(RING))

    for t in NEIGHBOURS:
        f_arrive(t)
    blocks = f_blocks(jnp.int32(1))
    for sc, blk in zip((sc0, sc1), blocks):
        f_scores(sc, blk)

    def f_half(t, used, made, b1, b2):
        n1, n2 = after = f_blocks(jnp.minimum(t + 1, T_END - 1))
        eventful = f_event(t + TWO) | (t >= T_LAST)
        f_scores(made[0], n1)
        f_use(used[0], b1)
        f_scores(made[1], n2)
        f_use(used[1], b2)

        @pl.when(eventful)
        def _():
            @pl.when(t >= T_LAST)
            def _():
                @pl.when(t > T_LAST)
                def _():
                    start_stats(t - T_LAST - 1)

                make_stats(t - T_LAST)

            f_arrive(t + TWO)
        return after

    def f_step(u, carry):
        t = TWO * u + 1
        after = f_half(t, (sc0, sc1), (dp0, dp1), *carry)

        @pl.when(t < T_END - 1)
        def _():
            f_half(t + 1, (dp0, dp1), (sc0, sc1), *after)
        return f_blocks(jnp.minimum(t + TWO, T_END - 1))

    lax.fori_loop(0, T_END // TWO, f_step, blocks)
    start_stats(GROUP - 1)

    o_all = stg.at[pl.ds(0, TWO * VAL)]

    def o_refs(slot, buf):
        return [(ot_s.at[slot, h], buf.at[pl.ds(h * VAL, VAL)]) for h in HALVES]

    def o_copies(s):
        d = (s // RING) ^ y0
        return remote(o_refs(s, xo.at[d, x]), xo_send.at[s], xo_recv.at[d, x], {'cp': GROUP * row + RING * y0 + s % RING}, o_all)

    def o_pair():
        return remote(o_refs(row_slot(RING), po), po_send.at[0], po_recv.at[0], row_dev(RING), o_all)

    def dq_srcs(s, p):
        r = pl.ds(p * ROWS, ROWS)
        return [dq_s.at[s, 0, r], dq_s.at[s, 1, r], dqr_s.at[s, r]]

    def dq_dsts(buf):
        return [buf.at[:, pl.ds(LANES * j, LANES)] for j in range(3)]

    def kv_srcs(s, h):
        return [dk_s.at[s, h], dv_s.at[s, h]]

    def kv_dsts(buf):
        return [buf.at[pl.ds(0, QK)], buf.at[pl.ds(QK, VAL)]]

    dq_near, dq_far, dq_across = ring_sums(row_slot, row_dev, lambda d, p: RING if d else p + 1, dq_srcs, dq_dsts, (xq, xqv, pq), q_sums_sems, stg.at[pl.ds(0, ROWS * 3 * LANES // HALF)])
    kv_near, kv_far, kv_across = ring_sums(col_slot, col_dev, lambda d, p: p + 1, kv_srcs, kv_dsts, (zkv, zkvv, pkv), kv_sums_sems, stg.at[pl.ds(0, KV)])

    def local(pairs, n=0):
        return [pltpu.make_async_copy(src, dst, loc.at[n + i]) for i, (src, dst) in enumerate(pairs)]

    def o_local(d):
        return local([(xo.at[d, (x + gray(r)) % RING], stg.at[pl.ds(HALF * (r - 1), HALF // TWO)]) for r in range(1, RING)])

    def fetch_o(d):
        for r in range(1, RING):
            s = (x + gray(r)) % RING
            landed(remote(o_refs(0, xo.at[d, s]), xo_send.at[r], xo_recv.at[d, s], row_dev(r), o_all))
        start(o_local(d))

    def add_o(slot, d):
        done(o_local(d))
        for h in HALVES:
            ot_s[slot, h] = ot_s[slot, h] + sum(stg[HALF * n + h * VAL:HALF * n + (h + 1) * VAL] for n in range(FAR))

    def kv_local(d, h):
        return local([(zkv.at[d, n, h], stg.at[pl.ds(KV * (TWO * h + n), KV)]) for n in HALVES], TWO * h)

    def fetch_kv(d, h):
        for r in NEIGHBOURS:
            landed(kv_near(RING * d + r, h))
        start(kv_local(d, h))

    def add_kv(slot, d, h):
        done(kv_local(d, h))
        u = KV * TWO * h
        v = u + KV
        dk_s[slot, h] = dk_s[slot, h] + (stg[u:u + QK] + stg[v:v + QK])
        dv_s[slot, h] = dv_s[slot, h] + (stg[u + QK:v] + stg[v + QK:v + KV])

    def kv_via_local(d):
        return local([(zkvv.at[d, h], stg.at[pl.ds(KV * h, KV)]) for h in HALVES])

    def fetch_kv_via(d):
        for h in HALVES:
            landed(kv_far(d, h))
        start(kv_via_local(d))

    def add_kv_via(d):
        done(kv_via_local(d))
        for h in HALVES:
            slot, u = col_slot(RING * d + 1 + h), KV * h
            dk_s[slot, h] = dk_s[slot, h] + stg[u:u + QK]
            dv_s[slot, h] = dv_s[slot, h] + stg[u + QK:u + KV]

    def dq_stage(n, p):
        return stg.at[pl.ds(HALF * n + ROWS * p, ROWS), pl.ds(0, 3 * LANES)]

    def add_dq(slot, p, ns):
        r = part(p, ROWS)
        for j in range(3):
            c = part(j, LANES)
            total = sum(stg[HALF * n + ROWS * p:HALF * n + ROWS * (p + 1), c] for n in ns)
            if j < TWO:
                dq_s[slot, j, r] = dq_s[slot, j, r] + total
            else:
                dqr_s[slot, r] = dqr_s[slot, r] + total

    def sum_dq_via(d):
        for p in HALVES:
            landed(dq_far(d, p))
        copies = local([(xqv.at[d, p], dq_stage(0, p)) for p in HALVES])
        start(copies)
        done(copies)
        for p in HALVES:
            add_dq(row_slot(FAR if d else 1 + p), p, (0,))

    def dq_arrived(d):
        for p in HALVES:
            for r in NEIGHBOURS:
                landed(dq_near(RING * d + r, p))
        return [(xq.at[d, n, p], dq_stage(n, p)) for n in HALVES for p in HALVES]

    def columns(v):
        flat = jnp.concatenate([v[part(j, 1)] for j in range(BLOCKS)], axis=1)
        hi = flat.astype(BF).astype(F32)
        mid = (flat - hi).astype(BF).astype(F32)
        return jnp.concatenate([hi, mid, flat - hi - mid, jnp.zeros((AUG - 3, HALF), F32)], axis=0).T.astype(BF)

    def wait_stats(qs):
        landed(stats_copies(qs, 1))

    def prepare_two(qs):
        for n in HALVES:
            wait_stats(qs + n)
        for n in HALVES:
            prepare(qs + n)

    def prepare(qs):
        m, l, d = (st_r[qs, :, part(i, GROUP)] for i in range(3))
        m_all = jnp.max(m, axis=0)
        w = jnp.exp2((m - m_all[None]) * EXP2_SCALE)
        l_all = jnp.sum(w * l, axis=0)
        inv = 1.0 / l_all
        delta = jnp.sum(w * d, axis=0) * inv
        lse = m_all + jnp.log2(l_all) * (1.0 / EXP2_SCALE)
        mine = jnp.exp2((st_s[qs, :GROUP] - m_all) * EXP2_SCALE) * inv
        for h in HALVES:
            q_s[qs, h, :, QK:] = columns(-lse[part(h, BLOCKS)])
            do_s[qs, h, :, VAL:] = columns(-delta[part(h, BLOCKS)])
            for j in range(BLOCKS):
                c = part(j, LANES)
                ot_s[qs, h, :, c] = ot_s[qs, h, :, c] * mine[part(BLOCKS * h + j, 1)]

    def b_mixed(m):
        first, near, far = m < M_NEAR, m < M_FAR, m < M_OWN
        rest = jnp.where(near, m - M_NEAR, jnp.where(far, m - M_FAR, (m - M_OWN) // TWO))
        qs = row_slot(jnp.where(first, order(m // RING, Q_FIRST), order(rest, Q_REST)))
        kind = jnp.where(first, m % RING, jnp.where(near, 0, jnp.where(far, 1, TWO + m % TWO)))
        ks = jnp.where(kind < TWO, col_slot(K_ORDER[-1]), row)
        same = kind % TWO == 1
        h = diagonal_half(ks, qs)
        return ks, qs, jnp.where(same, h, 0), jnp.where(same, h, 1)

    def b_blocks(t):
        pick = lambda a, b: tuple(jnp.where(t < T_MIX, i, j) for i, j in zip(a, b))
        plain = two_blocks(col_slot(order(t // GROUP, K_ORDER)), t % GROUP)
        return tuple(pick(b, b_mixed(TWO * (t - T_MIX) + n)) for n, b in enumerate(plain))

    def b_scores(sc, dp, blk):
        ks, qs, kh, qh = blk
        sc[:] = mm(q_s[qs, qh], kt_s[ks, kh])
        dp[:] = mm(do_s[qs, qh], vt_s[ks, kh])

    def b_elem(sc, dp, pr, ds, mask=False):
        p = jnp.exp2(sc[:] * EXP2_SCALE)
        if mask:
            rows = lax.broadcasted_iota(jnp.int32, p.shape, 0)
            p = jnp.where(lax.broadcasted_iota(jnp.int32, p.shape, 1) <= rows, p, 0.0)
        pr[:] = p.astype(BF)
        ds[:] = (p * dp[:]).astype(BF)

    def b_grads(pr, ds, blk):
        ks, qs, kh, qh = blk
        p = pr[:]
        g = ds[:]
        dv_s[ks, kh] += mm(dot_s[qs, qh], p)
        dk_s[ks, kh] += mm(qt_s[qs, qh], g)
        dq = mm(g, k_s[ks, kh])
        dq_s[qs, qh] += dq[:, :NOPE]
        side = lax.broadcasted_iota(jnp.int32, (1, LANES), 1) // ROPE
        dqr_s[qs] += jnp.where(side == qh, dq[:, NOPE:], 0.0)

    early_half = 1 - diagonal_half(col_slot(K_ORDER[-1]), 0)

    def b_events(t):
        @pl.when((t <= GROUP) | among(t, (*T_VIA, *T_FETCH, *T_ADD, *T_NEAR, *T_ONE, T_NEAR_MID, T_NEAR_LAST, T_PAIR_O - 1, T_PAIR_O, T_PAIR_O + 1, T_VIA_Q, T_Q_FIVE, T_Q_SIX)) | among(t, tuple(v + i for v in T_PAIR_KV for i in range(3))))
        def _():
            @pl.when((t < GROUP - 1) & (t % TWO == 1))
            def _():
                prepare_two(t + 1)

            @pl.when((t <= GROUP) & ((t - 1) % RING != x))
            def _():
                start(o_copies(t - 1))

            @pl.when(among(t, T_VIA))
            def _():
                for h in HALVES:
                    start(kv_far(at(t, T_VIA, (1, 0)), h))

            @pl.when(among(t, T_FETCH))
            def _():
                fetch_kv_via(at(t, T_FETCH, (1, 0)))

            @pl.when(among(t, T_ADD))
            def _():
                add_kv_via(at(t, T_ADD, (1, 0)))

            @pl.when(among(t, T_NEAR))
            def _():
                for h in HALVES:
                    start(kv_near(at(t, T_NEAR, NEAR), h))

            @pl.when(among(t, T_ONE))
            def _():
                start(kv_near(1, at(t, T_ONE, (1, 0))))

            @pl.when(t == T_NEAR_MID)
            def _():
                start(kv_near(K_ORDER[-1], early_half))

            @pl.when(t == T_NEAR_LAST)
            def _():
                start(kv_near(K_ORDER[-1], 1 - early_half))

            @pl.when(t == T_VIA_Q)
            def _():
                for p in HALVES:
                    start(dq_far(1, p))

            @pl.when(t == T_Q_FIVE)
            def _():
                start(dq_near(5, 0) + dq_near(5, 1))

            @pl.when(t == T_Q_SIX)
            def _():
                start(dq_near(6, 0) + dq_near(6, 1))

            @pl.when(t == T_PAIR_O - 1)
            def _():
                fetch_o(1)

            @pl.when(t == T_PAIR_O)
            def _():
                add_o(row_slot(RING), 1)

            @pl.when(t == T_PAIR_O + 1)
            def _():
                start(o_pair())

            for h, v in enumerate(T_PAIR_KV):
                @pl.when(t == v)
                def _():
                    fetch_kv(1, h)

                @pl.when(t == v + 1)
                def _():
                    add_kv(col_slot(RING), 1, h)

                @pl.when(t == v + TWO)
                def _():
                    start(kv_across(h))

    def b_step(t, carry):
        before, (b1, b2) = carry
        after = b_blocks(jnp.minimum(t + 1, T_END - TWO))
        b_scores(sc1, dp1, b2)
        b_elem(sc0, dp0, pr0, ds0)
        b_grads(pr1, ds1, before)
        b_scores(sc0, dp0, after[0])
        b_elem(sc1, dp1, pr1, ds1)
        b_grads(pr0, ds0, b1)
        b_events(t + 1)
        return b2, after

    for ref in (pr1, ds1):
        ref[:] = jnp.zeros(ref.shape, BF)
    prepare_two(0)
    blocks = b_blocks(jnp.int32(0))
    b_scores(sc0, dp0, blocks[0])
    before, _ = lax.fori_loop(0, T_END - 1, b_step, (blocks[1], blocks))
    start(dq_near(1, 1) + dq_near(2, 0))
    b_grads(pr1, ds1, before)

    def own_b():
        for blk in own_blocks:
            b_scores(sc0, dp0, blk)
            b_elem(sc0, dp0, pr0, ds0, mask=blk[TWO] == blk[3])
            b_grads(pr0, ds0, blk)

    own_b()

    def finish_o():
        fetch_o(0)
        add_o(col, 0)
        landed(o_pair())
        last_o = local([(po, stg.at[pl.ds(HALF // TWO, HALF // TWO)])])
        start(last_o)
        for n in range(RING):
            left(own_copies(*do_kind, n))
        done(last_o)
        for h in HALVES:
            do_s[col, h, :, :VAL] = (ot_s[col, h] + stg[part(TWO + h, VAL)]).T.astype(BF)

    sum_dq_via(1)
    start(dq_far(0, 0) + dq_far(0, 1))
    for pr, h in zip((pr0, pr1), HALVES):
        pr[:] = c_in[h].T

    def finish_dq_pair():
        copies = local(dq_arrived(1))
        start(copies)
        done(copies)
        for p in HALVES:
            add_dq(row_slot(RING), p, HALVES)

    finish_dq_pair()
    start(dq_across(0))

    def finish_dkv():
        sums = None
        pair = local([(pkv.at[h], sc.at[pl.ds(0, KV)]) for h, sc in enumerate((sc0, sc1))], RING)
        for h in HALVES:
            landed(kv_across(h))
        start(pair)
        for h in HALVES:
            fetch_kv(0, h)
        done(pair)
        for h, sc in enumerate((sc0, sc1)):
            add_kv(row, 0, h)
            dk = (dk_s[row, h] + sc[:QK]) * SCALE
            dv = dv_s[row, h] + sc[QK:KV]
            rope_s[:, part(h, HALF)] = dk[NOPE:]
            kv = jnp.concatenate([dk[:NOPE].T, dv.T], axis=1)
            (dp0, dp1)[h][:, :NOPE + VAL] = kv
            product = mm((pr0, pr1)[h][:].astype(F32), kv)
            sums = product if sums is None else sums + product
        w_s[0] = sums[:, :NOPE]
        w_s[1] = sums[:, NOPE:]

    finish_dkv()

    def w_swap(src, dst, n):
        return remote([(src, dst)], w_send.at[n], w_recv.at[n], mate, src)

    def strip(d):
        return rows_of(d, STRIP)

    def to_all(n, src, dst):
        to_others(lambda d: pltpu.make_async_remote_copy(src(d), dst, strip_send.at[n], strip_recv.at[n], device_id={'cp': d}).start())

    def all_of(sem, n):
        strips = wr_r.at[pl.ds(0, CHIPS - 1)]
        pltpu.make_async_copy(strips, strips, sem.at[n]).wait()

    first = w_swap(w_s.at[1 - core], ws_r, 0)
    start(first)

    def left_early():
        left(stats_copies(0, 1))
        for r in PEERS:
            left(stats_copies(r, 1))
            if r != RING:
                left(o_copies(row_slot(r)))
            if r % RING in NEIGHBOURS:
                for p in HALVES:
                    left(kv_near(r, p))
        for p in HALVES:
            left(kv_across(p) + dq_far(1, p))
            for r in NEIGHBOURS:
                left(dq_near(RING + r, p))
            for d in HALVES:
                left(kv_far(d, p))
        left(o_pair())
        for n in range(RING):
            left(own_copies(*q_kind, n) + own_copies(*k_kind, n))
        for n in range(FAR):
            left(pair_copies(*q_kind, n) + pair_copies(*k_kind, n) + pair_copies(*do_kind, n))

    def finish_c():
        w_all = jnp.concatenate([wk_in[:], wv_in[:]], axis=1).astype(F32)
        for kv, out in ((dp0, sc0), (dp1, sc1)):
            out[:] = mm_t(kv[:, :NOPE + VAL], w_all)

    def w_one():
        landed(first)
        wr_s[:] = w_s[core] + ws_r[:]

    w_one()
    to_all(0, lambda d: wr_s.at[strip(d)], wr_r.at[me])
    start(dq_across(1))
    wr_r[me] = wr_s[strip(me)]
    sum_dq_via(0)
    start(dq_near(1, 0) + dq_near(2, 1))
    finish_o()
    finish_c()
    outputs = [(do_s.at[col, :, :, :VAL], out_o), (sc0, out_c.at[0]), (sc1, out_c.at[1]), (rope_s, out_r)]
    finals = [pltpu.make_async_copy(src, dst, outs.at[n]) for n, (src, dst) in enumerate(outputs)]
    start(finals)
    left(first)

    left_early()

    def w_two():
        all_of(strip_recv, 0)
        w_s[core, strip(me)] = jnp.sum(wr_r[:], axis=0)

    w_two()
    mine = w_s.at[core, strip(me)]
    to_all(1, lambda d: mine, mine)

    def finish_dq():
        pairs = dq_arrived(0)
        for p in HALVES:
            landed(dq_across(p))
        copies = local(pairs + [(pq.at[p], dq_stage(TWO, p)) for p in HALVES])
        start(copies)
        done(copies)
        for p in HALVES:
            add_dq(col, p, range(3))
        for h in HALVES:
            q_out_s[:NOPE, part(h, HALF)] = (dq_s[col, h] * SCALE).T
        rope = (dqr_s[col] * SCALE).T
        for h in HALVES:
            q_out_s[NOPE:, part(h, HALF)] = rope[part(h, ROPE)]

    finish_dq()
    q_out = [pltpu.make_async_copy(q_out_s, out_q, outs.at[RING])]
    start(q_out)

    def w_three():
        all_of(strip_recv, 1)

    w_three()
    last = w_swap(w_s.at[core], wl_r, 1)
    own_w = [pltpu.make_async_copy(w_s.at[core], out_w.at[core], outs.at[RING + 1])]
    start(last + own_w)

    def left_late():
        for n in HALVES:
            all_of(strip_send, n)
        for p in HALVES:
            left(dq_across(p) + dq_far(0, p))
            for r in NEIGHBOURS:
                left(dq_near(r, p))

    left_late()

    def out_done():
        landed(last)
        mate_w = [pltpu.make_async_copy(wl_r, out_w.at[1 - core], outs.at[RING + TWO])]
        start(mate_w)
        left(last)
        done(finals + q_out + own_w + mate_w)

    out_done()


def core_call(c, kpe, q, wk, wv, do):
    dma = lambda *s: pltpu.SemaphoreType.DMA(s)
    shape = jax.ShapeDtypeStruct
    per = (GROUP, TWO)
    wide = lambda *s: pltpu.VMEM(per + s, BF)
    sums = lambda *s: pltpu.VMEM(per + s, F32)
    f32 = lambda *s: pltpu.VMEM(s, F32)
    packed = pltpu.VMEM((GROUP, HALF, LANES), BF)

    def sum_sems():
        return [dma(*s) for s in ((GROUP, TWO), (TWO, TWO, TWO), (TWO, TWO), (TWO, TWO), (TWO,), (TWO,))]

    def sum_bufs(*s):
        return [shape((TWO, TWO, TWO, *s), F32), shape((TWO, TWO, *s), F32), shape((TWO, *s), F32)]

    square = (HALF, HALF)
    scratch = [pltpu.VMEM(a.shape, a.dtype) for a in (c, kpe, q, wk, wv, do)] + [
        wide(HALF, QK + AUG), packed, wide(HALF, QK + ROPE), packed, wide(VAL + AUG, HALF), wide(HALF, VAL + AUG),
        wide(QK, HALF), wide(QK + AUG, HALF), wide(VAL, HALF),
        sums(VAL, HALF), sums(1, HALF), sums(1, HALF),
        sums(HALF, NOPE), f32(GROUP, HALF, LANES), sums(QK, HALF), sums(VAL, HALF),
        f32(GROUP, 3 * GROUP, LANES), f32(GROUP, GROUP, 3 * GROUP, LANES), f32(3 * HALF, HALF),
        f32(TWO, LATENT, NOPE), f32(LATENT, NOPE), f32(LATENT, NOPE), f32(ROPE, TWO * HALF), f32(QK, TWO * HALF),
        f32(LATENT, NOPE), f32(CHIPS, STRIP, NOPE),
        *[f32(*square)] * RING, *[pltpu.VMEM(square, BF)] * RING,
        *[dma(GROUP)] * GROUP, dma(GROUP), dma(TWO, RING), dma(1), dma(1),
        sum_sems(), sum_sems(), dma(GROUP), dma(GROUP), dma(TWO), dma(TWO), dma(TWO), dma(TWO),
    ]
    results = [
        shape((TWO, HALF, VAL), BF), shape((QK, TWO * HALF), F32), shape((TWO, HALF, LATENT), F32), shape((ROPE, TWO * HALF), F32),
        shape((TWO, LATENT, NOPE), F32),
    ]
    landing = [shape((TWO, RING, TWO * VAL, HALF), F32), shape((TWO * VAL, HALF), F32), *sum_bufs(ROWS, 3 * LANES), *sum_bufs(KV, HALF)]
    anywhere = pl.BlockSpec(memory_space=pl.ANY)
    return pl.pallas_call(
        core_kernel,
        out_shape=results + landing,
        in_specs=[anywhere] * 6,
        out_specs=[anywhere] * len(results + landing),
        scratch_shapes=scratch,
        compiler_params=pltpu.CompilerParams(collective_id=0, has_side_effects=True, vmem_limit_bytes=67043328),
        name='core',
    )(c, kpe, q, wk, wv, do)[:len(results)]


def solution(mesh):
    batch = ('pod', 'data')
    token_spec = P(batch, 'cp')
    sum_spec = P('pod')

    def per_device(c_latent, k_rope, queries, w_uk, w_uv, d_out):
        halves = lambda a: a.reshape(TWO, HALF, a.shape[-1])
        o, gq, gc, gr, gw = core_call(halves(c_latent), k_rope[0].T, queries[0, :, 0].T, w_uk[:, 0], w_uv[:, 0], halves(d_out))
        return o.reshape(d_out.shape), gq.T.reshape(queries.shape), gc.reshape(c_latent.shape), gr.T.reshape(k_rope.shape), gw[0, :, None], gw[1, :, None]

    return jax.shard_map(per_device, mesh=mesh, in_specs=(token_spec, token_spec, token_spec, P(), P(), token_spec), out_specs=(token_spec, token_spec, token_spec, token_spec, sum_spec, sum_spec), check_vma=False)
```
